8 devices in a mesh: dp: 1 (over z), tp: 8 (over y, x, core).
Axes of the slice: x: 2, y: 2, z: 1, core: 2. Of those that a mesh axis runs over, the one named last changes fastest.
Arguments:
- hidden: bfloat16 [256, 4096], P('dp')
- positions: int32 [256], P('dp')
- k_cache: bfloat16 [2, 256, 128, 8, 128], P(None, 'dp', None, 'tp')
- v_cache: bfloat16 [2, 256, 128, 8, 128], P(None, 'dp', None, 'tp')
- attn_norm: bfloat16 [2, 4096], replicated
- w_query: bfloat16 [2, 4096, 4096], P(None, None, 'tp')
- w_key: bfloat16 [2, 4096, 1024], P(None, None, 'tp')
- w_value: bfloat16 [2, 4096, 1024], P(None, None, 'tp')
- w_out: bfloat16 [2, 4096, 4096], P(None, 'tp')
- mlp_norm: bfloat16 [2, 4096], replicated
- w_gate: bfloat16 [2, 4096, 14336], P(None, None, 'tp')
- w_up: bfloat16 [2, 4096, 14336], P(None, None, 'tp')
- w_down: bfloat16 [2, 14336, 4096], P(None, 'tp')
Outputs:
- output 1: bfloat16 [256, 4096], P('dp')
- output 2: bfloat16 [2, 256, 128, 8, 128], P(None, 'dp', None, 'tp')
- output 3: bfloat16 [2, 256, 128, 8, 128], P(None, 'dp', None, 'tp')
All inputs are finite; a program needn't handle non-finite values.
Results may differ from the reference program's by a relative error of at most 0.02.
Values are sent between devices in bfloat16 or wider.
A program may use at most 1 GiB of HBM per device.

```python
import math
import jax
import jax.numpy as jnp
from jax import lax

LAYERS = 2
BATCH = 256
SEQ = 128
D = 4096
HEADS = 32
KV_HEADS = 8
HEAD = 128
FF = 14336


def normal_weight(rng_key, shape, scale):
    return (jax.random.normal(rng_key, shape, jnp.float32) * scale).astype(jnp.bfloat16)


def setup_inputs(seed: int = 0, part: int = 0) -> dict:
    base_key = jax.random.key(seed)
    shared_keys = jax.random.split(base_key, 9)
    part_keys = jax.random.split(jax.random.fold_in(base_key, part), 5)
    cache_shape = (LAYERS, BATCH, SEQ, KV_HEADS, HEAD)
    drawn_pos = jax.random.randint(part_keys[1], (BATCH,), SEQ // 8, SEQ, dtype=jnp.int32)
    drawn_pos = drawn_pos.at[0].set(SEQ - 1).at[1].set(SEQ // 8)
    return dict(
        hidden=normal_weight(part_keys[0], (BATCH, D), 1.0),
        positions=jax.random.permutation(part_keys[2], drawn_pos),
        k_cache=normal_weight(part_keys[3], cache_shape, 1.0),
        v_cache=normal_weight(part_keys[4], cache_shape, 1.0),
        attn_norm=(1.0 + 0.3 * jax.random.normal(shared_keys[0], (LAYERS, D), jnp.float32)).astype(jnp.bfloat16),
        w_query=normal_weight(shared_keys[1], (LAYERS, D, HEADS * HEAD), D ** -0.5),
        w_key=normal_weight(shared_keys[2], (LAYERS, D, KV_HEADS * HEAD), 1.5 * D ** -0.5),
        w_value=normal_weight(shared_keys[3], (LAYERS, D, KV_HEADS * HEAD), 1.5 * D ** -0.5),
        w_out=normal_weight(shared_keys[4], (LAYERS, HEADS * HEAD, D), 0.5 * (SEQ / (HEADS * HEAD)) ** 0.5),
        mlp_norm=(1.0 + 0.3 * jax.random.normal(shared_keys[5], (LAYERS, D), jnp.float32)).astype(jnp.bfloat16),
        w_gate=normal_weight(shared_keys[6], (LAYERS, D, FF), D ** -0.5),
        w_up=normal_weight(shared_keys[7], (LAYERS, D, FF), D ** -0.5),
        w_down=normal_weight(shared_keys[8], (LAYERS, FF, D), 1.5 * FF ** -0.5),
    )


def rms_norm(hidden, weight):
    hidden_f32 = hidden.astype(jnp.float32)
    mean_sq = jnp.mean(hidden_f32 * hidden_f32, axis=-1, keepdims=True)
    return (hidden_f32 * lax.rsqrt(mean_sq + 1e-5) * weight.astype(jnp.float32)).astype(jnp.bfloat16)


def rope_tables(positions, head_dim):
    half_dim = head_dim // 2
    inv_freq = jnp.power(500000.0, -jnp.arange(half_dim, dtype=jnp.float32) * (2.0 / head_dim))
    wavelen = (2.0 * math.pi) / inv_freq
    smooth = (8192.0 / wavelen - 1.0) / 3.0
    blended = (1.0 - smooth) * inv_freq / 8.0 + smooth * inv_freq
    scaled = jnp.where(wavelen < 2048.0, inv_freq, jnp.where(wavelen > 8192.0, inv_freq / 8.0, blended))
    angles = positions.astype(jnp.float32)[:, None] * scaled[None, :]
    return jnp.cos(angles), jnp.sin(angles)


def apply_rope(vectors, cos_tab, sin_tab):
    half_dim = vectors.shape[-1] // 2
    vec_f32 = vectors.astype(jnp.float32)
    first = vec_f32[..., :half_dim]
    second = vec_f32[..., half_dim:]
    cos_b = cos_tab[:, None, :]
    sin_b = sin_tab[:, None, :]
    return jnp.concatenate([first * cos_b - second * sin_b, second * cos_b + first * sin_b], axis=-1).astype(jnp.bfloat16)


def attend(query, k_all, v_all, visible):
    scores = jnp.einsum('bkgd,bskd->bkgs', query.astype(jnp.float32), k_all.astype(jnp.float32)) * (query.shape[-1] ** -0.5)
    scores = jnp.where(visible, scores, -jnp.inf)
    prob_rows = jax.nn.softmax(scores, axis=-1).astype(jnp.bfloat16)
    attn_out = jnp.einsum('bkgs,bskd->bkgd', prob_rows.astype(jnp.float32), v_all.astype(jnp.float32))
    return attn_out.astype(jnp.bfloat16)


def reference(hidden, positions, k_cache, v_cache, attn_norm, w_query, w_key, w_value, w_out, mlp_norm, w_gate, w_up, w_down):
    group = HEADS // KV_HEADS
    cos_tab, sin_tab = rope_tables(positions, HEAD)
    seq_ids = jnp.arange(SEQ)
    at_pos = (seq_ids[None, :] == positions[:, None])[:, :, None, None]
    visible = (seq_ids[None, :] <= positions[:, None])[:, None, None, :]

    def layer_step(state, layer_args):
        norm_attn, wq_layer, wk_layer, wv_layer, wo_layer, norm_mlp, wg_layer, wu_layer, wd_layer, k_layer, v_layer = layer_args
        normed = rms_norm(state, norm_attn)
        query = jnp.dot(normed, wq_layer, preferred_element_type=jnp.float32).astype(jnp.bfloat16)
        key_new = jnp.dot(normed, wk_layer, preferred_element_type=jnp.float32).astype(jnp.bfloat16)
        value_new = jnp.dot(normed, wv_layer, preferred_element_type=jnp.float32).astype(jnp.bfloat16)
        query = apply_rope(query.reshape(BATCH, HEADS, HEAD), cos_tab, sin_tab)
        key_new = apply_rope(key_new.reshape(BATCH, KV_HEADS, HEAD), cos_tab, sin_tab)
        value_new = value_new.reshape(BATCH, KV_HEADS, HEAD)
        k_layer = jnp.where(at_pos, key_new[:, None], k_layer)
        v_layer = jnp.where(at_pos, value_new[:, None], v_layer)
        attended = attend(query.reshape(BATCH, KV_HEADS, group, HEAD), k_layer, v_layer, visible)
        mixed = jnp.dot(attended.reshape(BATCH, HEADS * HEAD), wo_layer, preferred_element_type=jnp.float32)
        state = state + mixed.astype(jnp.bfloat16)
        normed = rms_norm(state, norm_mlp)
        gate_proj = jnp.dot(normed, wg_layer, preferred_element_type=jnp.float32).astype(jnp.bfloat16)
        up_proj = jnp.dot(normed, wu_layer, preferred_element_type=jnp.float32).astype(jnp.bfloat16)
        activated = (jax.nn.silu(gate_proj.astype(jnp.float32)) * up_proj.astype(jnp.float32)).astype(jnp.bfloat16)
        state = state + jnp.dot(activated, wd_layer, preferred_element_type=jnp.float32).astype(jnp.bfloat16)
        return state, (k_layer, v_layer)

    stacked = (attn_norm, w_query, w_key, w_value, w_out, mlp_norm, w_gate, w_up, w_down, k_cache, v_cache)
    final, (k_out, v_out) = lax.scan(layer_step, hidden, stacked)
    return final, k_out, v_out
```

```python
import functools
import math
import jax
import jax.numpy as jnp
from jax import lax
from jax.experimental import pallas as pl
from jax.experimental.pallas import tpu as pltpu
from jax.sharding import PartitionSpec as P

MESH = pl.DeviceIdType.MESH
F32 = jnp.float32
BF16 = jnp.bfloat16
ANY = pl.BlockSpec(memory_space=pl.ANY)
VMEM = pl.BlockSpec(memory_space=pltpu.VMEM)
SMEM = pl.BlockSpec(memory_space=pltpu.SMEM)

B = 256
D = 4096
S = 128
HD = 128
G = 4
QW = G * HD
NP = 8
PW = D // NP
FW = 1792
HB = B // 2

CB = 16
NCH = B // CB
NS = 6


def rope_tables(positions):
    half = HD // 2
    inv_freq = jnp.power(500000.0, -jnp.arange(half, dtype=F32) * (2.0 / HD))
    wavelen = (2.0 * math.pi) / inv_freq
    smooth = (8192.0 / wavelen - 1.0) / 3.0
    blended = (1.0 - smooth) * inv_freq / 8.0 + smooth * inv_freq
    scaled = jnp.where(wavelen < 2048.0, inv_freq, jnp.where(wavelen > 8192.0, inv_freq / 8.0, blended))
    angles = positions.astype(F32)[:, None] * scaled[None, :]
    c, s = jnp.cos(angles), jnp.sin(angles)
    return jnp.concatenate([c, c], axis=1), jnp.concatenate([-s, s], axis=1)


def norm_rows(x_ref, h_ref, w_ref, rows=32):
    def step(i, carry):
        sl = pl.ds(pl.multiple_of(i * rows, rows), rows)
        acc = jnp.zeros((rows, 128), F32)
        for c in range(D // 128):
            t = x_ref[sl, c * 128:(c + 1) * 128].astype(F32)
            acc = acc + t * t
        r = lax.rsqrt(jnp.sum(acc, axis=1, keepdims=True) * (1.0 / D) + 1e-5)
        for c in range(D // 512):
            cs = slice(c * 512, (c + 1) * 512)
            h_ref[sl, cs] = (x_ref[sl, cs].astype(F32) * r * w_ref[:, cs].astype(F32)).astype(BF16)
        return carry
    lax.fori_loop(0, B // rows, step, 0, unroll=2)


def attn_kernel(layer, first, pos_ref, x_hbm, nw_ref, cos_ref, sin_ref, wq_hbm, wk_hbm, wv_hbm, kc_hbm, vc_hbm, *rest):
    if first:
        o_ref, ko_hbm, vo_hbm = rest[:3]
        rest = rest[3:]
    else:
        o_ref, ko_hbm, vo_hbm = rest[2:5]
        rest = rest[5:]
    x_v, h_v, wq_v, wk_v, wv_v, acc, q4, o4, kn, vn, rid, kb, vb, wsem, xsem, ksem, vsem, kosem, vosem = rest

    def kv_in(c, slot):
        rs = pl.ds(c * CB, CB)
        return (pltpu.make_async_copy(kc_hbm.at[layer, rs], kb.at[slot], ksem.at[slot]),
                pltpu.make_async_copy(vc_hbm.at[layer, rs], vb.at[slot], vsem.at[slot]))

    def kv_out(c, slot):
        rs = pl.ds(c * CB, CB)
        return (pltpu.make_async_copy(kb.at[slot], ko_hbm.at[layer, rs], kosem.at[slot]),
                pltpu.make_async_copy(vb.at[slot], vo_hbm.at[layer, rs], vosem.at[slot]))

    xcopy = pltpu.make_async_copy(x_hbm, x_v, xsem)
    xcopy.start()
    KC = D // 4
    wcopies = []
    for c in range(4):
        rs = pl.ds(c * KC, KC)
        cs = [pltpu.make_async_copy(wq_hbm.at[layer, rs], wq_v.at[rs], wsem.at[c, 0]),
              pltpu.make_async_copy(wk_hbm.at[layer, rs], wk_v.at[rs], wsem.at[c, 1]),
              pltpu.make_async_copy(wv_hbm.at[layer, rs], wv_v.at[rs], wsem.at[c, 2])]
        for t in cs:
            t.start()
        wcopies.append(cs)
    for c in range(NS - 2):
        for t in kv_in(c, c):
            t.start()

    rid[...] = lax.broadcasted_iota(jnp.int32, (S, HD), 0).astype(F32).astype(BF16)
    xcopy.wait()
    norm_rows(x_v, h_v, nw_ref)
    for c in range(4):
        for t in wcopies[c]:
            t.wait()
        rs = slice(c * KC, (c + 1) * KC)
        w = jnp.concatenate([wq_v[rs, :], wk_v[rs, :], wv_v[rs, :]], axis=1)
        r = jnp.dot(h_v[:, rs], w, preferred_element_type=F32)
        if c == 0:
            acc[...] = r
        else:
            acc[...] += r

    cos = cos_ref[...]
    sin = sin_ref[...]

    def rope(t):
        t = t.astype(BF16).astype(F32)
        return (t * cos + pltpu.roll(t, HD // 2, 1) * sin).astype(BF16).astype(F32)

    for hd in range(G):
        q4[pl.ds(hd, B, stride=G), :] = rope(acc[:, hd * HD:(hd + 1) * HD])
    kn[...] = rope(acc[:, QW:QW + HD])
    vn[...] = acc[:, QW + HD:QW + 2 * HD].astype(BF16).astype(F32)

    scale = HD ** -0.5
    row = lax.broadcasted_iota(jnp.int32, (4 * G, HD), 0) // G
    lane = lax.broadcasted_iota(jnp.int32, (4 * G, HD), 1)
    even = (row % 2) == 0
    low = row < 2

    def chunk(c, carry):
        slot = c % NS
        for t in kv_in(c, slot):
            t.wait()
        rowid = rid[...]
        for g in range(CB // 4):
            b0 = c * CB + 4 * g
            ks, vs = [], []
            posr = jnp.zeros((4 * G, HD), jnp.int32)
            for i in range(4):
                p = pos_ref[b0 + i]
                posr = jnp.where(row == i, p, posr)
                hit = rowid == jnp.full((S, HD), p.astype(F32), F32).astype(BF16)
                kr = jnp.broadcast_to(kn[pl.ds(b0 + i, 1), :], (S, HD)).astype(BF16)
                vr = jnp.broadcast_to(vn[pl.ds(b0 + i, 1), :], (S, HD)).astype(BF16)
                k = jnp.where(hit, kr, kb[slot, 4 * g + i])
                v = jnp.where(hit, vr, vb[slot, 4 * g + i])
                kb[slot, 4 * g + i] = k
                vb[slot, 4 * g + i] = v
                ks.append(k)
                vs.append(v)
            q = q4[pl.ds(pl.multiple_of(b0 * G, 4 * G), 4 * G), :]
            lhs = jnp.concatenate([jnp.where(even, q, 0.0), jnp.where(even, 0.0, q)], axis=1).astype(BF16)
            kt = jnp.concatenate([jnp.concatenate(ks[:2], axis=1), jnp.concatenate(ks[2:], axis=1)], axis=0)
            s2 = lax.dot_general(lhs, kt, (((1,), (1,)), ((), ())), preferred_element_type=F32)
            s = jnp.where(low, s2[:, :S], s2[:, S:]) * scale
            s = jnp.where(lane <= posr, s, -jnp.inf)
            m = jnp.max(s, axis=1, keepdims=True)
            e = jnp.exp(s - m)
            p = e / jnp.sum(e, axis=1, keepdims=True)
            lhs = jnp.concatenate([jnp.where(low, p, 0.0), jnp.where(low, 0.0, p)], axis=1).astype(BF16)
            vt = jnp.concatenate([jnp.concatenate(vs[:2], axis=1), jnp.concatenate(vs[2:], axis=1)], axis=0)
            o2 = jnp.dot(lhs, vt, preferred_element_type=F32)
            o4[pl.ds(pl.multiple_of(b0 * G, 4 * G), 4 * G), :] = jnp.where(even, o2[:, :HD], o2[:, HD:])
        for t in kv_out(c, slot):
            t.start()
        nxt = c + NS - 2
        ns = nxt % NS

        @pl.when(nxt < NCH)
        def _():
            @pl.when(nxt >= NS)
            def _():
                for t in kv_out(nxt - NS, ns):
                    t.wait()
            for t in kv_in(nxt, ns):
                t.start()
        return carry

    lax.fori_loop(0, NCH, chunk, 0)
    for hd in range(G):
        o_ref[:, hd * HD:(hd + 1) * HD] = o4[pl.ds(hd, B, stride=G), :].astype(BF16)
    for c in range(NCH - NS, NCH):
        for t in kv_out(c, c % NS):
            t.wait()


def attn_call(layer, pos, x, nw, cos, sin, wq, wk, wv, kc, vc, prev):
    first = prev is None
    cache = jax.ShapeDtypeStruct(kc.shape, BF16)
    ins = [pos, x, nw, cos, sin, wq, wk, wv, kc, vc]
    specs = [SMEM, ANY, VMEM, VMEM, VMEM] + [ANY] * 5
    alias = {}
    if not first:
        alias = {len(ins): 1, len(ins) + 1: 2}
        ins += list(prev)
        specs += [ANY, ANY]
    return pl.pallas_call(
        functools.partial(attn_kernel, layer, first),
        name=f"attn{layer}",
        out_shape=(jax.ShapeDtypeStruct((B, QW), BF16), cache, cache),
        in_specs=specs,
        out_specs=(VMEM, ANY, ANY),
        scratch_shapes=[
            pltpu.VMEM((B, D), BF16),
            pltpu.VMEM((B, D), BF16),
            pltpu.VMEM((D, QW), BF16),
            pltpu.VMEM((D, HD), BF16),
            pltpu.VMEM((D, HD), BF16),
            pltpu.VMEM((B, QW + 2 * HD), F32),
            pltpu.VMEM((B * G, HD), F32),
            pltpu.VMEM((B * G, HD), F32),
            pltpu.VMEM((B, HD), F32),
            pltpu.VMEM((B, HD), F32),
            pltpu.VMEM((S, HD), BF16),
            pltpu.VMEM((NS, CB, S, HD), BF16),
            pltpu.VMEM((NS, CB, S, HD), BF16),
            pltpu.SemaphoreType.DMA((4, 3)),
            pltpu.SemaphoreType.DMA,
            pltpu.SemaphoreType.DMA((NS,)),
            pltpu.SemaphoreType.DMA((NS,)),
            pltpu.SemaphoreType.DMA((NS,)),
            pltpu.SemaphoreType.DMA((NS,)),
        ],
        input_output_aliases=alias,
        compiler_params=pltpu.CompilerParams(vmem_limit_bytes=60 * 2 ** 20),
    )(*ins)


def mlp_kernel(layer, o_ref, x_hbm, nw_ref, wo_hbm, wg_hbm, wu_hbm, wd_hbm, xo_hbm,
               wo_v, wg_v, wu_v, wd_v, part, xg, h_v, a_v, xown, d2d, r1, r2, wsem, xsem, ssem, rsem):
    me = lax.axis_index("tp")
    k = me % 2
    cx = (me // 2) % 2
    cy = me // 4
    pt = me + 1 - 2 * k
    xn = me + 2 - 4 * cx
    yn = me + 4 - 8 * cy
    dg = xn + 4 - 8 * cy

    def other(p):
        return p + 1 - 2 * k

    def pcols(p):
        return pl.ds(pl.multiple_of(p * PW, PW), PW)

    top = pl.ds(0, HB)
    bot = pl.ds(HB, HB)

    barrier = pltpu.get_barrier_semaphore()
    for d in (pt, xn, yn):
        pl.semaphore_signal(barrier, inc=1, device_id={"tp": d}, device_id_type=MESH)

    xc = pltpu.make_async_copy(x_hbm.at[:, pcols(me)], xown, xsem)
    xc.start()
    wcs = [pltpu.make_async_copy(wo_hbm.at[layer], wo_v, wsem.at[0])]
    NG = 4
    for i in range(NG):
        rs = pl.ds(i * (D // NG), D // NG)
        wcs.append(pltpu.make_async_copy(wg_hbm.at[layer, rs], wg_v.at[rs], wsem.at[1 + 2 * i]))
        wcs.append(pltpu.make_async_copy(wu_hbm.at[layer, rs], wu_v.at[rs], wsem.at[2 + 2 * i]))
    ND = 4
    for i in range(ND):
        rs = pl.ds(i * (FW // ND), FW // ND)
        wcs.append(pltpu.make_async_copy(wd_hbm.at[layer, rs], wd_v.at[rs], wsem.at[1 + 2 * NG + i]))
    for t in wcs:
        t.start()
    pl.semaphore_wait(barrier, 3)

    def send(src, dst, i, dev):
        c = pltpu.make_async_remote_copy(src_ref=src, dst_ref=dst, send_sem=ssem.at[i], recv_sem=rsem.at[i],
                                         device_id={"tp": dev}, device_id_type=MESH)
        c.start()
        return c

    def all_reduce(piece):
        order = (dg, xn, yn, me)
        dcs = []
        for t, p in enumerate(order):
            q = other(p)
            piece(q)
            dcs.append(send(part.at[q], d2d.at[t], t, pt))
            piece(p)

        def pair(t):
            dcs[t].wait_recv()
            p = order[t]
            part[p] = (part[p].astype(F32) + d2d[t].astype(F32)).astype(BF16)

        pair(0)
        sa0 = send(part.at[dg, top], r1.at[0], 4, xn)
        sb0 = send(part.at[dg, bot], r1.at[2], 5, yn)
        pair(1)
        sa1 = send(part.at[xn, top], r1.at[1], 6, xn)
        pair(2)
        sb1 = send(part.at[yn, bot], r1.at[3], 7, yn)
        sa0.wait_recv()
        part[yn, top] = (part[yn, top].astype(F32) + r1[0].astype(F32)).astype(BF16)
        sa2 = send(part.at[yn, top], r2.at[0], 8, yn)
        sb0.wait_recv()
        part[xn, bot] = (part[xn, bot].astype(F32) + r1[2].astype(F32)).astype(BF16)
        sb2 = send(part.at[xn, bot], r2.at[1], 9, xn)
        pair(3)
        sa1.wait_recv()
        sb1.wait_recv()
        sa2.wait_recv()
        tot = part[me, top].astype(F32) + r1[1].astype(F32) + r2[0].astype(F32)
        new = (xown[top].astype(F32) + tot.astype(BF16).astype(F32)).astype(BF16)
        xown[top] = new
        xg[me, top] = new
        ga0 = send(xg.at[me, top], xg.at[me, top], 10, yn)
        ga1 = send(xg.at[me, top], xg.at[me, top], 11, xn)
        sb2.wait_recv()
        tot = part[me, bot].astype(F32) + r1[3].astype(F32) + r2[1].astype(F32)
        new = (xown[bot].astype(F32) + tot.astype(BF16).astype(F32)).astype(BF16)
        xown[bot] = new
        xg[me, bot] = new
        gb0 = send(xg.at[me, bot], xg.at[me, bot], 12, xn)
        gb1 = send(xg.at[me, bot], xg.at[me, bot], 13, yn)
        gp = [send(xg.at[me], xg.at[me], 14, pt)]
        ga0.wait_recv()
        ga2 = send(xg.at[yn, top], xg.at[yn, top], 15, xn)
        gp.append(send(xg.at[yn, top], xg.at[yn, top], 16, pt))
        gb0.wait_recv()
        gb2 = send(xg.at[xn, bot], xg.at[xn, bot], 17, yn)
        gp.append(send(xg.at[xn, bot], xg.at[xn, bot], 18, pt))
        ga1.wait_recv()
        gp.append(send(xg.at[xn, top], xg.at[xn, top], 19, pt))
        gb1.wait_recv()
        gp.append(send(xg.at[yn, bot], xg.at[yn, bot], 20, pt))
        ga2.wait_recv()
        gp.append(send(xg.at[dg, top], xg.at[dg, top], 21, pt))
        gb2.wait_recv()
        gp.append(send(xg.at[dg, bot], xg.at[dg, bot], 22, pt))
        for c in gp:
            c.wait_recv()
        for c in dcs + [sa0, sb0, sa1, sb1, sa2, sb2, ga0, ga1, gb0, gb1, ga2, gb2] + gp:
            c.wait_send()

    wcs[0].wait()

    def out_piece(p):
        part[p] = jnp.dot(o_ref[...], wo_v[:, pcols(p)], preferred_element_type=F32).astype(BF16)

    xc.wait()
    all_reduce(out_piece)

    rows = 32

    def norm_step(i, carry):
        sl = pl.ds(pl.multiple_of(i * rows, rows), rows)
        acc = jnp.zeros((rows, 128), F32)
        for p in range(NP):
            for c in range(PW // 128):
                t = xg[p, sl, c * 128:(c + 1) * 128].astype(F32)
                acc = acc + t * t
        r = lax.rsqrt(jnp.sum(acc, axis=1, keepdims=True) * (1.0 / D) + 1e-5)
        for p in range(NP):
            cs = slice(p * PW, (p + 1) * PW)
            h_v[sl, cs] = (xg[p, sl].astype(F32) * r * nw_ref[:, cs].astype(F32)).astype(BF16)
        return carry

    lax.fori_loop(0, B // rows, norm_step, 0, unroll=2)

    for t in wcs[1:1 + 2 * NG]:
        t.wait()

    TN = 256

    def gate_up(j, carry):
        cs = pl.ds(pl.multiple_of(j * TN, TN), TN)
        w = jnp.concatenate([wg_v[:, cs], wu_v[:, cs]], axis=1)
        gu = jnp.dot(h_v[...], w, preferred_element_type=F32)
        gt = gu[:, :TN].astype(BF16).astype(F32)
        up = gu[:, TN:].astype(BF16).astype(F32)
        a_v[:, cs] = (gt * (1.0 / (1.0 + jnp.exp(-gt))) * up).astype(BF16)
        return carry

    lax.fori_loop(0, FW // TN, gate_up, 0)

    for t in wcs[1 + 2 * NG:]:
        t.wait()

    def down_piece(p):
        part[p] = jnp.dot(a_v[...], wd_v[:, pcols(p)], preferred_element_type=F32).astype(BF16)

    all_reduce(down_piece)

    ocs = [pltpu.make_async_copy(xg.at[p], xo_hbm.at[:, pl.ds(p * PW, PW)], ssem.at[p]) for p in range(NP)]
    for t in ocs:
        t.start()
    for t in ocs:
        t.wait()


def mlp_call(layer, o, x, nw, wo, wg, wu, wd):
    return pl.pallas_call(
        functools.partial(mlp_kernel, layer),
        name=f"mlp{layer}",
        out_shape=jax.ShapeDtypeStruct((B, D), BF16),
        in_specs=[VMEM, ANY, VMEM, ANY, ANY, ANY, ANY],
        out_specs=ANY,
        scratch_shapes=[
            pltpu.VMEM((QW, D), BF16),
            pltpu.VMEM((D, FW), BF16),
            pltpu.VMEM((D, FW), BF16),
            pltpu.VMEM((FW, D), BF16),
            pltpu.VMEM((NP, B, PW), BF16),
            pltpu.VMEM((NP, B, PW), BF16),
            pltpu.VMEM((B, D), BF16),
            pltpu.VMEM((B, FW), BF16),
            pltpu.VMEM((B, PW), BF16),
            pltpu.VMEM((4, B, PW), BF16),
            pltpu.VMEM((4, HB, PW), BF16),
            pltpu.VMEM((2, HB, PW), BF16),
            pltpu.SemaphoreType.DMA((13,)),
            pltpu.SemaphoreType.DMA,
            pltpu.SemaphoreType.DMA((23,)),
            pltpu.SemaphoreType.DMA((23,)),
        ],
        compiler_params=pltpu.CompilerParams(collective_id=layer, has_side_effects=True, vmem_limit_bytes=67043328),
    )(o, x, nw, wo, wg, wu, wd)


def solution(mesh):
    row_spec = P('dp', None)
    pos_spec = P('dp')
    cache_spec = P(None, 'dp', None, 'tp', None)
    norm_spec = P(None, None)
    col_spec = P(None, None, 'tp')
    split_rows = P(None, 'tp', None)

    def local_step(hidden, positions, k_cache, v_cache, attn_norm, w_query, w_key, w_value, w_out, mlp_norm, w_gate, w_up, w_down):
        cos, sin = rope_tables(positions)
        kc = k_cache.reshape(2, B, S, HD)
        vc = v_cache.reshape(2, B, S, HD)
        x = hidden
        prev = None
        for layer in range(2):
            o, ko, vo = attn_call(layer, positions, x, attn_norm[layer][None, :], cos, sin, w_query, w_key, w_value, kc, vc, prev)
            prev = (ko, vo)
            x = mlp_call(layer, o, x, mlp_norm[layer][None, :], w_out, w_gate, w_up, w_down)
        return x, prev[0].reshape(k_cache.shape), prev[1].reshape(v_cache.shape)

    return jax.shard_map(local_step, mesh=mesh, in_specs=(row_spec, pos_spec, cache_spec, cache_spec, norm_spec, col_spec, col_spec, col_spec, split_rows, norm_spec, col_spec, col_spec, split_rows), out_specs=(row_spec, cache_spec, cache_spec), check_vma=False)
```

```python
import functools
import math
import jax
import jax.numpy as jnp
from jax import lax
from jax.experimental import pallas as pl
from jax.experimental.pallas import tpu as pltpu
from jax.sharding import PartitionSpec as P

MESH = pl.DeviceIdType.MESH
F32 = jnp.float32
BF16 = jnp.bfloat16
ANY = pl.BlockSpec(memory_space=pl.ANY)
VMEM = pl.BlockSpec(memory_space=pltpu.VMEM)
SMEM = pl.BlockSpec(memory_space=pltpu.SMEM)

B = 256
D = 4096
S = 128
HD = 128
G = 4
QW = G * HD
NP = 8
PW = D // NP
FW = 1792
HB = B // 2

CB = 32
NCH = B // CB
NS = 5
PF = 3


def rope_tables(positions):
    half = HD // 2
    inv_freq = jnp.power(500000.0, -jnp.arange(half, dtype=F32) * (2.0 / HD))
    wavelen = (2.0 * math.pi) / inv_freq
    smooth = (8192.0 / wavelen - 1.0) / 3.0
    blended = (1.0 - smooth) * inv_freq / 8.0 + smooth * inv_freq
    scaled = jnp.where(wavelen < 2048.0, inv_freq, jnp.where(wavelen > 8192.0, inv_freq / 8.0, blended))
    angles = positions.astype(F32)[:, None] * scaled[None, :]
    c, s = jnp.cos(angles), jnp.sin(angles)
    return jnp.concatenate([c, c], axis=1), jnp.concatenate([-s, s], axis=1)


def norm_rows(x_ref, h_ref, w_ref, rows=32):
    def step(i, carry):
        sl = pl.ds(pl.multiple_of(i * rows, rows), rows)
        acc = jnp.zeros((rows, 128), F32)
        for c in range(D // 128):
            t = x_ref[sl, c * 128:(c + 1) * 128].astype(F32)
            acc = acc + t * t
        r = lax.rsqrt(jnp.sum(acc, axis=1, keepdims=True) * (1.0 / D) + 1e-5)
        for c in range(D // 512):
            cs = slice(c * 512, (c + 1) * 512)
            h_ref[sl, cs] = (x_ref[sl, cs].astype(F32) * r * w_ref[:, cs].astype(F32)).astype(BF16)
        return carry
    lax.fori_loop(0, B // rows, step, 0, unroll=2)


def attn_kernel(layer, first, pos_ref, x_hbm, nw_ref, cos_ref, sin_ref, wq_hbm, wk_hbm, wv_hbm, kc_hbm, vc_hbm, *rest):
    if first:
        o_ref, ko_hbm, vo_hbm = rest[:3]
        rest = rest[3:]
    else:
        o_ref, ko_hbm, vo_hbm = rest[2:5]
        rest = rest[5:]
    x_v, h_v, wq_v, wk_v, wv_v, acc, q4, o4, kn, vn, rid, kb, vb, wsem, xsem, ksem, vsem, kosem, vosem = rest

    def kv_in(c, slot):
        rs = pl.ds(c * CB, CB)
        return (pltpu.make_async_copy(kc_hbm.at[layer, rs], kb.at[slot], ksem.at[slot]),
                pltpu.make_async_copy(vc_hbm.at[layer, rs], vb.at[slot], vsem.at[slot]))

    def kv_out(c, slot):
        rs = pl.ds(c * CB, CB)
        return (pltpu.make_async_copy(kb.at[slot], ko_hbm.at[layer, rs], kosem.at[slot]),
                pltpu.make_async_copy(vb.at[slot], vo_hbm.at[layer, rs], vosem.at[slot]))

    xcopy = pltpu.make_async_copy(x_hbm, x_v, xsem)
    xcopy.start()
    KC = D // 4
    wcopies = []
    for c in range(4):
        rs = pl.ds(c * KC, KC)
        cs = [pltpu.make_async_copy(wq_hbm.at[layer, rs], wq_v.at[rs], wsem.at[c, 0]),
              pltpu.make_async_copy(wk_hbm.at[layer, rs], wk_v.at[rs], wsem.at[c, 1]),
              pltpu.make_async_copy(wv_hbm.at[layer, rs], wv_v.at[rs], wsem.at[c, 2])]
        for t in cs:
            t.start()
        wcopies.append(cs)
    for c in range(PF):
        for t in kv_in(c, c):
            t.start()

    rid[...] = lax.broadcasted_iota(jnp.int32, (S, HD), 0).astype(F32).astype(BF16)
    xcopy.wait()
    norm_rows(x_v, h_v, nw_ref)
    for c in range(4):
        for t in wcopies[c]:
            t.wait()
        rs = slice(c * KC, (c + 1) * KC)
        w = jnp.concatenate([wq_v[rs, :], wk_v[rs, :], wv_v[rs, :]], axis=1)
        r = jnp.dot(h_v[:, rs], w, preferred_element_type=F32)
        if c == 0:
            acc[...] = r
        else:
            acc[...] += r

    cos = cos_ref[...]
    sin = sin_ref[...]

    def rope(t):
        t = t.astype(BF16).astype(F32)
        return (t * cos + pltpu.roll(t, HD // 2, 1) * sin).astype(BF16).astype(F32)

    for hd in range(G):
        q4[pl.ds(hd, B, stride=G), :] = rope(acc[:, hd * HD:(hd + 1) * HD])
    kn[...] = rope(acc[:, QW:QW + HD])
    vn[...] = acc[:, QW + HD:QW + 2 * HD].astype(BF16).astype(F32)

    scale = HD ** -0.5
    row = lax.broadcasted_iota(jnp.int32, (4 * G, HD), 0) // G
    lane = lax.broadcasted_iota(jnp.int32, (CB * G, HD), 1)
    even = (row % 2) == 0
    low = row < 2

    def place(buf, new, slot, b0, i, rowid):
        hit = rowid == jnp.full((S, HD), pos_ref[b0 + i].astype(F32), F32).astype(BF16)
        r = jnp.broadcast_to(new[pl.ds(b0 + i, 1), :], (S, HD)).astype(BF16)
        t = jnp.where(hit, r, buf[slot, i])
        buf[slot, i] = t
        return t

    def quad(ts):
        return jnp.concatenate([jnp.concatenate(ts[:2], axis=1), jnp.concatenate(ts[2:], axis=1)], axis=0)

    def scores(c):
        slot = c % NS
        b0 = c * CB
        kv_in(c, slot)[0].wait()
        rowid = rid[...]
        out = []
        for g in range(CB // 4):
            kt = quad([place(kb, kn, slot, b0, 4 * g + i, rowid) for i in range(4)])
            q = q4[pl.ds(pl.multiple_of(b0 * G + 4 * G * g, 4 * G), 4 * G), :]
            lhs = jnp.concatenate([jnp.where(even, q, 0.0), jnp.where(even, 0.0, q)], axis=1).astype(BF16)
            s2 = lax.dot_general(lhs, kt, (((1,), (1,)), ((), ())), preferred_element_type=F32)
            out.append(jnp.where(low, s2[:, :S], s2[:, S:]))
        return jnp.concatenate(out, axis=0)

    def values(c, s):
        slot = c % NS
        b0 = c * CB
        kv_in(c, slot)[1].wait()
        rowid = rid[...]
        posr = []
        for g in range(CB // 4):
            t = jnp.zeros((4 * G, HD), jnp.int32)
            for i in range(4):
                t = jnp.where(row == i, pos_ref[b0 + 4 * g + i], t)
            posr.append(t)
        s = jnp.where(lane <= jnp.concatenate(posr, axis=0), s * scale, -jnp.inf)
        e = jnp.exp(s - jnp.max(s, axis=1, keepdims=True))
        p = e / jnp.sum(e, axis=1, keepdims=True)
        for g in range(CB // 4):
            vt = quad([place(vb, vn, slot, b0, 4 * g + i, rowid) for i in range(4)])
            pg = p[4 * G * g:4 * G * (g + 1)]
            lhs = jnp.concatenate([jnp.where(low, pg, 0.0), jnp.where(low, 0.0, pg)], axis=1).astype(BF16)
            o2 = jnp.dot(lhs, vt, preferred_element_type=F32)
            o4[pl.ds(pl.multiple_of(b0 * G + 4 * G * g, 4 * G), 4 * G), :] = jnp.where(even, o2[:, :HD], o2[:, HD:])

    def turn(c, j):
        kv_out(c, c % NS)[j].start()
        nxt = c + PF

        @pl.when(nxt < NCH)
        def _():
            @pl.when(nxt >= NS)
            def _():
                kv_out(nxt - NS, nxt % NS)[j].wait()
            kv_in(nxt, nxt % NS)[j].start()

    s0 = scores(0)
    turn(0, 0)

    def chunk(c, s):
        sn = scores(c + 1)
        values(c, s)
        turn(c + 1, 0)
        turn(c, 1)
        return sn

    sl = lax.fori_loop(0, NCH - 1, chunk, s0)
    values(NCH - 1, sl)
    turn(NCH - 1, 1)
    for hd in range(G):
        o_ref[:, hd * HD:(hd + 1) * HD] = o4[pl.ds(hd, B, stride=G), :].astype(BF16)
    for c in range(NCH - NS, NCH):
        for t in kv_out(c, c % NS):
            t.wait()


def attn_call(layer, pos, x, nw, cos, sin, wq, wk, wv, kc, vc, prev):
    first = prev is None
    cache = jax.ShapeDtypeStruct(kc.shape, BF16)
    ins = [pos, x, nw, cos, sin, wq, wk, wv, kc, vc]
    specs = [SMEM, ANY, VMEM, VMEM, VMEM] + [ANY] * 5
    alias = {}
    if not first:
        alias = {len(ins): 1, len(ins) + 1: 2}
        ins += list(prev)
        specs += [ANY, ANY]
    return pl.pallas_call(
        functools.partial(attn_kernel, layer, first),
        name=f"attn{layer}",
        out_shape=(jax.ShapeDtypeStruct((B, QW), BF16), cache, cache),
        in_specs=specs,
        out_specs=(VMEM, ANY, ANY),
        scratch_shapes=[
            pltpu.VMEM((B, D), BF16),
            pltpu.VMEM((B, D), BF16),
            pltpu.VMEM((D, QW), BF16),
            pltpu.VMEM((D, HD), BF16),
            pltpu.VMEM((D, HD), BF16),
            pltpu.VMEM((B, QW + 2 * HD), F32),
            pltpu.VMEM((B * G, HD), F32),
            pltpu.VMEM((B * G, HD), F32),
            pltpu.VMEM((B, HD), F32),
            pltpu.VMEM((B, HD), F32),
            pltpu.VMEM((S, HD), BF16),
            pltpu.VMEM((NS, CB, S, HD), BF16),
            pltpu.VMEM((NS, CB, S, HD), BF16),
            pltpu.SemaphoreType.DMA((4, 3)),
            pltpu.SemaphoreType.DMA,
            pltpu.SemaphoreType.DMA((NS,)),
            pltpu.SemaphoreType.DMA((NS,)),
            pltpu.SemaphoreType.DMA((NS,)),
            pltpu.SemaphoreType.DMA((NS,)),
        ],
        input_output_aliases=alias,
        compiler_params=pltpu.CompilerParams(vmem_limit_bytes=60 * 2 ** 20),
    )(*ins)


def mlp_kernel(layer, o_ref, x_hbm, nw_ref, wo_hbm, wg_hbm, wu_hbm, wd_hbm, xo_hbm,
               wo_v, wg_v, wu_v, wd_v, part, xg, h_v, a_v, xown, d2d, r1, r2, wsem, xsem, ssem, rsem):
    me = lax.axis_index("tp")
    k = me % 2
    cx = (me // 2) % 2
    cy = me // 4
    pt = me + 1 - 2 * k
    xn = me + 2 - 4 * cx
    yn = me + 4 - 8 * cy
    dg = xn + 4 - 8 * cy

    def other(p):
        return p + 1 - 2 * k

    def pcols(p):
        return pl.ds(pl.multiple_of(p * PW, PW), PW)

    top = pl.ds(0, HB)
    bot = pl.ds(HB, HB)

    barrier = pltpu.get_barrier_semaphore()
    for d in (pt, xn, yn):
        pl.semaphore_signal(barrier, inc=1, device_id={"tp": d}, device_id_type=MESH)

    xc = pltpu.make_async_copy(x_hbm.at[:, pcols(me)], xown, xsem)
    xc.start()
    wcs = [pltpu.make_async_copy(wo_hbm.at[layer], wo_v, wsem.at[0])]
    NG = 4
    for i in range(NG):
        rs = pl.ds(i * (D // NG), D // NG)
        wcs.append(pltpu.make_async_copy(wg_hbm.at[layer, rs], wg_v.at[rs], wsem.at[1 + 2 * i]))
        wcs.append(pltpu.make_async_copy(wu_hbm.at[layer, rs], wu_v.at[rs], wsem.at[2 + 2 * i]))
    ND = 4
    for i in range(ND):
        rs = pl.ds(i * (FW // ND), FW // ND)
        wcs.append(pltpu.make_async_copy(wd_hbm.at[layer, rs], wd_v.at[rs], wsem.at[1 + 2 * NG + i]))
    for t in wcs:
        t.start()
    pl.semaphore_wait(barrier, 3)

    def send(src, dst, i, dev):
        c = pltpu.make_async_remote_copy(src_ref=src, dst_ref=dst, send_sem=ssem.at[i], recv_sem=rsem.at[i],
                                         device_id={"tp": dev}, device_id_type=MESH)
        c.start()
        return c

    def all_reduce(piece):
        order = (dg, xn, yn, me)
        dcs = []
        for t, p in enumerate(order):
            q = other(p)
            piece(q)
            dcs.append(send(part.at[q], d2d.at[t], t, pt))
            piece(p)

        def pair(t):
            dcs[t].wait_recv()
            p = order[t]
            part[p] = (part[p].astype(F32) + d2d[t].astype(F32)).astype(BF16)

        pair(0)
        sa0 = send(part.at[dg, top], r1.at[0], 4, xn)
        sb0 = send(part.at[dg, bot], r1.at[2], 5, yn)
        pair(1)
        sa1 = send(part.at[xn, top], r1.at[1], 6, xn)
        pair(2)
        sb1 = send(part.at[yn, bot], r1.at[3], 7, yn)
        sa0.wait_recv()
        part[yn, top] = (part[yn, top].astype(F32) + r1[0].astype(F32)).astype(BF16)
        sa2 = send(part.at[yn, top], r2.at[0], 8, yn)
        sb0.wait_recv()
        part[xn, bot] = (part[xn, bot].astype(F32) + r1[2].astype(F32)).astype(BF16)
        sb2 = send(part.at[xn, bot], r2.at[1], 9, xn)
        pair(3)
        sa1.wait_recv()
        sb1.wait_recv()
        sa2.wait_recv()
        tot = part[me, top].astype(F32) + r1[1].astype(F32) + r2[0].astype(F32)
        new = (xown[top].astype(F32) + tot.astype(BF16).astype(F32)).astype(BF16)
        xown[top] = new
        xg[me, top] = new
        ga0 = send(xg.at[me, top], xg.at[me, top], 10, yn)
        ga1 = send(xg.at[me, top], xg.at[me, top], 11, xn)
        sb2.wait_recv()
        tot = part[me, bot].astype(F32) + r1[3].astype(F32) + r2[1].astype(F32)
        new = (xown[bot].astype(F32) + tot.astype(BF16).astype(F32)).astype(BF16)
        xown[bot] = new
        xg[me, bot] = new
        gb0 = send(xg.at[me, bot], xg.at[me, bot], 12, xn)
        gb1 = send(xg.at[me, bot], xg.at[me, bot], 13, yn)
        gp = [send(xg.at[me], xg.at[me], 14, pt)]
        ga0.wait_recv()
        ga2 = send(xg.at[yn, top], xg.at[yn, top], 15, xn)
        gp.append(send(xg.at[yn, top], xg.at[yn, top], 16, pt))
        gb0.wait_recv()
        gb2 = send(xg.at[xn, bot], xg.at[xn, bot], 17, yn)
        gp.append(send(xg.at[xn, bot], xg.at[xn, bot], 18, pt))
        ga1.wait_recv()
        gp.append(send(xg.at[xn, top], xg.at[xn, top], 19, pt))
        gb1.wait_recv()
        gp.append(send(xg.at[yn, bot], xg.at[yn, bot], 20, pt))
        ga2.wait_recv()
        gp.append(send(xg.at[dg, top], xg.at[dg, top], 21, pt))
        gb2.wait_recv()
        gp.append(send(xg.at[dg, bot], xg.at[dg, bot], 22, pt))
        for c in gp:
            c.wait_recv()
        for c in dcs + [sa0, sb0, sa1, sb1, sa2, sb2, ga0, ga1, gb0, gb1, ga2, gb2] + gp:
            c.wait_send()

    wcs[0].wait()

    def out_piece(p):
        part[p] = jnp.dot(o_ref[...], wo_v[:, pcols(p)], preferred_element_type=F32).astype(BF16)

    xc.wait()
    all_reduce(out_piece)

    rows = 32

    def norm_step(i, carry):
        sl = pl.ds(pl.multiple_of(i * rows, rows), rows)
        acc = jnp.zeros((rows, 128), F32)
        for p in range(NP):
            for c in range(PW // 128):
                t = xg[p, sl, c * 128:(c + 1) * 128].astype(F32)
                acc = acc + t * t
        r = lax.rsqrt(jnp.sum(acc, axis=1, keepdims=True) * (1.0 / D) + 1e-5)
        for p in range(NP):
            cs = slice(p * PW, (p + 1) * PW)
            h_v[sl, cs] = (xg[p, sl].astype(F32) * r * nw_ref[:, cs].astype(F32)).astype(BF16)
        return carry

    lax.fori_loop(0, B // rows, norm_step, 0, unroll=2)

    for t in wcs[1:1 + 2 * NG]:
        t.wait()

    TN = 256

    def gate_up(j, carry):
        cs = pl.ds(pl.multiple_of(j * TN, TN), TN)
        w = jnp.concatenate([wg_v[:, cs], wu_v[:, cs]], axis=1)
        gu = jnp.dot(h_v[...], w, preferred_element_type=F32)
        gt = gu[:, :TN].astype(BF16).astype(F32)
        up = gu[:, TN:].astype(BF16).astype(F32)
        a_v[:, cs] = (gt * (1.0 / (1.0 + jnp.exp(-gt))) * up).astype(BF16)
        return carry

    lax.fori_loop(0, FW // TN, gate_up, 0)

    for t in wcs[1 + 2 * NG:]:
        t.wait()

    def down_piece(p):
        part[p] = jnp.dot(a_v[...], wd_v[:, pcols(p)], preferred_element_type=F32).astype(BF16)

    all_reduce(down_piece)

    ocs = [pltpu.make_async_copy(xg.at[p], xo_hbm.at[:, pl.ds(p * PW, PW)], ssem.at[p]) for p in range(NP)]
    for t in ocs:
        t.start()
    for t in ocs:
        t.wait()


def mlp_call(layer, o, x, nw, wo, wg, wu, wd):
    return pl.pallas_call(
        functools.partial(mlp_kernel, layer),
        name=f"mlp{layer}",
        out_shape=jax.ShapeDtypeStruct((B, D), BF16),
        in_specs=[VMEM, ANY, VMEM, ANY, ANY, ANY, ANY],
        out_specs=ANY,
        scratch_shapes=[
            pltpu.VMEM((QW, D), BF16),
            pltpu.VMEM((D, FW), BF16),
            pltpu.VMEM((D, FW), BF16),
            pltpu.VMEM((FW, D), BF16),
            pltpu.VMEM((NP, B, PW), BF16),
            pltpu.VMEM((NP, B, PW), BF16),
            pltpu.VMEM((B, D), BF16),
            pltpu.VMEM((B, FW), BF16),
            pltpu.VMEM((B, PW), BF16),
            pltpu.VMEM((4, B, PW), BF16),
            pltpu.VMEM((4, HB, PW), BF16),
            pltpu.VMEM((2, HB, PW), BF16),
            pltpu.SemaphoreType.DMA((13,)),
            pltpu.SemaphoreType.DMA,
            pltpu.SemaphoreType.DMA((23,)),
            pltpu.SemaphoreType.DMA((23,)),
        ],
        compiler_params=pltpu.CompilerParams(collective_id=layer, has_side_effects=True, vmem_limit_bytes=67043328),
    )(o, x, nw, wo, wg, wu, wd)


def solution(mesh):
    row_spec = P('dp', None)
    pos_spec = P('dp')
    cache_spec = P(None, 'dp', None, 'tp', None)
    norm_spec = P(None, None)
    col_spec = P(None, None, 'tp')
    split_rows = P(None, 'tp', None)

    def local_step(hidden, positions, k_cache, v_cache, attn_norm, w_query, w_key, w_value, w_out, mlp_norm, w_gate, w_up, w_down):
        cos, sin = rope_tables(positions)
        kc = k_cache.reshape(2, B, S, HD)
        vc = v_cache.reshape(2, B, S, HD)
        x = hidden
        prev = None
        for layer in range(2):
            o, ko, vo = attn_call(layer, positions, x, attn_norm[layer][None, :], cos, sin, w_query, w_key, w_value, kc, vc, prev)
            prev = (ko, vo)
            x = mlp_call(layer, o, x, mlp_norm[layer][None, :], w_out, w_gate, w_up, w_down)
        return x, prev[0].reshape(k_cache.shape), prev[1].reshape(v_cache.shape)

    return jax.shard_map(local_step, mesh=mesh, in_specs=(row_spec, pos_spec, cache_spec, cache_spec, norm_spec, col_spec, col_spec, col_spec, split_rows, norm_spec, col_spec, col_spec, split_rows), out_specs=(row_spec, cache_spec, cache_spec), check_vma=False)
```

```python
import functools
import math
import jax
import jax.numpy as jnp
from jax import lax
from jax.experimental import pallas as pl
from jax.experimental.pallas import tpu as pltpu
from jax.sharding import PartitionSpec as P

MESH = pl.DeviceIdType.MESH
F32 = jnp.float32
BF16 = jnp.bfloat16
ANY = pl.BlockSpec(memory_space=pl.ANY)
VMEM = pl.BlockSpec(memory_space=pltpu.VMEM)
SMEM = pl.BlockSpec(memory_space=pltpu.SMEM)

B = 256
D = 4096
S = 128
HD = 128
G = 4
QW = G * HD
NP = 8
PW = D // NP
FW = 1792
HB = B // 2
PH = PW // 2
NC = 23

CB = 32
NCH = B // CB
NS = 5
PF = 3


def rope_tables(shape):
    half = HD // 2
    lane = lax.broadcasted_iota(jnp.int32, shape, 1)
    index = jnp.where(lane < half, lane, lane - half).astype(F32)
    inv_freq = jnp.exp(index * (-2.0 / HD * math.log(500000.0)))
    wavelen = (2.0 * math.pi) / inv_freq
    smooth = (8192.0 / wavelen - 1.0) / 3.0
    blended = (1.0 - smooth) * inv_freq / 8.0 + smooth * inv_freq
    scaled = jnp.where(wavelen < 2048.0, inv_freq, jnp.where(wavelen > 8192.0, inv_freq / 8.0, blended))
    angles = lax.broadcasted_iota(jnp.int32, shape, 0).astype(F32) * scaled
    return jnp.cos(angles), jnp.where(lane < half, -1.0, 1.0) * jnp.sin(angles)


def norm_rows(x_ref, h_ref, w_ref, layer, rows=32):
    def step(i, carry):
        sl = pl.ds(pl.multiple_of(i * rows, rows), rows)
        acc = jnp.zeros((rows, 128), F32)
        for c in range(D // 128):
            t = x_ref[sl, c * 128:(c + 1) * 128].astype(F32)
            acc = acc + t * t
        r = lax.rsqrt(jnp.sum(acc, axis=1, keepdims=True) * (1.0 / D) + 1e-5)
        for c in range(D // 512):
            cs = slice(c * 512, (c + 1) * 512)
            h_ref[sl, cs] = (x_ref[sl, cs].astype(F32) * r * w_ref[layer:layer + 1, cs].astype(F32)).astype(BF16)
        return carry
    lax.fori_loop(0, B // rows, step, 0, unroll=2)


def attn_kernel(layer, first, pos_ref, x_hbm, nw_ref, wq_hbm, wk_hbm, wv_hbm, kc_hbm, vc_hbm, *rest):
    if first:
        o_ref, ko_hbm, vo_hbm = rest[:3]
        rest = rest[3:]
    else:
        o_ref, ko_hbm, vo_hbm = rest[2:5]
        rest = rest[5:]
    x_v, h_v, cos_t, sin_t, cos_ref, sin_ref, wq_v, wk_v, wv_v, acc, q4, o4, kn, vn, rid, kb, vb, wsem, xsem, ksem, vsem, kosem, vosem = rest

    def kv_in(c, slot):
        rs = pl.ds(c * CB, CB)
        return (pltpu.make_async_copy(kc_hbm.at[layer, rs], kb.at[slot], ksem.at[slot]),
                pltpu.make_async_copy(vc_hbm.at[layer, rs], vb.at[slot], vsem.at[slot]))

    def kv_out(c, slot):
        rs = pl.ds(c * CB, CB)
        return (pltpu.make_async_copy(kb.at[slot], ko_hbm.at[layer, rs], kosem.at[slot]),
                pltpu.make_async_copy(vb.at[slot], vo_hbm.at[layer, rs], vosem.at[slot]))

    xcopy = pltpu.make_async_copy(x_hbm, x_v, xsem)
    xcopy.start()
    KC = D // 4
    wcopies = []
    for c in range(4):
        rs = pl.ds(c * KC, KC)
        cs = [pltpu.make_async_copy(wq_hbm.at[layer, rs], wq_v.at[rs], wsem.at[c, 0]),
              pltpu.make_async_copy(wk_hbm.at[layer, rs], wk_v.at[rs], wsem.at[c, 1]),
              pltpu.make_async_copy(wv_hbm.at[layer, rs], wv_v.at[rs], wsem.at[c, 2])]
        for t in cs:
            t.start()
        wcopies.append(cs)
    for c in range(PF):
        for t in kv_in(c, c):
            t.start()

    rid[...] = lax.broadcasted_iota(jnp.int32, (S, HD), 0).astype(F32).astype(BF16)
    cos_t[...], sin_t[...] = rope_tables((S, HD))

    def look_up(b, carry):
        p = pos_ref[b]
        cos_ref[pl.ds(b, 1), :] = cos_t[pl.ds(p, 1), :]
        sin_ref[pl.ds(b, 1), :] = sin_t[pl.ds(p, 1), :]
        return carry

    lax.fori_loop(0, B, look_up, 0, unroll=8)
    xcopy.wait()
    norm_rows(x_v, h_v, nw_ref, layer)
    for c in range(4):
        for t in wcopies[c]:
            t.wait()
        rs = slice(c * KC, (c + 1) * KC)
        w = jnp.concatenate([wq_v[rs, :], wk_v[rs, :], wv_v[rs, :]], axis=1)
        r = jnp.dot(h_v[:, rs], w, preferred_element_type=F32)
        if c == 0:
            acc[...] = r
        else:
            acc[...] += r

    cos = cos_ref[...]
    sin = sin_ref[...]

    def rope(t):
        t = t.astype(BF16).astype(F32)
        return (t * cos + pltpu.roll(t, HD // 2, 1) * sin).astype(BF16).astype(F32)

    for hd in range(G):
        q4[pl.ds(hd, B, stride=G), :] = rope(acc[:, hd * HD:(hd + 1) * HD])
    kn[...] = rope(acc[:, QW:QW + HD])
    vn[...] = acc[:, QW + HD:QW + 2 * HD].astype(BF16).astype(F32)

    scale = HD ** -0.5
    row = lax.broadcasted_iota(jnp.int32, (4 * G, HD), 0) // G
    lane = lax.broadcasted_iota(jnp.int32, (CB * G, HD), 1)
    even = (row % 2) == 0
    low = row < 2

    def place(buf, new, slot, b0, i, rowid):
        hit = rowid == jnp.full((S, HD), pos_ref[b0 + i].astype(F32), F32).astype(BF16)
        r = jnp.broadcast_to(new[pl.ds(b0 + i, 1), :], (S, HD)).astype(BF16)
        t = jnp.where(hit, r, buf[slot, i])
        buf[slot, i] = t
        return t

    def quad(ts):
        return jnp.concatenate([jnp.concatenate(ts[:2], axis=1), jnp.concatenate(ts[2:], axis=1)], axis=0)

    def scores(c):
        slot = c % NS
        b0 = c * CB
        kv_in(c, slot)[0].wait()
        rowid = rid[...]
        out = []
        for g in range(CB // 4):
            kt = quad([place(kb, kn, slot, b0, 4 * g + i, rowid) for i in range(4)])
            q = q4[pl.ds(pl.multiple_of(b0 * G + 4 * G * g, 4 * G), 4 * G), :]
            lhs = jnp.concatenate([jnp.where(even, q, 0.0), jnp.where(even, 0.0, q)], axis=1).astype(BF16)
            s2 = lax.dot_general(lhs, kt, (((1,), (1,)), ((), ())), preferred_element_type=F32)
            out.append(jnp.where(low, s2[:, :S], s2[:, S:]))
        return jnp.concatenate(out, axis=0)

    def values(c, s):
        slot = c % NS
        b0 = c * CB
        kv_in(c, slot)[1].wait()
        rowid = rid[...]
        posr = []
        for g in range(CB // 4):
            t = jnp.zeros((4 * G, HD), jnp.int32)
            for i in range(4):
                t = jnp.where(row == i, pos_ref[b0 + 4 * g + i], t)
            posr.append(t)
        s = jnp.where(lane <= jnp.concatenate(posr, axis=0), s * scale, -jnp.inf)
        e = jnp.exp(s - jnp.max(s, axis=1, keepdims=True))
        p = e / jnp.sum(e, axis=1, keepdims=True)
        for g in range(CB // 4):
            vt = quad([place(vb, vn, slot, b0, 4 * g + i, rowid) for i in range(4)])
            pg = p[4 * G * g:4 * G * (g + 1)]
            lhs = jnp.concatenate([jnp.where(low, pg, 0.0), jnp.where(low, 0.0, pg)], axis=1).astype(BF16)
            o2 = jnp.dot(lhs, vt, preferred_element_type=F32)
            o4[pl.ds(pl.multiple_of(b0 * G + 4 * G * g, 4 * G), 4 * G), :] = jnp.where(even, o2[:, :HD], o2[:, HD:])

    def turn(c, j):
        kv_out(c, c % NS)[j].start()
        nxt = c + PF

        @pl.when(nxt < NCH)
        def _():
            @pl.when(nxt >= NS)
            def _():
                kv_out(nxt - NS, nxt % NS)[j].wait()
            kv_in(nxt, nxt % NS)[j].start()

    s0 = scores(0)
    turn(0, 0)

    def chunk(c, s):
        sn = scores(c + 1)
        values(c, s)
        turn(c + 1, 0)
        turn(c, 1)
        return sn

    sl = lax.fori_loop(0, NCH - 1, chunk, s0)
    values(NCH - 1, sl)
    turn(NCH - 1, 1)
    for hd in range(G):
        o_ref[:, hd * HD:(hd + 1) * HD] = o4[pl.ds(hd, B, stride=G), :].astype(BF16)
    for c in range(NCH - NS, NCH):
        for t in kv_out(c, c % NS):
            t.wait()


def attn_call(layer, pos, x, nw, wq, wk, wv, kc, vc, prev):
    first = prev is None
    cache = jax.ShapeDtypeStruct(kc.shape, BF16)
    ins = [pos, x, nw, wq, wk, wv, kc, vc]
    specs = [SMEM, ANY, VMEM] + [ANY] * 5
    alias = {}
    if not first:
        alias = {len(ins): 1, len(ins) + 1: 2}
        ins += list(prev)
        specs += [ANY, ANY]
    return pl.pallas_call(
        functools.partial(attn_kernel, layer, first),
        name=f"attn{layer}",
        out_shape=(jax.ShapeDtypeStruct((B, QW), BF16), cache, cache),
        in_specs=specs,
        out_specs=(VMEM, ANY, ANY),
        scratch_shapes=[
            pltpu.VMEM((B, D), BF16),
            pltpu.VMEM((B, D), BF16),
            pltpu.VMEM((S, HD), F32),
            pltpu.VMEM((S, HD), F32),
            pltpu.VMEM((B, HD), F32),
            pltpu.VMEM((B, HD), F32),
            pltpu.VMEM((D, QW), BF16),
            pltpu.VMEM((D, HD), BF16),
            pltpu.VMEM((D, HD), BF16),
            pltpu.VMEM((B, QW + 2 * HD), F32),
            pltpu.VMEM((B * G, HD), F32),
            pltpu.VMEM((B * G, HD), F32),
            pltpu.VMEM((B, HD), F32),
            pltpu.VMEM((B, HD), F32),
            pltpu.VMEM((S, HD), BF16),
            pltpu.VMEM((NS, CB, S, HD), BF16),
            pltpu.VMEM((NS, CB, S, HD), BF16),
            pltpu.SemaphoreType.DMA((4, 3)),
            pltpu.SemaphoreType.DMA,
            pltpu.SemaphoreType.DMA((NS,)),
            pltpu.SemaphoreType.DMA((NS,)),
            pltpu.SemaphoreType.DMA((NS,)),
            pltpu.SemaphoreType.DMA((NS,)),
        ],
        input_output_aliases=alias,
        compiler_params=pltpu.CompilerParams(vmem_limit_bytes=60 * 2 ** 20),
    )(*ins)


def mlp_kernel(layer, o_ref, x_hbm, nw_ref, wo_hbm, wg_hbm, wu_hbm, wd_hbm, xo_hbm,
               wo_v, wg_v, wu_v, wd_v, part, xg, hc, acc, a_v, xown, d2d, r1, r2, ssb, r_v,
               wsem, osem, xsem, ssem, rsem):
    me = lax.axis_index("tp")
    k = me % 2
    cx = (me // 2) % 2
    cy = me // 4
    pt = me + 1 - 2 * k
    xn = me + 2 - 4 * cx
    yn = me + 4 - 8 * cy
    dg = xn + 4 - 8 * cy

    def other(p):
        return p + 1 - 2 * k

    peers = (pt, xn, yn, dg, other(xn), other(yn), other(dg))
    order = (dg, xn, yn, me)
    top = pl.ds(0, HB)
    bot = pl.ds(HB, HB)

    def cols(p, h):
        return pl.ds(pl.multiple_of(p * PW + h * PH, PH), PH)

    def chip_cols(p):
        return pl.ds(pl.multiple_of((p // 2) * 2 * PW, 2 * PW), 2 * PW)

    barrier = pltpu.get_barrier_semaphore()
    for d in peers:
        pl.semaphore_signal(barrier, inc=1, device_id={"tp": d}, device_id_type=MESH)

    wos = [pltpu.make_async_copy(wo_hbm.at[layer, :, chip_cols(p)], wo_v.at[:, chip_cols(p)], osem.at[i]) for i, p in enumerate(order)]
    xcs = [pltpu.make_async_copy(x_hbm.at[:, cols(me, h)], xown.at[h], xsem.at[h]) for h in range(2)]
    NG = 4
    gus = []
    for i in range(NG):
        rs = pl.ds(i * (D // NG), D // NG)
        gus.append(pltpu.make_async_copy(wg_hbm.at[layer, rs], wg_v.at[rs], wsem.at[2 * i]))
        gus.append(pltpu.make_async_copy(wu_hbm.at[layer, rs], wu_v.at[rs], wsem.at[2 * i + 1]))
    ND = 4
    wds = []
    for i in range(ND):
        rs = pl.ds(i * (FW // ND), FW // ND)
        wds.append(pltpu.make_async_copy(wd_hbm.at[layer, rs], wd_v.at[rs], wsem.at[2 * NG + i]))
    for t in wos + xcs + gus + wds:
        t.start()
    pl.semaphore_wait(barrier, len(peers))

    def send(src, dst, i, dev):
        c = pltpu.make_async_remote_copy(src_ref=src, dst_ref=dst, send_sem=ssem.at[i], recv_sem=rsem.at[i],
                                         device_id={"tp": dev}, device_id_type=MESH)
        c.start()
        return c

    def reduce_scatter(make):
        live = [{}, {}]

        def pair(h, t):
            c = live[h]
            p = order[t]
            c["d%d" % t].wait_recv()
            part[h, p] = (part[h, p].astype(F32) + d2d[h, t].astype(F32)).astype(BF16)
            if t == 0:
                c["a0"] = send(part.at[h, dg, top], r1.at[h, 0], NC * h + 4, xn)
                c["b0"] = send(part.at[h, dg, bot], r1.at[h, 2], NC * h + 5, yn)
            elif t == 1:
                c["a1"] = send(part.at[h, xn, top], r1.at[h, 1], NC * h + 6, xn)
            elif t == 2:
                c["b1"] = send(part.at[h, yn, bot], r1.at[h, 3], NC * h + 7, yn)

        todo = []
        for h in range(2):
            for t, p in enumerate(order):
                q = other(p)
                make(h, t, p, q)
                live[h]["d%d" % t] = send(part.at[h, q], d2d.at[h, t], NC * h + t, pt)
                if todo:
                    pair(*todo.pop(0))
                todo.append((h, t))
        pair(*todo.pop(0))
        for h in range(2):
            c = live[h]
            c["a0"].wait_recv()
            part[h, yn, top] = (part[h, yn, top].astype(F32) + r1[h, 0].astype(F32)).astype(BF16)
            c["a2"] = send(part.at[h, yn, top], r2.at[h, 0], NC * h + 8, yn)
            c["b0"].wait_recv()
            part[h, xn, bot] = (part[h, xn, bot].astype(F32) + r1[h, 2].astype(F32)).astype(BF16)
            c["b2"] = send(part.at[h, xn, bot], r2.at[h, 1], NC * h + 9, xn)
        return live

    def final(h, c):
        for rs, a, b, i, j in ((top, "a1", "a2", 1, 0), (bot, "b1", "b2", 3, 1)):
            c[a].wait_recv()
            c[b].wait_recv()
            tot = part[h, me, rs].astype(F32) + r1[h, i].astype(F32) + r2[h, j].astype(F32)
            new = (xown[h, rs].astype(F32) + tot.astype(BF16).astype(F32)).astype(BF16)
            xown[h, rs] = new
            xg[h, me, rs] = new

    def gather_start(h, c):
        def go(name, p, rs, i, dev):
            c[name] = send(xg.at[h, p, rs], xg.at[h, p, rs], NC * h + i, dev)
        go("ga0", me, top, 10, yn)
        go("gb0", me, bot, 11, xn)
        go("ga1", me, top, 12, xn)
        go("gb1", me, bot, 13, yn)
        c["p0"] = send(xg.at[h, me], xg.at[h, me], NC * h + 14, pt)

    def forward(h, c, got, name, p, rs, i):
        c[got].wait_recv()
        c[name] = send(xg.at[h, p, rs], xg.at[h, p, rs], NC * h + i, pt)

    def relay(h, c):
        forward(h, c, "ga0", "p1", yn, top, 15)
        c["ga2"] = send(xg.at[h, yn, top], xg.at[h, yn, top], NC * h + 16, xn)
        forward(h, c, "gb0", "p2", xn, bot, 17)
        c["gb2"] = send(xg.at[h, xn, bot], xg.at[h, xn, bot], NC * h + 18, yn)

    def near(h, c):
        forward(h, c, "ga1", "p3", xn, top, 19)
        forward(h, c, "gb1", "p4", yn, bot, 20)

    def far(h, c):
        forward(h, c, "ga2", "p5", dg, top, 21)
        forward(h, c, "gb2", "p6", dg, bot, 22)

    def drain(live):
        for c in live:
            for t in c.values():
                t.wait_send()

    def got(live, *names):
        for c in live:
            for n in names:
                c[n].wait_recv()

    def out_half(h, i, p, q):
        if h == 0:
            wos[i].wait()
        w = jnp.concatenate([wo_v[:, cols(p, h)], wo_v[:, cols(q, h)]], axis=1)
        t = jnp.dot(o_ref[...], w, preferred_element_type=F32).astype(BF16)
        part[h, p] = t[:, :PH]
        part[h, q] = t[:, PH:]

    live = reduce_scatter(out_half)
    for t in xcs:
        t.wait()
    final(0, live[0])
    gather_start(0, live[0])
    final(1, live[1])
    sq = jnp.zeros((B, 128), F32)
    for h in range(2):
        for c in range(PH // 128):
            t = xg[h, me, :, c * 128:(c + 1) * 128].astype(F32)
            sq = sq + t * t
    ssb[0] = jnp.broadcast_to(jnp.sum(sq.T, axis=0, keepdims=True), (8, B))
    sss = [send(ssb.at[0], ssb.at[1 + j], 2 * NC + j, d) for j, d in enumerate(peers)]
    gather_start(1, live[1])
    relay(0, live[0])
    for t in sss:
        t.wait_recv()
    tot = ssb[0]
    for j in range(len(peers)):
        tot = tot + ssb[1 + j]
    rr = lax.rsqrt(tot * (1.0 / D) + 1e-5)
    r_v[...] = jnp.broadcast_to(rr[0:1], (128, B)).T
    relay(1, live[1])
    for h in range(2):
        near(h, live[h])
    for t in gus:
        t.wait()

    TN = 256

    def gate_up(p, first, last):
        base = pl.multiple_of((p // 2) * 2 * PW, 2 * PW)

        def norm_step(i, carry):
            sl = pl.ds(pl.multiple_of(i * 64, 64), 64)
            r = r_v[sl, :]
            for c in range(2 * PW // 128):
                cs = slice(c * 128, (c + 1) * 128)
                e, h, o = c // 4, (c // 2) % 2, (c % 2) * 128
                w = nw_ref[layer:layer + 1, pl.ds(pl.multiple_of(base + c * 128, 128), 128)].astype(F32)
                hc[sl, cs] = (xg[h, (p // 2) * 2 + e, sl, o:o + 128].astype(F32) * r * w).astype(BF16)
            return carry

        lax.fori_loop(0, B // 64, norm_step, 0)

        def tile(j, carry):
            cs = pl.ds(pl.multiple_of(j * TN, TN), TN)
            ks = pl.ds(base, 2 * PW)
            w = jnp.concatenate([wg_v[ks, cs], wu_v[ks, cs]], axis=1)
            gu = jnp.dot(hc[...], w, preferred_element_type=F32)
            if not first:
                gu = gu + acc[j]
            if not last:
                acc[j] = gu
            else:
                gt = gu[:, :TN].astype(BF16).astype(F32)
                up = gu[:, TN:].astype(BF16).astype(F32)
                a_v[:, cs] = (gt * (1.0 / (1.0 + jnp.exp(-gt))) * up).astype(BF16)
            return carry

        lax.fori_loop(0, FW // TN, tile, 0)

    got(live, "p0")
    gate_up(me, True, False)
    got(live, "p2", "p3")
    gate_up(xn, False, False)
    for h in range(2):
        far(h, live[h])
    got(live, "p1", "p4")
    gate_up(yn, False, False)
    got(live, "p5", "p6")
    gate_up(dg, False, True)
    drain(live)
    for t in sss:
        t.wait_send()
    for t in wds:
        t.wait()

    def down_half(h, i, p, q):
        w = jnp.concatenate([wd_v[:, cols(p, h)], wd_v[:, cols(q, h)]], axis=1)
        t = jnp.dot(a_v[...], w, preferred_element_type=F32).astype(BF16)
        part[h, p] = t[:, :PH]
        part[h, q] = t[:, PH:]

    live = reduce_scatter(down_half)
    for h in range(2):
        final(h, live[h])
        gather_start(h, live[h])
    for h in range(2):
        relay(h, live[h])
    for h in range(2):
        near(h, live[h])
    outs = []

    def write(p):
        for e in range(2):
            for h in range(2):
                n = (p // 2) * 2 + e
                c = pltpu.make_async_copy(xg.at[h, n], xo_hbm.at[:, cols(n, h)], wsem.at[len(outs)])
                c.start()
                outs.append(c)

    got(live, "p0")
    write(me)
    for h in range(2):
        far(h, live[h])
    got(live, "p2", "p3")
    write(xn)
    got(live, "p1", "p4")
    write(yn)
    got(live, "p5", "p6")
    write(dg)
    drain(live)
    for c in outs:
        c.wait()


def mlp_call(layer, o, x, nw, wo, wg, wu, wd):
    return pl.pallas_call(
        functools.partial(mlp_kernel, layer),
        name=f"mlp{layer}",
        out_shape=jax.ShapeDtypeStruct((B, D), BF16),
        in_specs=[VMEM, ANY, VMEM, ANY, ANY, ANY, ANY],
        out_specs=ANY,
        scratch_shapes=[
            pltpu.VMEM((QW, D), BF16),
            pltpu.VMEM((D, FW), BF16),
            pltpu.VMEM((D, FW), BF16),
            pltpu.VMEM((FW, D), BF16),
            pltpu.VMEM((2, NP, B, PH), BF16),
            pltpu.VMEM((2, NP, B, PH), BF16),
            pltpu.VMEM((B, 2 * PW), BF16),
            pltpu.VMEM((FW // 256, B, 512), F32),
            pltpu.VMEM((B, FW), BF16),
            pltpu.VMEM((2, B, PH), BF16),
            pltpu.VMEM((2, 4, B, PH), BF16),
            pltpu.VMEM((2, 4, HB, PH), BF16),
            pltpu.VMEM((2, 2, HB, PH), BF16),
            pltpu.VMEM((8, 8, B), F32),
            pltpu.VMEM((B, 128), F32),
            pltpu.SemaphoreType.DMA((16,)),
            pltpu.SemaphoreType.DMA((4,)),
            pltpu.SemaphoreType.DMA((2,)),
            pltpu.SemaphoreType.DMA((2 * NC + 7,)),
            pltpu.SemaphoreType.DMA((2 * NC + 7,)),
        ],
        compiler_params=pltpu.CompilerParams(collective_id=layer, has_side_effects=True, vmem_limit_bytes=67043328),
    )(o, x, nw, wo, wg, wu, wd)


def solution(mesh):
    row_spec = P('dp', None)
    pos_spec = P('dp')
    cache_spec = P(None, 'dp', None, 'tp', None)
    norm_spec = P(None, None)
    col_spec = P(None, None, 'tp')
    split_rows = P(None, 'tp', None)

    def local_step(hidden, positions, k_cache, v_cache, attn_norm, w_query, w_key, w_value, w_out, mlp_norm, w_gate, w_up, w_down):
        kc = k_cache.reshape(2, B, S, HD)
        vc = v_cache.reshape(2, B, S, HD)
        x = hidden
        prev = None
        for layer in range(2):
            o, ko, vo = attn_call(layer, positions, x, attn_norm, w_query, w_key, w_value, kc, vc, prev)
            prev = (ko, vo)
            x = mlp_call(layer, o, x, mlp_norm, w_out, w_gate, w_up, w_down)
        return x, prev[0].reshape(k_cache.shape), prev[1].reshape(v_cache.shape)

    return jax.shard_map(local_step, mesh=mesh, in_specs=(row_spec, pos_spec, cache_spec, cache_spec, norm_spec, col_spec, col_spec, col_spec, split_rows, norm_spec, col_spec, col_spec, split_rows), out_specs=(row_spec, cache_spec, cache_spec), check_vma=False)
```

```python
import functools
import math
import jax
import jax.numpy as jnp
from jax import lax
from jax.experimental import pallas as pl
from jax.experimental.pallas import tpu as pltpu
from jax.sharding import PartitionSpec as P

MESH = pl.DeviceIdType.MESH
F32 = jnp.float32
BF16 = jnp.bfloat16
ANY = pl.BlockSpec(memory_space=pl.ANY)
VMEM = pl.BlockSpec(memory_space=pltpu.VMEM)
SMEM = pl.BlockSpec(memory_space=pltpu.SMEM)

B = 256
D = 4096
S = 128
HD = 128
G = 4
QW = G * HD
NP = 8
PW = D // NP
FW = 1792
HB = B // 2
PH = PW // 2
NC = 23
UN = True

CB = 32
NCH = B // CB
NS = 8
PF = 6


def rope_tables(shape):
    half = HD // 2
    lane = lax.broadcasted_iota(jnp.int32, shape, 1)
    index = jnp.where(lane < half, lane, lane - half).astype(F32)
    inv_freq = jnp.exp(index * (-2.0 / HD * math.log(500000.0)))
    wavelen = (2.0 * math.pi) / inv_freq
    smooth = (8192.0 / wavelen - 1.0) / 3.0
    blended = (1.0 - smooth) * inv_freq / 8.0 + smooth * inv_freq
    scaled = jnp.where(wavelen < 2048.0, inv_freq, jnp.where(wavelen > 8192.0, inv_freq / 8.0, blended))
    angles = lax.broadcasted_iota(jnp.int32, shape, 0).astype(F32) * scaled
    return jnp.cos(angles), jnp.where(lane < half, -1.0, 1.0) * jnp.sin(angles)


def norm_rows(x_ref, h_ref, w_ref, layer, rows=32):
    def step(i, carry):
        sl = pl.ds(pl.multiple_of(i * rows, rows), rows)
        acc = jnp.zeros((rows, 128), F32)
        for c in range(D // 128):
            t = x_ref[sl, c * 128:(c + 1) * 128].astype(F32)
            acc = acc + t * t
        r = lax.rsqrt(jnp.sum(acc, axis=1, keepdims=True) * (1.0 / D) + 1e-5)
        for c in range(D // 512):
            cs = slice(c * 512, (c + 1) * 512)
            h_ref[sl, cs] = (x_ref[sl, cs].astype(F32) * r * w_ref[layer:layer + 1, cs].astype(F32)).astype(BF16)
        return carry
    lax.fori_loop(0, B // rows, step, 0, unroll=2)


def attn_kernel(layer, first, pos_ref, x_hbm, nw_ref, wq_hbm, wk_hbm, wv_hbm, kc_hbm, vc_hbm, *rest):
    if first:
        o_ref, ko_hbm, vo_hbm = rest[:3]
        rest = rest[3:]
    else:
        o_ref, ko_hbm, vo_hbm = rest[2:5]
        rest = rest[5:]
    x_v, h_v, cos_t, sin_t, cos_ref, sin_ref, wq_v, wk_v, wv_v, acc, q4, o4, kn, vn, rid, kb, vb, wsem, xsem, ksem, vsem, kosem, vosem = rest

    def kv_in(c, slot):
        rs = pl.ds(c * CB, CB)
        return (pltpu.make_async_copy(kc_hbm.at[layer, rs], kb.at[slot], ksem.at[slot]),
                pltpu.make_async_copy(vc_hbm.at[layer, rs], vb.at[slot], vsem.at[slot]))

    def kv_out(c, slot):
        rs = pl.ds(c * CB, CB)
        return (pltpu.make_async_copy(kb.at[slot], ko_hbm.at[layer, rs], kosem.at[slot]),
                pltpu.make_async_copy(vb.at[slot], vo_hbm.at[layer, rs], vosem.at[slot]))

    xcopy = pltpu.make_async_copy(x_hbm, x_v, xsem)
    xcopy.start()
    KC = D // 4
    wcopies = []
    for c in range(4):
        rs = pl.ds(c * KC, KC)
        cs = [pltpu.make_async_copy(wq_hbm.at[layer, rs], wq_v.at[rs], wsem.at[c, 0]),
              pltpu.make_async_copy(wk_hbm.at[layer, rs], wk_v.at[rs], wsem.at[c, 1]),
              pltpu.make_async_copy(wv_hbm.at[layer, rs], wv_v.at[rs], wsem.at[c, 2])]
        wcopies.append(cs)
    for t in wcopies[0]:
        t.start()

    rid[...] = lax.broadcasted_iota(jnp.int32, (S, HD), 0).astype(F32).astype(BF16)
    cos_t[...], sin_t[...] = rope_tables((S, HD))

    def look_up(b, carry):
        p = pos_ref[b]
        cos_ref[pl.ds(b, 1), :] = cos_t[pl.ds(p, 1), :]
        sin_ref[pl.ds(b, 1), :] = sin_t[pl.ds(p, 1), :]
        return carry

    lax.fori_loop(0, B, look_up, 0, unroll=8)
    xcopy.wait()
    for cs in wcopies[1:]:
        for t in cs:
            t.start()
    norm_rows(x_v, h_v, nw_ref, layer)
    for c in range(PF):
        for t in kv_in(c, c):
            t.start()
    for c in range(4):
        for t in wcopies[c]:
            t.wait()
        rs = slice(c * KC, (c + 1) * KC)
        w = jnp.concatenate([wq_v[rs, :], wk_v[rs, :], wv_v[rs, :]], axis=1)
        r = jnp.dot(h_v[:, rs], w, preferred_element_type=F32)
        if c == 0:
            acc[...] = r
        else:
            acc[...] += r

    cos = cos_ref[...]
    sin = sin_ref[...]

    def rope(t):
        t = t.astype(BF16).astype(F32)
        return (t * cos + pltpu.roll(t, HD // 2, 1) * sin).astype(BF16).astype(F32)

    for hd in range(G):
        q4[pl.ds(hd, B, stride=G), :] = rope(acc[:, hd * HD:(hd + 1) * HD])
    kn[...] = rope(acc[:, QW:QW + HD])
    vn[...] = acc[:, QW + HD:QW + 2 * HD].astype(BF16).astype(F32)

    scale = HD ** -0.5
    row = lax.broadcasted_iota(jnp.int32, (4 * G, HD), 0) // G
    lane = lax.broadcasted_iota(jnp.int32, (CB * G, HD), 1)
    even = (row % 2) == 0
    low = row < 2

    def place(buf, new, slot, b0, i, rowid):
        hit = rowid == jnp.full((S, HD), pos_ref[b0 + i].astype(F32), F32).astype(BF16)
        r = jnp.broadcast_to(new[pl.ds(b0 + i, 1), :], (S, HD)).astype(BF16)
        t = jnp.where(hit, r, buf[slot, i])
        buf[slot, i] = t
        return t

    def quad(ts):
        return jnp.concatenate([jnp.concatenate(ts[:2], axis=1), jnp.concatenate(ts[2:], axis=1)], axis=0)

    def scores(c):
        slot = c % NS
        b0 = c * CB
        kv_in(c, slot)[0].wait()
        rowid = rid[...]
        out = []
        for g in range(CB // 4):
            kt = quad([place(kb, kn, slot, b0, 4 * g + i, rowid) for i in range(4)])
            q = q4[pl.ds(pl.multiple_of(b0 * G + 4 * G * g, 4 * G), 4 * G), :]
            lhs = jnp.concatenate([jnp.where(even, q, 0.0), jnp.where(even, 0.0, q)], axis=1).astype(BF16)
            s2 = lax.dot_general(lhs, kt, (((1,), (1,)), ((), ())), preferred_element_type=F32)
            out.append(jnp.where(low, s2[:, :S], s2[:, S:]))
        return jnp.concatenate(out, axis=0)

    def values(c, s):
        slot = c % NS
        b0 = c * CB
        kv_in(c, slot)[1].wait()
        rowid = rid[...]
        posr = []
        for g in range(CB // 4):
            t = jnp.zeros((4 * G, HD), jnp.int32)
            for i in range(4):
                t = jnp.where(row == i, pos_ref[b0 + 4 * g + i], t)
            posr.append(t)
        s = jnp.where(lane <= jnp.concatenate(posr, axis=0), s * scale, -jnp.inf)
        e = jnp.exp(s - jnp.max(s, axis=1, keepdims=True))
        p = e / jnp.sum(e, axis=1, keepdims=True)
        for g in range(CB // 4):
            vt = quad([place(vb, vn, slot, b0, 4 * g + i, rowid) for i in range(4)])
            pg = p[4 * G * g:4 * G * (g + 1)]
            lhs = jnp.concatenate([jnp.where(low, pg, 0.0), jnp.where(low, 0.0, pg)], axis=1).astype(BF16)
            o2 = jnp.dot(lhs, vt, preferred_element_type=F32)
            o4[pl.ds(pl.multiple_of(b0 * G + 4 * G * g, 4 * G), 4 * G), :] = jnp.where(even, o2[:, :HD], o2[:, HD:])

    def turn(c, j):
        kv_out(c, c % NS)[j].start()
        nxt = c + PF

        @pl.when(nxt < NCH)
        def _():
            @pl.when(nxt >= NS)
            def _():
                kv_out(nxt - NS, nxt % NS)[j].wait()
            kv_in(nxt, nxt % NS)[j].start()

    s0 = scores(0)
    turn(0, 0)

    def chunk(c, s):
        sn = scores(c + 1)
        values(c, s)
        turn(c + 1, 0)
        turn(c, 1)
        return sn

    sl = lax.fori_loop(0, NCH - 1, chunk, s0)
    values(NCH - 1, sl)
    turn(NCH - 1, 1)
    for hd in range(G):
        o_ref[:, hd * HD:(hd + 1) * HD] = o4[pl.ds(hd, B, stride=G), :].astype(BF16)
    for c in range(NCH - NS, NCH):
        for t in kv_out(c, c % NS):
            t.wait()


def attn_call(layer, pos, x, nw, wq, wk, wv, kc, vc, prev):
    first = prev is None
    cache = jax.ShapeDtypeStruct(kc.shape, BF16)
    ins = [pos, x, nw, wq, wk, wv, kc, vc]
    specs = [SMEM, ANY, VMEM] + [ANY] * 5
    alias = {}
    if not first:
        alias = {len(ins): 1, len(ins) + 1: 2}
        ins += list(prev)
        specs += [ANY, ANY]
    return pl.pallas_call(
        functools.partial(attn_kernel, layer, first),
        name=f"attn{layer}",
        out_shape=(jax.ShapeDtypeStruct((B, QW), BF16), cache, cache),
        in_specs=specs,
        out_specs=(VMEM, ANY, ANY),
        scratch_shapes=[
            pltpu.VMEM((B, D), BF16),
            pltpu.VMEM((B, D), BF16),
            pltpu.VMEM((S, HD), F32),
            pltpu.VMEM((S, HD), F32),
            pltpu.VMEM((B, HD), F32),
            pltpu.VMEM((B, HD), F32),
            pltpu.VMEM((D, QW), BF16),
            pltpu.VMEM((D, HD), BF16),
            pltpu.VMEM((D, HD), BF16),
            pltpu.VMEM((B, QW + 2 * HD), F32),
            pltpu.VMEM((B * G, HD), F32),
            pltpu.VMEM((B * G, HD), F32),
            pltpu.VMEM((B, HD), F32),
            pltpu.VMEM((B, HD), F32),
            pltpu.VMEM((S, HD), BF16),
            pltpu.VMEM((NS, CB, S, HD), BF16),
            pltpu.VMEM((NS, CB, S, HD), BF16),
            pltpu.SemaphoreType.DMA((4, 3)),
            pltpu.SemaphoreType.DMA,
            pltpu.SemaphoreType.DMA((NS,)),
            pltpu.SemaphoreType.DMA((NS,)),
            pltpu.SemaphoreType.DMA((NS,)),
            pltpu.SemaphoreType.DMA((NS,)),
        ],
        input_output_aliases=alias,
        compiler_params=pltpu.CompilerParams(vmem_limit_bytes=40 * 2 ** 20),
    )(*ins)


def mlp_kernel(layer, o_ref, x_hbm, nw_ref, wo_hbm, wg_hbm, wu_hbm, wd_hbm, xo_hbm,
               wo_v, wg_v, wu_v, wd_v, part, xg, hc, acc, a_v, xown, d2d, r1, r2, ssb, r_v,
               wsem, osem, xsem, ssem, rsem):
    me = lax.axis_index("tp")
    k = me % 2
    cx = (me // 2) % 2
    cy = me // 4
    pt = me + 1 - 2 * k
    xn = me + 2 - 4 * cx
    yn = me + 4 - 8 * cy
    dg = xn + 4 - 8 * cy

    def other(p):
        return p + 1 - 2 * k

    peers = (pt, xn, yn, dg, other(xn), other(yn), other(dg))
    order = (dg, xn, yn, me)
    top = pl.ds(0, HB)
    bot = pl.ds(HB, HB)

    def cols(p, h):
        return pl.ds(pl.multiple_of(p * PW + h * PH, PH), PH)

    def chip_cols(p):
        return pl.ds(pl.multiple_of((p // 2) * 2 * PW, 2 * PW), 2 * PW)

    barrier = pltpu.get_barrier_semaphore()
    for d in peers:
        pl.semaphore_signal(barrier, inc=1, device_id={"tp": d}, device_id_type=MESH)

    wos = [pltpu.make_async_copy(wo_hbm.at[layer, :, chip_cols(p)], wo_v.at[:, chip_cols(p)], osem.at[i]) for i, p in enumerate(order)]
    xcs = [pltpu.make_async_copy(x_hbm.at[:, cols(me, h)], xown.at[h], xsem.at[h]) for h in range(2)]
    NG = 4
    gus = []
    for i in range(NG):
        rs = pl.ds(i * (D // NG), D // NG)
        gus.append(pltpu.make_async_copy(wg_hbm.at[layer, rs], wg_v.at[rs], wsem.at[2 * i]))
        gus.append(pltpu.make_async_copy(wu_hbm.at[layer, rs], wu_v.at[rs], wsem.at[2 * i + 1]))
    ND = 4
    wds = []
    for i in range(ND):
        rs = pl.ds(i * (FW // ND), FW // ND)
        wds.append(pltpu.make_async_copy(wd_hbm.at[layer, rs], wd_v.at[rs], wsem.at[2 * NG + i]))
    for t in wos + xcs:
        t.start()

    def send(src, dst, i, dev):
        c = pltpu.make_async_remote_copy(src_ref=src, dst_ref=dst, send_sem=ssem.at[i], recv_sem=rsem.at[i],
                                         device_id={"tp": dev}, device_id_type=MESH)
        c.start()
        return c

    def reduce_scatter(make, enter=False):
        live = [{}, {}]

        def pair(h, t):
            c = live[h]
            p = order[t]
            c["d%d" % t].wait_recv()
            part[h, p] = (part[h, p].astype(F32) + d2d[h, t].astype(F32)).astype(BF16)
            if t == 0:
                c["a0"] = send(part.at[h, dg, top], r1.at[h, 0], NC * h + 4, xn)
                c["b0"] = send(part.at[h, dg, bot], r1.at[h, 2], NC * h + 5, yn)
            elif t == 1:
                c["a1"] = send(part.at[h, xn, top], r1.at[h, 1], NC * h + 6, xn)
            elif t == 2:
                c["b1"] = send(part.at[h, yn, bot], r1.at[h, 3], NC * h + 7, yn)

        todo = []
        for h in range(2):
            for t, p in enumerate(order):
                q = other(p)
                make(h, t, p, q)
                if enter and (h, t) == (0, 0):
                    pl.semaphore_wait(barrier, len(peers))
                live[h]["d%d" % t] = send(part.at[h, q], d2d.at[h, t], NC * h + t, pt)
                if todo:
                    pair(*todo.pop(0))
                todo.append((h, t))
        pair(*todo.pop(0))
        for h in range(2):
            c = live[h]
            c["a0"].wait_recv()
            part[h, yn, top] = (part[h, yn, top].astype(F32) + r1[h, 0].astype(F32)).astype(BF16)
            c["a2"] = send(part.at[h, yn, top], r2.at[h, 0], NC * h + 8, yn)
            c["b0"].wait_recv()
            part[h, xn, bot] = (part[h, xn, bot].astype(F32) + r1[h, 2].astype(F32)).astype(BF16)
            c["b2"] = send(part.at[h, xn, bot], r2.at[h, 1], NC * h + 9, xn)
        return live

    def final(h, c):
        for rs, a, b, i, j in ((top, "a1", "a2", 1, 0), (bot, "b1", "b2", 3, 1)):
            c[a].wait_recv()
            c[b].wait_recv()
            tot = part[h, me, rs].astype(F32) + r1[h, i].astype(F32) + r2[h, j].astype(F32)
            new = (xown[h, rs].astype(F32) + tot.astype(BF16).astype(F32)).astype(BF16)
            xown[h, rs] = new
            xg[h, me, rs] = new

    def gather_start(h, c):
        def go(name, p, rs, i, dev):
            c[name] = send(xg.at[h, p, rs], xg.at[h, p, rs], NC * h + i, dev)
        go("ga0", me, top, 10, yn)
        go("gb0", me, bot, 11, xn)
        go("ga1", me, top, 12, xn)
        go("gb1", me, bot, 13, yn)
        c["p0"] = send(xg.at[h, me], xg.at[h, me], NC * h + 14, pt)

    def forward(h, c, got, name, p, rs, i):
        c[got].wait_recv()
        c[name] = send(xg.at[h, p, rs], xg.at[h, p, rs], NC * h + i, pt)

    def relay(h, c):
        forward(h, c, "ga0", "p1", yn, top, 15)
        c["ga2"] = send(xg.at[h, yn, top], xg.at[h, yn, top], NC * h + 16, xn)
        forward(h, c, "gb0", "p2", xn, bot, 17)
        c["gb2"] = send(xg.at[h, xn, bot], xg.at[h, xn, bot], NC * h + 18, yn)

    def near(h, c):
        forward(h, c, "ga1", "p3", xn, top, 19)
        forward(h, c, "gb1", "p4", yn, bot, 20)

    def far(h, c):
        forward(h, c, "ga2", "p5", dg, top, 21)
        forward(h, c, "gb2", "p6", dg, bot, 22)

    def drain(live):
        for c in live:
            for t in c.values():
                t.wait_send()

    def got(live, *names):
        for c in live:
            for n in names:
                c[n].wait_recv()

    def out_half(h, i, p, q):
        if h == 0:
            wos[i].wait()
            if i == 3:
                for t in gus:
                    t.start()
        w = jnp.concatenate([wo_v[:, cols(p, h)], wo_v[:, cols(q, h)]], axis=1)
        t = jnp.dot(o_ref[...], w, preferred_element_type=F32).astype(BF16)
        part[h, p] = t[:, :PH]
        part[h, q] = t[:, PH:]

    live = reduce_scatter(out_half, True)
    for t in xcs:
        t.wait()
    final(0, live[0])
    gather_start(0, live[0])
    final(1, live[1])
    sq = jnp.zeros((B, 128), F32)
    for h in range(2):
        for c in range(PH // 128):
            t = xg[h, me, :, c * 128:(c + 1) * 128].astype(F32)
            sq = sq + t * t
    ssb[0] = jnp.broadcast_to(jnp.sum(sq.T, axis=0, keepdims=True), (8, B))
    sss = [send(ssb.at[0], ssb.at[1 + j], 2 * NC + j, d) for j, d in enumerate(peers)]
    gather_start(1, live[1])
    relay(0, live[0])
    for t in sss:
        t.wait_recv()
    tot = ssb[0]
    for j in range(len(peers)):
        tot = tot + ssb[1 + j]
    rr = lax.rsqrt(tot * (1.0 / D) + 1e-5)
    r_v[...] = jnp.broadcast_to(rr[0:1], (128, B)).T
    for t in gus:
        t.wait()
    for t in wds:
        t.start()

    TN = 256

    def gate_up(p, first, last):
        base = pl.multiple_of((p // 2) * 2 * PW, 2 * PW)

        def norm_step(i, carry):
            sl = pl.ds(pl.multiple_of(i * 64, 64), 64)
            r = r_v[sl, :]
            for c in range(2 * PW // 128):
                cs = slice(c * 128, (c + 1) * 128)
                e, h, o = c // 4, (c // 2) % 2, (c % 2) * 128
                w = nw_ref[layer:layer + 1, pl.ds(pl.multiple_of(base + c * 128, 128), 128)].astype(F32)
                hc[sl, cs] = (xg[h, (p // 2) * 2 + e, sl, o:o + 128].astype(F32) * r * w).astype(BF16)
            return carry

        lax.fori_loop(0, B // 64, norm_step, 0)

        def tile(j, carry):
            cs = pl.ds(pl.multiple_of(j * TN, TN), TN)
            ks = pl.ds(base, 2 * PW)
            w = jnp.concatenate([wg_v[ks, cs], wu_v[ks, cs]], axis=1)
            gu = jnp.dot(hc[...], w, preferred_element_type=F32)
            if not first:
                gu = gu + acc[j]
            if not last:
                acc[j] = gu
            else:
                gt = gu[:, :TN].astype(BF16).astype(F32)
                up = gu[:, TN:].astype(BF16).astype(F32)
                a_v[:, cs] = (gt * (1.0 / (1.0 + jnp.exp(-gt))) * up).astype(BF16)
            return carry

        lax.fori_loop(0, FW // TN, tile, 0, unroll=UN)

    got(live, "p0")
    gate_up(me, True, False)
    relay(1, live[1])
    for h in range(2):
        near(h, live[h])
    got(live, "p2", "p3")
    gate_up(xn, False, False)
    for h in range(2):
        far(h, live[h])
    got(live, "p1", "p4")
    gate_up(yn, False, False)
    got(live, "p5", "p6")
    gate_up(dg, False, True)
    drain(live)
    for t in sss:
        t.wait_send()
    for t in wds:
        t.wait()

    def down_half(h, i, p, q):
        w = jnp.concatenate([wd_v[:, cols(p, h)], wd_v[:, cols(q, h)]], axis=1)
        t = jnp.dot(a_v[...], w, preferred_element_type=F32).astype(BF16)
        part[h, p] = t[:, :PH]
        part[h, q] = t[:, PH:]

    live = reduce_scatter(down_half)
    for h in range(2):
        final(h, live[h])
        gather_start(h, live[h])
    for h in range(2):
        relay(h, live[h])
    for h in range(2):
        near(h, live[h])
    outs = []

    def write(p):
        for e in range(2):
            for h in range(2):
                n = (p // 2) * 2 + e
                c = pltpu.make_async_copy(xg.at[h, n], xo_hbm.at[:, cols(n, h)], wsem.at[len(outs)])
                c.start()
                outs.append(c)

    got(live, "p0")
    write(me)
    for h in range(2):
        far(h, live[h])
    got(live, "p2", "p3")
    write(xn)
    got(live, "p1", "p4")
    write(yn)
    got(live, "p5", "p6")
    write(dg)
    drain(live)
    for c in outs:
        c.wait()


def mlp_call(layer, o, x, nw, wo, wg, wu, wd):
    return pl.pallas_call(
        functools.partial(mlp_kernel, layer),
        name=f"mlp{layer}",
        out_shape=jax.ShapeDtypeStruct((B, D), BF16),
        in_specs=[VMEM, ANY, VMEM, ANY, ANY, ANY, ANY],
        out_specs=ANY,
        scratch_shapes=[
            pltpu.VMEM((QW, D), BF16),
            pltpu.VMEM((D, FW), BF16),
            pltpu.VMEM((D, FW), BF16),
            pltpu.VMEM((FW, D), BF16),
            pltpu.VMEM((2, NP, B, PH), BF16),
            pltpu.VMEM((2, NP, B, PH), BF16),
            pltpu.VMEM((B, 2 * PW), BF16),
            pltpu.VMEM((FW // 256, B, 512), F32),
            pltpu.VMEM((B, FW), BF16),
            pltpu.VMEM((2, B, PH), BF16),
            pltpu.VMEM((2, 4, B, PH), BF16),
            pltpu.VMEM((2, 4, HB, PH), BF16),
            pltpu.VMEM((2, 2, HB, PH), BF16),
            pltpu.VMEM((8, 8, B), F32),
            pltpu.VMEM((B, 128), F32),
            pltpu.SemaphoreType.DMA((16,)),
            pltpu.SemaphoreType.DMA((4,)),
            pltpu.SemaphoreType.DMA((2,)),
            pltpu.SemaphoreType.DMA((2 * NC + 7,)),
            pltpu.SemaphoreType.DMA((2 * NC + 7,)),
        ],
        compiler_params=pltpu.CompilerParams(collective_id=layer, has_side_effects=True, vmem_limit_bytes=67043328),
    )(o, x, nw, wo, wg, wu, wd)


def solution(mesh):
    row_spec = P('dp', None)
    pos_spec = P('dp')
    cache_spec = P(None, 'dp', None, 'tp', None)
    norm_spec = P(None, None)
    col_spec = P(None, None, 'tp')
    split_rows = P(None, 'tp', None)

    def local_step(hidden, positions, k_cache, v_cache, attn_norm, w_query, w_key, w_value, w_out, mlp_norm, w_gate, w_up, w_down):
        kc = k_cache.reshape(2, B, S, HD)
        vc = v_cache.reshape(2, B, S, HD)
        x = hidden
        prev = None
        for layer in range(2):
            o, ko, vo = attn_call(layer, positions, x, attn_norm, w_query, w_key, w_value, kc, vc, prev)
            prev = (ko, vo)
            x = mlp_call(layer, o, x, mlp_norm, w_out, w_gate, w_up, w_down)
        return x, prev[0].reshape(k_cache.shape), prev[1].reshape(v_cache.shape)

    return jax.shard_map(local_step, mesh=mesh, in_specs=(row_spec, pos_spec, cache_spec, cache_spec, norm_spec, col_spec, col_spec, col_spec, split_rows, norm_spec, col_spec, col_spec, split_rows), out_specs=(row_spec, cache_spec, cache_spec), check_vma=False)
```

```python
import functools
import math
import jax
import jax.numpy as jnp
from jax import lax
from jax.experimental import pallas as pl
from jax.experimental.pallas import tpu as pltpu
from jax.sharding import PartitionSpec as P

MESH = pl.DeviceIdType.MESH
F32 = jnp.float32
BF16 = jnp.bfloat16
ANY = pl.BlockSpec(memory_space=pl.ANY)
VMEM = pl.BlockSpec(memory_space=pltpu.VMEM)
SMEM = pl.BlockSpec(memory_space=pltpu.SMEM)

B = 256
D = 4096
S = 128
HD = 128
G = 4
QW = G * HD
NP = 8
PW = D // NP
FW = 1792
HB = B // 2
PH = PW // 2
NC = 23

CB = 32
NCH = B // CB
NS = 8
PF = 6


def rope_tables(shape):
    half = HD // 2
    lane = lax.broadcasted_iota(jnp.int32, shape, 1)
    index = jnp.where(lane < half, lane, lane - half).astype(F32)
    inv_freq = jnp.exp(index * (-2.0 / HD * math.log(500000.0)))
    wavelen = (2.0 * math.pi) / inv_freq
    smooth = (8192.0 / wavelen - 1.0) / 3.0
    blended = (1.0 - smooth) * inv_freq / 8.0 + smooth * inv_freq
    scaled = jnp.where(wavelen < 2048.0, inv_freq, jnp.where(wavelen > 8192.0, inv_freq / 8.0, blended))
    angles = lax.broadcasted_iota(jnp.int32, shape, 0).astype(F32) * scaled
    return jnp.cos(angles), jnp.where(lane < half, -1.0, 1.0) * jnp.sin(angles)


def norm_rows(x_ref, h_ref, w_ref, layer, rows=32):
    def step(i, carry):
        sl = pl.ds(pl.multiple_of(i * rows, rows), rows)
        acc = jnp.zeros((rows, 128), F32)
        for c in range(D // 128):
            t = x_ref[sl, c * 128:(c + 1) * 128].astype(F32)
            acc = acc + t * t
        r = lax.rsqrt(jnp.sum(acc, axis=1, keepdims=True) * (1.0 / D) + 1e-5)
        for c in range(D // 512):
            cs = slice(c * 512, (c + 1) * 512)
            h_ref[sl, cs] = (x_ref[sl, cs].astype(F32) * r * w_ref[layer:layer + 1, cs].astype(F32)).astype(BF16)
        return carry
    lax.fori_loop(0, B // rows, step, 0, unroll=2)


def attn_kernel(layer, first, pos_ref, x_hbm, nw_ref, wq_hbm, wk_hbm, wv_hbm, kc_hbm, vc_hbm, *rest):
    if first:
        o_ref, ko_hbm, vo_hbm = rest[:3]
        rest = rest[3:]
    else:
        o_ref, ko_hbm, vo_hbm = rest[2:5]
        rest = rest[5:]
    x_v, h_v, cos_t, sin_t, cos_ref, sin_ref, wq_v, wk_v, wv_v, acc, q4, o4, kn, vn, rid, kb, vb, wsem, xsem, ksem, vsem, kosem, vosem = rest

    def kv_in(c, slot):
        rs = pl.ds(c * CB, CB)
        return (pltpu.make_async_copy(kc_hbm.at[layer, rs], kb.at[slot], ksem.at[slot]),
                pltpu.make_async_copy(vc_hbm.at[layer, rs], vb.at[slot], vsem.at[slot]))

    def kv_out(c, slot):
        rs = pl.ds(c * CB, CB)
        return (pltpu.make_async_copy(kb.at[slot], ko_hbm.at[layer, rs], kosem.at[slot]),
                pltpu.make_async_copy(vb.at[slot], vo_hbm.at[layer, rs], vosem.at[slot]))

    xcopy = pltpu.make_async_copy(x_hbm, x_v, xsem)
    xcopy.start()
    KC = D // 4
    wcopies = []
    for c in range(4):
        rs = pl.ds(c * KC, KC)
        cs = [pltpu.make_async_copy(wq_hbm.at[layer, rs], wq_v.at[rs], wsem.at[c, 0]),
              pltpu.make_async_copy(wk_hbm.at[layer, rs], wk_v.at[rs], wsem.at[c, 1]),
              pltpu.make_async_copy(wv_hbm.at[layer, rs], wv_v.at[rs], wsem.at[c, 2])]
        wcopies.append(cs)
    for t in wcopies[0]:
        t.start()

    rid[...] = lax.broadcasted_iota(jnp.int32, (S, HD), 0).astype(F32).astype(BF16)
    cos_t[...], sin_t[...] = rope_tables((S, HD))

    def look_up(b, carry):
        p = pos_ref[b]
        cos_ref[pl.ds(b, 1), :] = cos_t[pl.ds(p, 1), :]
        sin_ref[pl.ds(b, 1), :] = sin_t[pl.ds(p, 1), :]
        return carry

    lax.fori_loop(0, B, look_up, 0, unroll=8)
    xcopy.wait()
    for cs in wcopies[1:]:
        for t in cs:
            t.start()
    norm_rows(x_v, h_v, nw_ref, layer)
    for c in range(PF):
        for t in kv_in(c, c):
            t.start()
    for c in range(4):
        for t in wcopies[c]:
            t.wait()
        rs = slice(c * KC, (c + 1) * KC)
        w = jnp.concatenate([wq_v[rs, :], wk_v[rs, :], wv_v[rs, :]], axis=1)
        r = jnp.dot(h_v[:, rs], w, preferred_element_type=F32)
        if c == 0:
            acc[...] = r
        else:
            acc[...] += r

    cos = cos_ref[...]
    sin = sin_ref[...]

    def rope(t):
        t = t.astype(BF16).astype(F32)
        return (t * cos + pltpu.roll(t, HD // 2, 1) * sin).astype(BF16).astype(F32)

    for hd in range(G):
        q4[pl.ds(hd, B, stride=G), :] = rope(acc[:, hd * HD:(hd + 1) * HD])
    kn[...] = rope(acc[:, QW:QW + HD])
    vn[...] = acc[:, QW + HD:QW + 2 * HD].astype(BF16).astype(F32)

    scale = HD ** -0.5
    row = lax.broadcasted_iota(jnp.int32, (4 * G, HD), 0) // G
    lane = lax.broadcasted_iota(jnp.int32, (CB * G, HD), 1)
    even = (row % 2) == 0
    low = row < 2

    def place(buf, new, slot, b0, i, rowid):
        hit = rowid == jnp.full((S, HD), pos_ref[b0 + i].astype(F32), F32).astype(BF16)
        r = jnp.broadcast_to(new[pl.ds(b0 + i, 1), :], (S, HD)).astype(BF16)
        t = jnp.where(hit, r, buf[slot, i])
        buf[slot, i] = t
        return t

    def quad(ts):
        return jnp.concatenate([jnp.concatenate(ts[:2], axis=1), jnp.concatenate(ts[2:], axis=1)], axis=0)

    def scores(c):
        slot = c % NS
        b0 = c * CB
        kv_in(c, slot)[0].wait()
        rowid = rid[...]
        out = []
        for g in range(CB // 4):
            kt = quad([place(kb, kn, slot, b0, 4 * g + i, rowid) for i in range(4)])
            q = q4[pl.ds(pl.multiple_of(b0 * G + 4 * G * g, 4 * G), 4 * G), :]
            lhs = jnp.concatenate([jnp.where(even, q, 0.0), jnp.where(even, 0.0, q)], axis=1).astype(BF16)
            s2 = lax.dot_general(lhs, kt, (((1,), (1,)), ((), ())), preferred_element_type=F32)
            out.append(jnp.where(low, s2[:, :S], s2[:, S:]))
        return jnp.concatenate(out, axis=0)

    def values(c, s):
        slot = c % NS
        b0 = c * CB
        kv_in(c, slot)[1].wait()
        rowid = rid[...]
        posr = []
        for g in range(CB // 4):
            t = jnp.zeros((4 * G, HD), jnp.int32)
            for i in range(4):
                t = jnp.where(row == i, pos_ref[b0 + 4 * g + i], t)
            posr.append(t)
        s = jnp.where(lane <= jnp.concatenate(posr, axis=0), s * scale, -jnp.inf)
        e = jnp.exp(s - jnp.max(s, axis=1, keepdims=True))
        p = e / jnp.sum(e, axis=1, keepdims=True)
        for g in range(CB // 4):
            vt = quad([place(vb, vn, slot, b0, 4 * g + i, rowid) for i in range(4)])
            pg = p[4 * G * g:4 * G * (g + 1)]
            lhs = jnp.concatenate([jnp.where(low, pg, 0.0), jnp.where(low, 0.0, pg)], axis=1).astype(BF16)
            o2 = jnp.dot(lhs, vt, preferred_element_type=F32)
            o4[pl.ds(pl.multiple_of(b0 * G + 4 * G * g, 4 * G), 4 * G), :] = jnp.where(even, o2[:, :HD], o2[:, HD:])

    def turn(c, j):
        kv_out(c, c % NS)[j].start()
        nxt = c + PF

        @pl.when(nxt < NCH)
        def _():
            @pl.when(nxt >= NS)
            def _():
                kv_out(nxt - NS, nxt % NS)[j].wait()
            kv_in(nxt, nxt % NS)[j].start()

    s0 = scores(0)
    turn(0, 0)

    def chunk(c, s):
        sn = scores(c + 1)
        values(c, s)
        turn(c + 1, 0)
        turn(c, 1)
        return sn

    sl = lax.fori_loop(0, NCH - 1, chunk, s0)
    values(NCH - 1, sl)
    turn(NCH - 1, 1)
    for hd in range(G):
        o_ref[:, hd * HD:(hd + 1) * HD] = o4[pl.ds(hd, B, stride=G), :].astype(BF16)
    for c in range(NCH - NS, NCH):
        for t in kv_out(c, c % NS):
            t.wait()


def attn_call(layer, pos, x, nw, wq, wk, wv, kc, vc, prev):
    first = prev is None
    cache = jax.ShapeDtypeStruct(kc.shape, BF16)
    ins = [pos, x, nw, wq, wk, wv, kc, vc]
    specs = [SMEM, ANY, VMEM] + [ANY] * 5
    alias = {}
    if not first:
        alias = {len(ins): 1, len(ins) + 1: 2}
        ins += list(prev)
        specs += [ANY, ANY]
    return pl.pallas_call(
        functools.partial(attn_kernel, layer, first),
        name=f"attn{layer}",
        out_shape=(jax.ShapeDtypeStruct((B, QW), BF16), cache, cache),
        in_specs=specs,
        out_specs=(VMEM, ANY, ANY),
        scratch_shapes=[
            pltpu.VMEM((B, D), BF16),
            pltpu.VMEM((B, D), BF16),
            pltpu.VMEM((S, HD), F32),
            pltpu.VMEM((S, HD), F32),
            pltpu.VMEM((B, HD), F32),
            pltpu.VMEM((B, HD), F32),
            pltpu.VMEM((D, QW), BF16),
            pltpu.VMEM((D, HD), BF16),
            pltpu.VMEM((D, HD), BF16),
            pltpu.VMEM((B, QW + 2 * HD), F32),
            pltpu.VMEM((B * G, HD), F32),
            pltpu.VMEM((B * G, HD), F32),
            pltpu.VMEM((B, HD), F32),
            pltpu.VMEM((B, HD), F32),
            pltpu.VMEM((S, HD), BF16),
            pltpu.VMEM((NS, CB, S, HD), BF16),
            pltpu.VMEM((NS, CB, S, HD), BF16),
            pltpu.SemaphoreType.DMA((4, 3)),
            pltpu.SemaphoreType.DMA,
            pltpu.SemaphoreType.DMA((NS,)),
            pltpu.SemaphoreType.DMA((NS,)),
            pltpu.SemaphoreType.DMA((NS,)),
            pltpu.SemaphoreType.DMA((NS,)),
        ],
        input_output_aliases=alias,
        compiler_params=pltpu.CompilerParams(vmem_limit_bytes=67043328),
    )(*ins)


def mlp_kernel(layer, o_ref, x_hbm, nw_ref, wo_hbm, wg_hbm, wu_hbm, wd_hbm, xo_hbm,
               wo_v, wg_v, wu_v, wd_v, part, xg, hc, acc, a_v, xown, d2d, r1, r2, ssb, r_v,
               wsem, osem, xsem, ssem, rsem):
    me = lax.axis_index("tp")
    k = me % 2
    cx = (me // 2) % 2
    cy = me // 4
    pt = me + 1 - 2 * k
    xn = me + 2 - 4 * cx
    yn = me + 4 - 8 * cy
    dg = xn + 4 - 8 * cy

    def other(p):
        return p + 1 - 2 * k

    peers = (pt, xn, yn, dg, other(xn), other(yn), other(dg))
    order = (dg, xn, yn, me)
    top = pl.ds(0, HB)
    bot = pl.ds(HB, HB)

    def cols(p, h):
        return pl.ds(pl.multiple_of(p * PW + h * PH, PH), PH)

    def chip_cols(p):
        return pl.ds(pl.multiple_of((p // 2) * 2 * PW, 2 * PW), 2 * PW)

    barrier = pltpu.get_barrier_semaphore()
    for d in peers:
        pl.semaphore_signal(barrier, inc=1, device_id={"tp": d}, device_id_type=MESH)

    wos = [pltpu.make_async_copy(wo_hbm.at[layer, :, chip_cols(p)], wo_v.at[:, chip_cols(p)], osem.at[i]) for i, p in enumerate(order)]
    xcs = [pltpu.make_async_copy(x_hbm.at[:, cols(me, h)], xown.at[h], xsem.at[h]) for h in range(2)]
    NG = 4
    gus = []
    for i in range(NG):
        rs = pl.ds(i * (D // NG), D // NG)
        gus.append(pltpu.make_async_copy(wg_hbm.at[layer, rs], wg_v.at[rs], wsem.at[2 * i]))
        gus.append(pltpu.make_async_copy(wu_hbm.at[layer, rs], wu_v.at[rs], wsem.at[2 * i + 1]))
    ND = 4
    wds = []
    for i in range(ND):
        rs = pl.ds(i * (FW // ND), FW // ND)
        wds.append(pltpu.make_async_copy(wd_hbm.at[layer, rs], wd_v.at[rs], wsem.at[2 * NG + i]))
    for t in wos + xcs:
        t.start()

    def send(src, dst, i, dev):
        c = pltpu.make_async_remote_copy(src_ref=src, dst_ref=dst, send_sem=ssem.at[i], recv_sem=rsem.at[i],
                                         device_id={"tp": dev}, device_id_type=MESH)
        c.start()
        return c

    def reduce_scatter(make, enter=False):
        live = [{}, {}]

        def pair(h, t):
            c = live[h]
            p = order[t]
            c["d%d" % t].wait_recv()
            part[h, p] = (part[h, p].astype(F32) + d2d[h, t].astype(F32)).astype(BF16)
            if t == 0:
                c["a0"] = send(part.at[h, dg, top], r1.at[h, 0], NC * h + 4, xn)
                c["b0"] = send(part.at[h, dg, bot], r1.at[h, 2], NC * h + 5, yn)
            elif t == 1:
                c["a1"] = send(part.at[h, xn, top], r1.at[h, 1], NC * h + 6, xn)
            elif t == 2:
                c["b1"] = send(part.at[h, yn, bot], r1.at[h, 3], NC * h + 7, yn)

        todo = []
        for h in range(2):
            for t, p in enumerate(order):
                q = other(p)
                make(h, t, p, q)
                if enter and (h, t) == (0, 0):
                    pl.semaphore_wait(barrier, len(peers))
                live[h]["d%d" % t] = send(part.at[h, q], d2d.at[h, t], NC * h + t, pt)
                if todo:
                    pair(*todo.pop(0))
                todo.append((h, t))
        pair(*todo.pop(0))
        for h in range(2):
            c = live[h]
            c["a0"].wait_recv()
            part[h, yn, top] = (part[h, yn, top].astype(F32) + r1[h, 0].astype(F32)).astype(BF16)
            c["a2"] = send(part.at[h, yn, top], r2.at[h, 0], NC * h + 8, yn)
            c["b0"].wait_recv()
            part[h, xn, bot] = (part[h, xn, bot].astype(F32) + r1[h, 2].astype(F32)).astype(BF16)
            c["b2"] = send(part.at[h, xn, bot], r2.at[h, 1], NC * h + 9, xn)
        return live

    def final(h, c):
        for rs, a, b, i, j in ((top, "a1", "a2", 1, 0), (bot, "b1", "b2", 3, 1)):
            c[a].wait_recv()
            c[b].wait_recv()
            tot = part[h, me, rs].astype(F32) + r1[h, i].astype(F32) + r2[h, j].astype(F32)
            new = (xown[h, rs].astype(F32) + tot.astype(BF16).astype(F32)).astype(BF16)
            xown[h, rs] = new
            xg[h, me, rs] = new

    def gather_start(h, c):
        def go(name, p, rs, i, dev):
            c[name] = send(xg.at[h, p, rs], xg.at[h, p, rs], NC * h + i, dev)
        go("ga0", me, top, 10, yn)
        go("gb0", me, bot, 11, xn)
        go("ga1", me, top, 12, xn)
        go("gb1", me, bot, 13, yn)
        c["p0"] = send(xg.at[h, me], xg.at[h, me], NC * h + 14, pt)

    def forward(h, c, got, name, p, rs, i):
        c[got].wait_recv()
        c[name] = send(xg.at[h, p, rs], xg.at[h, p, rs], NC * h + i, pt)

    def relay(h, c):
        forward(h, c, "ga0", "p1", yn, top, 15)
        c["ga2"] = send(xg.at[h, yn, top], xg.at[h, yn, top], NC * h + 16, xn)
        forward(h, c, "gb0", "p2", xn, bot, 17)
        c["gb2"] = send(xg.at[h, xn, bot], xg.at[h, xn, bot], NC * h + 18, yn)

    def near(h, c):
        forward(h, c, "ga1", "p3", xn, top, 19)
        forward(h, c, "gb1", "p4", yn, bot, 20)

    def far(h, c):
        forward(h, c, "ga2", "p5", dg, top, 21)
        forward(h, c, "gb2", "p6", dg, bot, 22)

    def drain(live):
        for c in live:
            for t in c.values():
                t.wait_send()

    def got(live, *names):
        for c in live:
            for n in names:
                c[n].wait_recv()

    def out_half(h, i, p, q):
        if h == 0:
            wos[i].wait()
            if i == 3:
                for t in gus:
                    t.start()
        w = jnp.concatenate([wo_v[:, cols(p, h)], wo_v[:, cols(q, h)]], axis=1)
        t = jnp.dot(o_ref[...], w, preferred_element_type=F32).astype(BF16)
        part[h, p] = t[:, :PH]
        part[h, q] = t[:, PH:]

    live = reduce_scatter(out_half, True)
    for t in xcs:
        t.wait()
    final(0, live[0])
    gather_start(0, live[0])
    final(1, live[1])
    sq = jnp.zeros((B, 128), F32)
    for h in range(2):
        for c in range(PH // 128):
            t = xg[h, me, :, c * 128:(c + 1) * 128].astype(F32)
            sq = sq + t * t
    ssb[0] = jnp.broadcast_to(jnp.sum(sq.T, axis=0, keepdims=True), (8, B))
    sss = [send(ssb.at[0], ssb.at[1 + j], 2 * NC + j, d) for j, d in enumerate(peers)]
    gather_start(1, live[1])
    relay(0, live[0])
    near(0, live[0])
    for t in sss:
        t.wait_recv()
    tot = ssb[0]
    for j in range(len(peers)):
        tot = tot + ssb[1 + j]
    rr = lax.rsqrt(tot * (1.0 / D) + 1e-5)
    r_v[...] = jnp.broadcast_to(rr[0:1], (128, B)).T
    relay(1, live[1])
    for t in gus:
        t.wait()
    for t in wds:
        t.start()

    TN = 256

    def gate_up(p, first, last, between={}):
        base = pl.multiple_of((p // 2) * 2 * PW, 2 * PW)

        def norm_step(i, carry):
            sl = pl.ds(pl.multiple_of(i * 64, 64), 64)
            r = r_v[sl, :]
            for c in range(2 * PW // 128):
                cs = slice(c * 128, (c + 1) * 128)
                e, h, o = c // 4, (c // 2) % 2, (c % 2) * 128
                w = nw_ref[layer:layer + 1, pl.ds(pl.multiple_of(base + c * 128, 128), 128)].astype(F32)
                hc[sl, cs] = (xg[h, (p // 2) * 2 + e, sl, o:o + 128].astype(F32) * r * w).astype(BF16)
            return carry

        lax.fori_loop(0, B // 64, norm_step, 0)

        ks = pl.ds(base, 2 * PW)
        for j in range(FW // TN):
            cs = slice(j * TN, (j + 1) * TN)
            w = jnp.concatenate([wg_v[ks, cs], wu_v[ks, cs]], axis=1)
            gu = jnp.dot(hc[...], w, preferred_element_type=F32)
            if not first:
                gu = gu + acc[j]
            if not last:
                acc[j] = gu
            else:
                gt = gu[:, :TN].astype(BF16).astype(F32)
                up = gu[:, TN:].astype(BF16).astype(F32)
                a_v[:, cs] = (gt * (1.0 / (1.0 + jnp.exp(-gt))) * up).astype(BF16)
            for act, h in between.get(j, ()):
                act(h, live[h])

    got(live, "p0")
    gate_up(me, True, False, {3: [(near, 1)]})
    got(live, "p2", "p3")
    gate_up(xn, False, False, {2: [(far, 0)], 6: [(far, 1)]})
    got(live, "p1", "p4")
    gate_up(yn, False, False)
    got(live, "p5", "p6")
    gate_up(dg, False, True)
    drain(live)
    for t in sss:
        t.wait_send()
    for t in wds:
        t.wait()

    def down_half(h, i, p, q):
        w = jnp.concatenate([wd_v[:, cols(p, h)], wd_v[:, cols(q, h)]], axis=1)
        t = jnp.dot(a_v[...], w, preferred_element_type=F32).astype(BF16)
        part[h, p] = t[:, :PH]
        part[h, q] = t[:, PH:]

    live = reduce_scatter(down_half)
    for h in range(2):
        final(h, live[h])
        gather_start(h, live[h])
    for h in range(2):
        relay(h, live[h])
    for h in range(2):
        near(h, live[h])
    outs = []

    def write(p):
        for e in range(2):
            for h in range(2):
                n = (p // 2) * 2 + e
                c = pltpu.make_async_copy(xg.at[h, n], xo_hbm.at[:, cols(n, h)], wsem.at[len(outs)])
                c.start()
                outs.append(c)

    got(live, "p0")
    write(me)
    for h in range(2):
        far(h, live[h])
    got(live, "p2", "p3")
    write(xn)
    got(live, "p1", "p4")
    write(yn)
    got(live, "p5", "p6")
    write(dg)
    drain(live)
    for c in outs:
        c.wait()


def mlp_call(layer, o, x, nw, wo, wg, wu, wd):
    return pl.pallas_call(
        functools.partial(mlp_kernel, layer),
        name=f"mlp{layer}",
        out_shape=jax.ShapeDtypeStruct((B, D), BF16),
        in_specs=[VMEM, ANY, VMEM, ANY, ANY, ANY, ANY],
        out_specs=ANY,
        scratch_shapes=[
            pltpu.VMEM((QW, D), BF16),
            pltpu.VMEM((D, FW), BF16),
            pltpu.VMEM((D, FW), BF16),
            pltpu.VMEM((FW, D), BF16),
            pltpu.VMEM((2, NP, B, PH), BF16),
            pltpu.VMEM((2, NP, B, PH), BF16),
            pltpu.VMEM((B, 2 * PW), BF16),
            pltpu.VMEM((FW // 256, B, 512), F32),
            pltpu.VMEM((B, FW), BF16),
            pltpu.VMEM((2, B, PH), BF16),
            pltpu.VMEM((2, 4, B, PH), BF16),
            pltpu.VMEM((2, 4, HB, PH), BF16),
            pltpu.VMEM((2, 2, HB, PH), BF16),
            pltpu.VMEM((8, 8, B), F32),
            pltpu.VMEM((B, 128), F32),
            pltpu.SemaphoreType.DMA((16,)),
            pltpu.SemaphoreType.DMA((4,)),
            pltpu.SemaphoreType.DMA((2,)),
            pltpu.SemaphoreType.DMA((2 * NC + 7,)),
            pltpu.SemaphoreType.DMA((2 * NC + 7,)),
        ],
        compiler_params=pltpu.CompilerParams(collective_id=layer, has_side_effects=True, vmem_limit_bytes=67043328),
    )(o, x, nw, wo, wg, wu, wd)


def copy_kernel(x_hbm, o_hbm, buf, isem, osem):
    n = buf.shape[0]
    rows = B // n
    ins = [pltpu.make_async_copy(x_hbm.at[pl.ds(i * rows, rows)], buf.at[i], isem.at[i]) for i in range(n)]
    outs = [pltpu.make_async_copy(buf.at[i], o_hbm.at[pl.ds(i * rows, rows)], osem.at[i]) for i in range(n)]
    for t in ins:
        t.start()
    for i in range(n):
        ins[i].wait()
        outs[i].start()
    for t in outs:
        t.wait()


def copy_call(x):
    n = 8
    return pl.pallas_call(
        copy_kernel,
        name="emit",
        out_shape=jax.ShapeDtypeStruct(x.shape, x.dtype),
        in_specs=[ANY],
        out_specs=ANY,
        scratch_shapes=[pltpu.VMEM((n, B // n, D), BF16), pltpu.SemaphoreType.DMA((n,)), pltpu.SemaphoreType.DMA((n,))],
        compiler_params=pltpu.CompilerParams(vmem_limit_bytes=67043328),
    )(x)


def solution(mesh):
    row_spec = P('dp', None)
    pos_spec = P('dp')
    cache_spec = P(None, 'dp', None, 'tp', None)
    norm_spec = P(None, None)
    col_spec = P(None, None, 'tp')
    split_rows = P(None, 'tp', None)

    def local_step(hidden, positions, k_cache, v_cache, attn_norm, w_query, w_key, w_value, w_out, mlp_norm, w_gate, w_up, w_down):
        kc = k_cache.reshape(2, B, S, HD)
        vc = v_cache.reshape(2, B, S, HD)
        x = hidden
        prev = None
        for layer in range(2):
            o, ko, vo = attn_call(layer, positions, x, attn_norm, w_query, w_key, w_value, kc, vc, prev)
            prev = (ko, vo)
            x = mlp_call(layer, o, x, mlp_norm, w_out, w_gate, w_up, w_down)
        return copy_call(x), prev[0].reshape(k_cache.shape), prev[1].reshape(v_cache.shape)

    return jax.shard_map(local_step, mesh=mesh, in_specs=(row_spec, pos_spec, cache_spec, cache_spec, norm_spec, col_spec, col_spec, col_spec, split_rows, norm_spec, col_spec, col_spec, split_rows), out_specs=(row_spec, cache_spec, cache_spec), check_vma=False)
```

```python
import functools
import math
import jax
import jax.numpy as jnp
from jax import lax
from jax.experimental import pallas as pl
from jax.experimental.pallas import tpu as pltpu
from jax.sharding import PartitionSpec as P

MESH = pl.DeviceIdType.MESH
F32 = jnp.float32
BF16 = jnp.bfloat16
ANY = pl.BlockSpec(memory_space=pl.ANY)
VMEM = pl.BlockSpec(memory_space=pltpu.VMEM)
SMEM = pl.BlockSpec(memory_space=pltpu.SMEM)

B = 256
D = 4096
S = 128
HD = 128
G = 4
QW = G * HD
NP = 8
PW = D // NP
FW = 1792
HB = B // 2
PH = PW // 2
NC = 23

CB = 32
NCH = B // CB
NS = 8
PF = 6


def rope_tables(shape):
    half = HD // 2
    lane = lax.broadcasted_iota(jnp.int32, shape, 1)
    index = jnp.where(lane < half, lane, lane - half).astype(F32)
    inv_freq = jnp.exp(index * (-2.0 / HD * math.log(500000.0)))
    wavelen = (2.0 * math.pi) / inv_freq
    smooth = (8192.0 / wavelen - 1.0) / 3.0
    blended = (1.0 - smooth) * inv_freq / 8.0 + smooth * inv_freq
    scaled = jnp.where(wavelen < 2048.0, inv_freq, jnp.where(wavelen > 8192.0, inv_freq / 8.0, blended))
    angles = lax.broadcasted_iota(jnp.int32, shape, 0).astype(F32) * scaled
    return jnp.cos(angles), jnp.where(lane < half, -1.0, 1.0) * jnp.sin(angles)


def norm_rows(x_ref, h_ref, w_ref, layer, rows=32):
    def step(i, carry):
        sl = pl.ds(pl.multiple_of(i * rows, rows), rows)
        acc = jnp.zeros((rows, 128), F32)
        for c in range(D // 128):
            t = x_ref[sl, c * 128:(c + 1) * 128].astype(F32)
            acc = acc + t * t
        r = lax.rsqrt(jnp.sum(acc, axis=1, keepdims=True) * (1.0 / D) + 1e-5)
        for c in range(D // 512):
            cs = slice(c * 512, (c + 1) * 512)
            h_ref[sl, cs] = (x_ref[sl, cs].astype(F32) * r * w_ref[layer:layer + 1, cs].astype(F32)).astype(BF16)
        return carry
    lax.fori_loop(0, B // rows, step, 0, unroll=2)


def attn_kernel(layer, first, pos_hbm, x_hbm, nw_hbm, wq_hbm, wk_hbm, wv_hbm, kc_hbm, vc_hbm, *rest):
    if first:
        o_ref, ko_hbm, vo_hbm = rest[:3]
        rest = rest[3:]
    else:
        o_ref, ko_hbm, vo_hbm = rest[2:5]
        rest = rest[5:]
    pos_ref, nw_ref, x_v, h_v, cos_t, sin_t, cos_ref, sin_ref, wq_v, wk_v, wv_v, acc, qkv_v, q4, o4, kn, vn, rid, kb, vb, wsem, xsem, psem, ksem, vsem, kosem, vosem = rest

    def kv_in(c, slot):
        rs = pl.ds(c * CB, CB)
        return (pltpu.make_async_copy(kc_hbm.at[layer, rs], kb.at[slot], ksem.at[slot]),
                pltpu.make_async_copy(vc_hbm.at[layer, rs], vb.at[slot], vsem.at[slot]))

    def kv_out(c, slot):
        rs = pl.ds(c * CB, CB)
        return (pltpu.make_async_copy(kb.at[slot], ko_hbm.at[layer, rs], kosem.at[slot]),
                pltpu.make_async_copy(vb.at[slot], vo_hbm.at[layer, rs], vosem.at[slot]))

    poscopy = pltpu.make_async_copy(pos_hbm, pos_ref, psem.at[0])
    poscopy.start()
    KC = D // 4
    if first:
        xcopy = pltpu.make_async_copy(x_hbm, x_v, xsem)
        xcopy.start()
        nwcopy = pltpu.make_async_copy(nw_hbm, nw_ref, psem.at[1])
        nwcopy.start()
        wcopies = []
        for c in range(4):
            rs = pl.ds(c * KC, KC)
            wcopies.append([pltpu.make_async_copy(wq_hbm.at[layer, rs], wq_v.at[rs], wsem.at[c, 0]),
                            pltpu.make_async_copy(wk_hbm.at[layer, rs], wk_v.at[rs], wsem.at[c, 1]),
                            pltpu.make_async_copy(wv_hbm.at[layer, rs], wv_v.at[rs], wsem.at[c, 2])])
        for t in wcopies[0]:
            t.start()
    else:
        xcopy = pltpu.make_async_copy(x_hbm, qkv_v, xsem)
        xcopy.start()
        for c in range(PF):
            for t in kv_in(c, c):
                t.start()

    rid[...] = lax.broadcasted_iota(jnp.int32, (S, HD), 0).astype(F32).astype(BF16)
    cos_t[...], sin_t[...] = rope_tables((S, HD))

    def look_up(b, carry):
        p = pos_ref[b]
        cos_ref[pl.ds(b, 1), :] = cos_t[pl.ds(p, 1), :]
        sin_ref[pl.ds(b, 1), :] = sin_t[pl.ds(p, 1), :]
        return carry

    poscopy.wait()
    lax.fori_loop(0, B, look_up, 0, unroll=8)
    xcopy.wait()
    if first:
        nwcopy.wait()
        for cs in wcopies[1:]:
            for t in cs:
                t.start()
        norm_rows(x_v, h_v, nw_ref, layer)
        for c in range(PF):
            for t in kv_in(c, c):
                t.start()
        for c in range(4):
            for t in wcopies[c]:
                t.wait()
            rs = slice(c * KC, (c + 1) * KC)
            w = jnp.concatenate([wq_v[rs, :], wk_v[rs, :], wv_v[rs, :]], axis=1)
            r = jnp.dot(h_v[:, rs], w, preferred_element_type=F32)
            if c == 0:
                acc[...] = r
            else:
                acc[...] += r
        qkv = acc
    else:
        qkv = qkv_v

    cos = cos_ref[...]
    sin = sin_ref[...]

    def rope(t):
        t = t.astype(BF16).astype(F32)
        return (t * cos + pltpu.roll(t, HD // 2, 1) * sin).astype(BF16).astype(F32)

    for hd in range(G):
        q4[pl.ds(hd, B, stride=G), :] = rope(qkv[:, hd * HD:(hd + 1) * HD])
    kn[...] = rope(qkv[:, QW:QW + HD])
    vn[...] = qkv[:, QW + HD:QW + 2 * HD].astype(BF16).astype(F32)

    scale = HD ** -0.5
    row = lax.broadcasted_iota(jnp.int32, (4 * G, HD), 0) // G
    lane = lax.broadcasted_iota(jnp.int32, (CB * G, HD), 1)
    even = (row % 2) == 0
    low = row < 2

    def place(buf, new, slot, b0, i, rowid):
        hit = rowid == jnp.full((S, HD), pos_ref[b0 + i].astype(F32), F32).astype(BF16)
        r = jnp.broadcast_to(new[pl.ds(b0 + i, 1), :], (S, HD)).astype(BF16)
        t = jnp.where(hit, r, buf[slot, i])
        buf[slot, i] = t
        return t

    def quad(ts):
        return jnp.concatenate([jnp.concatenate(ts[:2], axis=1), jnp.concatenate(ts[2:], axis=1)], axis=0)

    def scores(c):
        slot = c % NS
        b0 = c * CB
        kv_in(c, slot)[0].wait()
        rowid = rid[...]
        out = []
        for g in range(CB // 4):
            kt = quad([place(kb, kn, slot, b0, 4 * g + i, rowid) for i in range(4)])
            q = q4[pl.ds(pl.multiple_of(b0 * G + 4 * G * g, 4 * G), 4 * G), :]
            lhs = jnp.concatenate([jnp.where(even, q, 0.0), jnp.where(even, 0.0, q)], axis=1).astype(BF16)
            s2 = lax.dot_general(lhs, kt, (((1,), (1,)), ((), ())), preferred_element_type=F32)
            out.append(jnp.where(low, s2[:, :S], s2[:, S:]))
        return jnp.concatenate(out, axis=0)

    def values(c, s):
        slot = c % NS
        b0 = c * CB
        kv_in(c, slot)[1].wait()
        rowid = rid[...]
        posr = []
        for g in range(CB // 4):
            t = jnp.zeros((4 * G, HD), jnp.int32)
            for i in range(4):
                t = jnp.where(row == i, pos_ref[b0 + 4 * g + i], t)
            posr.append(t)
        s = jnp.where(lane <= jnp.concatenate(posr, axis=0), s * scale, -jnp.inf)
        e = jnp.exp(s - jnp.max(s, axis=1, keepdims=True))
        p = e / jnp.sum(e, axis=1, keepdims=True)
        for g in range(CB // 4):
            vt = quad([place(vb, vn, slot, b0, 4 * g + i, rowid) for i in range(4)])
            pg = p[4 * G * g:4 * G * (g + 1)]
            lhs = jnp.concatenate([jnp.where(low, pg, 0.0), jnp.where(low, 0.0, pg)], axis=1).astype(BF16)
            o2 = jnp.dot(lhs, vt, preferred_element_type=F32)
            o4[pl.ds(pl.multiple_of(b0 * G + 4 * G * g, 4 * G), 4 * G), :] = jnp.where(even, o2[:, :HD], o2[:, HD:])

    def turn(c, j):
        kv_out(c, c % NS)[j].start()
        nxt = c + PF

        @pl.when(nxt < NCH)
        def _():
            @pl.when(nxt >= NS)
            def _():
                kv_out(nxt - NS, nxt % NS)[j].wait()
            kv_in(nxt, nxt % NS)[j].start()

    s0 = scores(0)
    turn(0, 0)

    def chunk(c, s):
        sn = scores(c + 1)
        values(c, s)
        turn(c + 1, 0)
        turn(c, 1)
        return sn

    sl = lax.fori_loop(0, NCH - 1, chunk, s0)
    values(NCH - 1, sl)
    turn(NCH - 1, 1)
    for hd in range(G):
        o_ref[:, hd * HD:(hd + 1) * HD] = o4[pl.ds(hd, B, stride=G), :].astype(BF16)
    for c in range(NCH - NS, NCH):
        for t in kv_out(c, c % NS):
            t.wait()


def attn_call(layer, pos, x, nw, wq, wk, wv, kc, vc, prev):
    first = prev is None
    cache = jax.ShapeDtypeStruct(kc.shape, BF16)
    ins = [pos, x, nw, wq, wk, wv, kc, vc]
    specs = [ANY] * 8
    alias = {}
    if not first:
        alias = {len(ins): 1, len(ins) + 1: 2}
        ins += list(prev)
        specs += [ANY, ANY]
    return pl.pallas_call(
        functools.partial(attn_kernel, layer, first),
        name=f"attn{layer}",
        out_shape=(jax.ShapeDtypeStruct((B, QW), BF16), cache, cache),
        in_specs=specs,
        out_specs=(VMEM, ANY, ANY),
        scratch_shapes=[
            pltpu.SMEM((B,), jnp.int32),
            pltpu.VMEM((2, D), BF16),
            pltpu.VMEM((B, D), BF16),
            pltpu.VMEM((B, D), BF16),
            pltpu.VMEM((S, HD), F32),
            pltpu.VMEM((S, HD), F32),
            pltpu.VMEM((B, HD), F32),
            pltpu.VMEM((B, HD), F32),
            pltpu.VMEM((D, QW), BF16),
            pltpu.VMEM((D, HD), BF16),
            pltpu.VMEM((D, HD), BF16),
            pltpu.VMEM((B, QW + 2 * HD), F32),
            pltpu.VMEM((B, QW + 2 * HD), BF16),
            pltpu.VMEM((B * G, HD), F32),
            pltpu.VMEM((B * G, HD), F32),
            pltpu.VMEM((B, HD), F32),
            pltpu.VMEM((B, HD), F32),
            pltpu.VMEM((S, HD), BF16),
            pltpu.VMEM((NS, CB, S, HD), BF16),
            pltpu.VMEM((NS, CB, S, HD), BF16),
            pltpu.SemaphoreType.DMA((4, 3)),
            pltpu.SemaphoreType.DMA,
            pltpu.SemaphoreType.DMA((2,)),
            pltpu.SemaphoreType.DMA((NS,)),
            pltpu.SemaphoreType.DMA((NS,)),
            pltpu.SemaphoreType.DMA((NS,)),
            pltpu.SemaphoreType.DMA((NS,)),
        ],
        input_output_aliases=alias,
        compiler_params=pltpu.CompilerParams(vmem_limit_bytes=67043328),
    )(*ins)


def mlp_kernel(layer, last, o_hbm, x_hbm, nw_hbm, an_hbm, wo_hbm, wg_hbm, wu_hbm, wd_hbm, wq_hbm, wk_hbm, wv_hbm, *rest):
    if last:
        xo_hbm = rest[0]
        rest = rest[1:]
    else:
        xo_hbm, qkv_hbm = rest[:2]
        rest = rest[2:]
    (o_ref, nw_ref, an_ref, wo_v, wg_v, wu_v, wd_v, part, xg, hc, acc, a_v, qkv_v, xown, d2d, r1, r2, ssb, r_v,
     wsem, osem, xsem, isem, qsem, ssem, rsem) = rest
    me = lax.axis_index("tp")
    k = me % 2
    cx = (me // 2) % 2
    cy = me // 4
    pt = me + 1 - 2 * k
    xn = me + 2 - 4 * cx
    yn = me + 4 - 8 * cy
    dg = xn + 4 - 8 * cy

    def other(p):
        return p + 1 - 2 * k

    peers = (pt, xn, yn, dg, other(xn), other(yn), other(dg))
    order = (dg, xn, yn, me)
    top = pl.ds(0, HB)
    bot = pl.ds(HB, HB)

    def cols(p, h):
        return pl.ds(pl.multiple_of(p * PW + h * PH, PH), PH)

    def chip_cols(p):
        return pl.ds(pl.multiple_of((p // 2) * 2 * PW, 2 * PW), 2 * PW)

    barrier = pltpu.get_barrier_semaphore()
    for d in peers:
        pl.semaphore_signal(barrier, inc=1, device_id={"tp": d}, device_id_type=MESH)

    wos = [pltpu.make_async_copy(wo_hbm.at[layer, :, chip_cols(p)], wo_v.at[:, chip_cols(p)], osem.at[i]) for i, p in enumerate(order)]
    xcs = [pltpu.make_async_copy(x_hbm.at[h] if last else x_hbm.at[:, cols(me, h)], xown.at[h], xsem.at[h]) for h in range(2)]
    NG = 4
    gus = []
    for i in range(NG):
        rs = pl.ds(i * (D // NG), D // NG)
        gus.append(pltpu.make_async_copy(wg_hbm.at[layer, rs], wg_v.at[rs], wsem.at[2 * i]))
        gus.append(pltpu.make_async_copy(wu_hbm.at[layer, rs], wu_v.at[rs], wsem.at[2 * i + 1]))
    ND = 4
    wds = []
    for i in range(ND):
        rs = pl.ds(i * (FW // ND), FW // ND)
        wds.append(pltpu.make_async_copy(wd_hbm.at[layer, rs], wd_v.at[rs], wsem.at[2 * NG + i]))
    ocopy = pltpu.make_async_copy(o_hbm, o_ref, isem.at[0])
    ncopies = [pltpu.make_async_copy(nw_hbm, nw_ref, isem.at[1]), pltpu.make_async_copy(an_hbm, an_ref, isem.at[2])]
    for t in [ocopy] + wos + ncopies + xcs:
        t.start()
    ocopy.wait()

    def send(src, dst, i, dev):
        c = pltpu.make_async_remote_copy(src_ref=src, dst_ref=dst, send_sem=ssem.at[i], recv_sem=rsem.at[i],
                                         device_id={"tp": dev}, device_id_type=MESH)
        c.start()
        return c

    def reduce_scatter(make, enter=False):
        live = [{}, {}]

        def pair(h, t):
            c = live[h]
            p = order[t]
            c["d%d" % t].wait_recv()
            part[h, p] = (part[h, p].astype(F32) + d2d[h, t].astype(F32)).astype(BF16)
            if t == 0:
                c["a0"] = send(part.at[h, dg, top], r1.at[h, 0], NC * h + 4, xn)
                c["b0"] = send(part.at[h, dg, bot], r1.at[h, 2], NC * h + 5, yn)
            elif t == 1:
                c["a1"] = send(part.at[h, xn, top], r1.at[h, 1], NC * h + 6, xn)
            elif t == 2:
                c["b1"] = send(part.at[h, yn, bot], r1.at[h, 3], NC * h + 7, yn)

        todo = []
        for h in range(2):
            for t, p in enumerate(order):
                q = other(p)
                make(h, t, p, q)
                if enter and (h, t) == (0, 0):
                    pl.semaphore_wait(barrier, len(peers))
                live[h]["d%d" % t] = send(part.at[h, q], d2d.at[h, t], NC * h + t, pt)
                if todo:
                    pair(*todo.pop(0))
                todo.append((h, t))
        pair(*todo.pop(0))
        for h in range(2):
            c = live[h]
            c["a0"].wait_recv()
            part[h, yn, top] = (part[h, yn, top].astype(F32) + r1[h, 0].astype(F32)).astype(BF16)
            c["a2"] = send(part.at[h, yn, top], r2.at[h, 0], NC * h + 8, yn)
            c["b0"].wait_recv()
            part[h, xn, bot] = (part[h, xn, bot].astype(F32) + r1[h, 2].astype(F32)).astype(BF16)
            c["b2"] = send(part.at[h, xn, bot], r2.at[h, 1], NC * h + 9, xn)
        return live

    def final(h, c):
        for rs, a, b, i, j in ((top, "a1", "a2", 1, 0), (bot, "b1", "b2", 3, 1)):
            c[a].wait_recv()
            c[b].wait_recv()
            tot = part[h, me, rs].astype(F32) + r1[h, i].astype(F32) + r2[h, j].astype(F32)
            new = (xown[h, rs].astype(F32) + tot.astype(BF16).astype(F32)).astype(BF16)
            xown[h, rs] = new
            xg[h, me, rs] = new

    def gather_start(h, c):
        def go(name, p, rs, i, dev):
            c[name] = send(xg.at[h, p, rs], xg.at[h, p, rs], NC * h + i, dev)
        go("ga0", me, top, 10, yn)
        go("gb0", me, bot, 11, xn)
        go("ga1", me, top, 12, xn)
        go("gb1", me, bot, 13, yn)
        c["p0"] = send(xg.at[h, me], xg.at[h, me], NC * h + 14, pt)

    def forward(h, c, got, name, p, rs, i):
        c[got].wait_recv()
        c[name] = send(xg.at[h, p, rs], xg.at[h, p, rs], NC * h + i, pt)

    def relay(h, c):
        forward(h, c, "ga0", "p1", yn, top, 15)
        c["ga2"] = send(xg.at[h, yn, top], xg.at[h, yn, top], NC * h + 16, xn)
        forward(h, c, "gb0", "p2", xn, bot, 17)
        c["gb2"] = send(xg.at[h, xn, bot], xg.at[h, xn, bot], NC * h + 18, yn)

    def near(h, c):
        forward(h, c, "ga1", "p3", xn, top, 19)
        forward(h, c, "gb1", "p4", yn, bot, 20)

    def far(h, c):
        forward(h, c, "ga2", "p5", dg, top, 21)
        forward(h, c, "gb2", "p6", dg, bot, 22)

    def drain(live):
        for c in live:
            for t in c.values():
                t.wait_send()

    def got(live, *names):
        for c in live:
            for n in names:
                c[n].wait_recv()

    def out_half(h, i, p, q):
        if h == 0:
            wos[i].wait()
            if i == 3:
                for t in gus:
                    t.start()
        w = jnp.concatenate([wo_v[:, cols(p, h)], wo_v[:, cols(q, h)]], axis=1)
        t = jnp.dot(o_ref[...], w, preferred_element_type=F32).astype(BF16)
        part[h, p] = t[:, :PH]
        part[h, q] = t[:, PH:]

    def square_start():
        sq = jnp.zeros((B, 128), F32)
        for h in range(2):
            for c in range(PH // 128):
                t = xg[h, me, :, c * 128:(c + 1) * 128].astype(F32)
                sq = sq + t * t
        ssb[0] = jnp.broadcast_to(jnp.sum(sq.T, axis=0, keepdims=True), (8, B))
        return [send(ssb.at[0], ssb.at[1 + j], 2 * NC + j, d) for j, d in enumerate(peers)]

    def square_end(sss):
        for t in sss:
            t.wait_recv()
        tot = ssb[0]
        for j in range(len(peers)):
            tot = tot + ssb[1 + j]
        rr = lax.rsqrt(tot * (1.0 / D) + 1e-5)
        r_v[...] = jnp.broadcast_to(rr[0:1], (128, B)).T

    def norm_chunk(p, w_ref, row):
        base = pl.multiple_of((p // 2) * 2 * PW, 2 * PW)

        def norm_step(i, carry):
            sl = pl.ds(pl.multiple_of(i * 64, 64), 64)
            r = r_v[sl, :]
            for c in range(2 * PW // 128):
                cs = slice(c * 128, (c + 1) * 128)
                e, h, o = c // 4, (c // 2) % 2, (c % 2) * 128
                w = w_ref[row:row + 1, pl.ds(pl.multiple_of(base + c * 128, 128), 128)].astype(F32)
                hc[sl, cs] = (xg[h, (p // 2) * 2 + e, sl, o:o + 128].astype(F32) * r * w).astype(BF16)
            return carry

        lax.fori_loop(0, B // 64, norm_step, 0)
        return pl.ds(base, 2 * PW)

    live = reduce_scatter(out_half, True)
    for t in xcs + ncopies:
        t.wait()
    final(0, live[0])
    gather_start(0, live[0])
    final(1, live[1])
    sss = square_start()
    gather_start(1, live[1])
    relay(0, live[0])
    near(0, live[0])
    square_end(sss)
    relay(1, live[1])
    for t in gus:
        t.wait()
    for t in wds:
        t.start()

    TN = 256

    def gate_up(p, first, last, between={}):
        ks = norm_chunk(p, nw_ref, layer)
        for j in range(FW // TN):
            cs = slice(j * TN, (j + 1) * TN)
            w = jnp.concatenate([wg_v[ks, cs], wu_v[ks, cs]], axis=1)
            gu = jnp.dot(hc[...], w, preferred_element_type=F32)
            if not first:
                gu = gu + acc[j]
            if not last:
                acc[j] = gu
            else:
                gt = gu[:, :TN].astype(BF16).astype(F32)
                up = gu[:, TN:].astype(BF16).astype(F32)
                a_v[:, cs] = (gt * (1.0 / (1.0 + jnp.exp(-gt))) * up).astype(BF16)
            for act, h in between.get(j, ()):
                act(h, live[h])

    got(live, "p0")
    gate_up(me, True, False, {3: [(near, 1)]})
    got(live, "p2", "p3")
    gate_up(xn, False, False, {2: [(far, 0)], 6: [(far, 1)]})
    got(live, "p1", "p4")
    gate_up(yn, False, False)
    got(live, "p5", "p6")
    gate_up(dg, False, True)
    drain(live)
    for t in sss:
        t.wait_send()
    if not last:
        qs = []
        for i in range(2):
            rs = pl.ds(i * (D // 2), D // 2)
            qs += [pltpu.make_async_copy(wq_hbm.at[layer + 1, rs], wg_v.at[rs, pl.ds(0, QW)], qsem.at[i, 0]),
                   pltpu.make_async_copy(wk_hbm.at[layer + 1, rs], wg_v.at[rs, pl.ds(QW, HD)], qsem.at[i, 1]),
                   pltpu.make_async_copy(wv_hbm.at[layer + 1, rs], wg_v.at[rs, pl.ds(QW + HD, HD)], qsem.at[i, 2])]
    for t in wds:
        t.wait()
    if not last:
        for t in qs:
            t.start()

    def down_half(h, i, p, q):
        w = jnp.concatenate([wd_v[:, cols(p, h)], wd_v[:, cols(q, h)]], axis=1)
        t = jnp.dot(a_v[...], w, preferred_element_type=F32).astype(BF16)
        part[h, p] = t[:, :PH]
        part[h, q] = t[:, PH:]

    live = reduce_scatter(down_half)
    if last:
        for h in range(2):
            final(h, live[h])
            gather_start(h, live[h])
        for h in range(2):
            relay(h, live[h])
        for h in range(2):
            near(h, live[h])
        outs = []

        def write(p):
            for e in range(2):
                for h in range(2):
                    n = (p // 2) * 2 + e
                    c = pltpu.make_async_copy(xg.at[h, n], xo_hbm.at[:, cols(n, h)], wsem.at[len(outs)])
                    c.start()
                    outs.append(c)

        got(live, "p0")
        write(me)
        for h in range(2):
            far(h, live[h])
        got(live, "p2", "p3")
        write(xn)
        got(live, "p1", "p4")
        write(yn)
        got(live, "p5", "p6")
        write(dg)
        drain(live)
        for c in outs:
            c.wait()
    else:
        final(0, live[0])
        gather_start(0, live[0])
        final(1, live[1])
        sss = square_start()
        gather_start(1, live[1])
        outs = [pltpu.make_async_copy(xown, xo_hbm, isem.at[0])]
        outs[0].start()
        relay(0, live[0])
        near(0, live[0])
        square_end(sss)
        relay(1, live[1])
        near(1, live[1])
        for t in qs:
            t.wait()

        def qkv(p, first, end):
            ks = norm_chunk(p, an_ref, layer + 1)
            r = jnp.dot(hc[...], wg_v[ks, :QW + 2 * HD], preferred_element_type=F32)
            if not first:
                r = r + jnp.concatenate([acc[0], acc[1, :, :2 * HD]], axis=1)
            if end:
                qkv_v[...] = r.astype(BF16)
            else:
                acc[0] = r[:, :QW]
                acc[1, :, :2 * HD] = r[:, QW:]

        got(live, "p0")
        qkv(me, True, False)
        far(0, live[0])
        got(live, "p2", "p3")
        qkv(xn, False, False)
        far(1, live[1])
        got(live, "p1", "p4")
        qkv(yn, False, False)
        got(live, "p5", "p6")
        qkv(dg, False, True)
        outs.append(pltpu.make_async_copy(qkv_v, qkv_hbm, isem.at[1]))
        outs[1].start()
        drain(live)
        for t in sss:
            t.wait_send()
        for c in outs:
            c.wait()


def mlp_call(layer, last, o, x, nw, an, wo, wg, wu, wd, wq, wk, wv):
    if last:
        out_shape = jax.ShapeDtypeStruct((B, D), BF16)
        out_specs = ANY
    else:
        out_shape = (jax.ShapeDtypeStruct((2, B, PH), BF16), jax.ShapeDtypeStruct((B, QW + 2 * HD), BF16))
        out_specs = (ANY, ANY)
    return pl.pallas_call(
        functools.partial(mlp_kernel, layer, last),
        name=f"mlp{layer}",
        out_shape=out_shape,
        in_specs=[ANY] * 11,
        out_specs=out_specs,
        scratch_shapes=[
            pltpu.VMEM((B, QW), BF16),
            pltpu.VMEM((2, D), BF16),
            pltpu.VMEM((2, D), BF16),
            pltpu.VMEM((QW, D), BF16),
            pltpu.VMEM((D, FW), BF16),
            pltpu.VMEM((D, FW), BF16),
            pltpu.VMEM((FW, D), BF16),
            pltpu.VMEM((2, NP, B, PH), BF16),
            pltpu.VMEM((2, NP, B, PH), BF16),
            pltpu.VMEM((B, 2 * PW), BF16),
            pltpu.VMEM((FW // 256, B, 512), F32),
            pltpu.VMEM((B, FW), BF16),
            pltpu.VMEM((B, QW + 2 * HD), BF16),
            pltpu.VMEM((2, B, PH), BF16),
            pltpu.VMEM((2, 4, B, PH), BF16),
            pltpu.VMEM((2, 4, HB, PH), BF16),
            pltpu.VMEM((2, 2, HB, PH), BF16),
            pltpu.VMEM((8, 8, B), F32),
            pltpu.VMEM((B, 128), F32),
            pltpu.SemaphoreType.DMA((16,)),
            pltpu.SemaphoreType.DMA((4,)),
            pltpu.SemaphoreType.DMA((2,)),
            pltpu.SemaphoreType.DMA((3,)),
            pltpu.SemaphoreType.DMA((2, 3)),
            pltpu.SemaphoreType.DMA((2 * NC + 7,)),
            pltpu.SemaphoreType.DMA((2 * NC + 7,)),
        ],
        compiler_params=pltpu.CompilerParams(collective_id=layer, has_side_effects=True, vmem_limit_bytes=67043328),
    )(o, x, nw, an, wo, wg, wu, wd, wq, wk, wv)


def copy_kernel(x_hbm, o_hbm, buf, isem, osem):
    n = buf.shape[0]
    rows = B // n
    ins = [pltpu.make_async_copy(x_hbm.at[pl.ds(i * rows, rows)], buf.at[i], isem.at[i]) for i in range(n)]
    outs = [pltpu.make_async_copy(buf.at[i], o_hbm.at[pl.ds(i * rows, rows)], osem.at[i]) for i in range(n)]
    for t in ins:
        t.start()
    for i in range(n):
        ins[i].wait()
        outs[i].start()
    for t in outs:
        t.wait()


def copy_call(x):
    n = 8
    return pl.pallas_call(
        copy_kernel,
        name="emit",
        out_shape=jax.ShapeDtypeStruct(x.shape, x.dtype),
        in_specs=[ANY],
        out_specs=ANY,
        scratch_shapes=[pltpu.VMEM((n, B // n, D), BF16), pltpu.SemaphoreType.DMA((n,)), pltpu.SemaphoreType.DMA((n,))],
        compiler_params=pltpu.CompilerParams(vmem_limit_bytes=67043328),
    )(x)


def solution(mesh):
    row_spec = P('dp', None)
    pos_spec = P('dp')
    cache_spec = P(None, 'dp', None, 'tp', None)
    norm_spec = P(None, None)
    col_spec = P(None, None, 'tp')
    split_rows = P(None, 'tp', None)

    def local_step(hidden, positions, k_cache, v_cache, attn_norm, w_query, w_key, w_value, w_out, mlp_norm, w_gate, w_up, w_down):
        kc = k_cache.reshape(2, B, S, HD)
        vc = v_cache.reshape(2, B, S, HD)
        x = hidden
        prev = None
        for layer in range(2):
            o, ko, vo = attn_call(layer, positions, x if layer == 0 else qkv, attn_norm, w_query, w_key, w_value, kc, vc, prev)
            prev = (ko, vo)
            y = mlp_call(layer, layer == 1, o, x, mlp_norm, attn_norm, w_out, w_gate, w_up, w_down, w_query, w_key, w_value)
            if layer == 0:
                x, qkv = y
            else:
                x = y
        return copy_call(x), prev[0].reshape(k_cache.shape), prev[1].reshape(v_cache.shape)

    return jax.shard_map(local_step, mesh=mesh, in_specs=(row_spec, pos_spec, cache_spec, cache_spec, norm_spec, col_spec, col_spec, col_spec, split_rows, norm_spec, col_spec, col_spec, split_rows), out_specs=(row_spec, cache_spec, cache_spec), check_vma=False)
```

```python
import functools
import math
import jax
import jax.numpy as jnp
from jax import lax
from jax.experimental import pallas as pl
from jax.experimental.pallas import tpu as pltpu
from jax.sharding import PartitionSpec as P

MESH = pl.DeviceIdType.MESH
F32 = jnp.float32
BF16 = jnp.bfloat16
ANY = pl.BlockSpec(memory_space=pl.ANY)
VMEM = pl.BlockSpec(memory_space=pltpu.VMEM)
SMEM = pl.BlockSpec(memory_space=pltpu.SMEM)

B = 256
D = 4096
S = 128
HD = 128
G = 4
QW = G * HD
NP = 8
PW = D // NP
FW = 1792
HB = B // 2
PH = PW // 2
NC = 23

CB = 32
NCH = B // CB
NS = 8
PF = 6


def rope_tables(shape):
    half = HD // 2
    lane = lax.broadcasted_iota(jnp.int32, shape, 1)
    index = jnp.where(lane < half, lane, lane - half).astype(F32)
    inv_freq = jnp.exp(index * (-2.0 / HD * math.log(500000.0)))
    wavelen = (2.0 * math.pi) / inv_freq
    smooth = (8192.0 / wavelen - 1.0) / 3.0
    blended = (1.0 - smooth) * inv_freq / 8.0 + smooth * inv_freq
    scaled = jnp.where(wavelen < 2048.0, inv_freq, jnp.where(wavelen > 8192.0, inv_freq / 8.0, blended))
    angles = lax.broadcasted_iota(jnp.int32, shape, 0).astype(F32) * scaled
    return jnp.cos(angles), jnp.where(lane < half, -1.0, 1.0) * jnp.sin(angles)


def norm_rows(x_ref, h_ref, w_ref, layer, rows=32):
    def step(i, carry):
        sl = pl.ds(pl.multiple_of(i * rows, rows), rows)
        acc = jnp.zeros((rows, 128), F32)
        for c in range(D // 128):
            t = x_ref[sl, c * 128:(c + 1) * 128].astype(F32)
            acc = acc + t * t
        r = lax.rsqrt(jnp.sum(acc, axis=1, keepdims=True) * (1.0 / D) + 1e-5)
        for c in range(D // 512):
            cs = slice(c * 512, (c + 1) * 512)
            h_ref[sl, cs] = (x_ref[sl, cs].astype(F32) * r * w_ref[layer:layer + 1, cs].astype(F32)).astype(BF16)
        return carry
    lax.fori_loop(0, B // rows, step, 0, unroll=2)


def attn_kernel(layer, first, pos_hbm, x_hbm, nw_hbm, wq_hbm, wk_hbm, wv_hbm, kc_hbm, vc_hbm, *rest):
    if first:
        o_ref, ko_hbm, vo_hbm = rest[:3]
        rest = rest[3:]
    else:
        o_ref, ko_hbm, vo_hbm = rest[2:5]
        rest = rest[5:]
    pos_ref, nw_ref, x_v, h_v, cos_t, sin_t, cos_ref, sin_ref, wq_v, wk_v, wv_v, acc, qkv_v, o_v, q4, o4, kn, vn, rid, kb, vb, wsem, xsem, psem, ksem, vsem, kosem, vosem = rest

    def kv_in(c, slot):
        rs = pl.ds(c * CB, CB)
        return (pltpu.make_async_copy(kc_hbm.at[layer, rs], kb.at[slot], ksem.at[slot]),
                pltpu.make_async_copy(vc_hbm.at[layer, rs], vb.at[slot], vsem.at[slot]))

    def kv_out(c, slot):
        rs = pl.ds(c * CB, CB)
        return (pltpu.make_async_copy(kb.at[slot], ko_hbm.at[layer, rs], kosem.at[slot]),
                pltpu.make_async_copy(vb.at[slot], vo_hbm.at[layer, rs], vosem.at[slot]))

    poscopy = pltpu.make_async_copy(pos_hbm, pos_ref, psem.at[0])
    poscopy.start()
    KC = D // 4
    if first:
        xcopy = pltpu.make_async_copy(x_hbm, x_v, xsem)
        xcopy.start()
        nwcopy = pltpu.make_async_copy(nw_hbm, nw_ref, psem.at[1])
        nwcopy.start()
        wcopies = []
        for c in range(4):
            rs = pl.ds(c * KC, KC)
            wcopies.append([pltpu.make_async_copy(wq_hbm.at[layer, rs], wq_v.at[rs], wsem.at[c, 0]),
                            pltpu.make_async_copy(wk_hbm.at[layer, rs], wk_v.at[rs], wsem.at[c, 1]),
                            pltpu.make_async_copy(wv_hbm.at[layer, rs], wv_v.at[rs], wsem.at[c, 2])])
        for t in wcopies[0]:
            t.start()
    else:
        xcopy = pltpu.make_async_copy(x_hbm, qkv_v, xsem)
        xcopy.start()
        for c in range(PF):
            for t in kv_in(c, c):
                t.start()

    rid[...] = lax.broadcasted_iota(jnp.int32, (S, HD), 0).astype(F32).astype(BF16)
    cos_t[...], sin_t[...] = rope_tables((S, HD))

    def look_up(b, carry):
        p = pos_ref[b]
        cos_ref[pl.ds(b, 1), :] = cos_t[pl.ds(p, 1), :]
        sin_ref[pl.ds(b, 1), :] = sin_t[pl.ds(p, 1), :]
        return carry

    poscopy.wait()
    lax.fori_loop(0, B, look_up, 0, unroll=8)
    xcopy.wait()
    if first:
        nwcopy.wait()
        for cs in wcopies[1:]:
            for t in cs:
                t.start()
        norm_rows(x_v, h_v, nw_ref, layer)
        for c in range(PF):
            for t in kv_in(c, c):
                t.start()
        for c in range(4):
            for t in wcopies[c]:
                t.wait()
            rs = slice(c * KC, (c + 1) * KC)
            w = jnp.concatenate([wq_v[rs, :], wk_v[rs, :], wv_v[rs, :]], axis=1)
            r = jnp.dot(h_v[:, rs], w, preferred_element_type=F32)
            if c == 0:
                acc[...] = r
            else:
                acc[...] += r
        qkv = acc
    else:
        qkv = qkv_v

    cos = cos_ref[...]
    sin = sin_ref[...]

    def rope(t):
        t = t.astype(BF16).astype(F32)
        return (t * cos + pltpu.roll(t, HD // 2, 1) * sin).astype(BF16).astype(F32)

    for hd in range(G):
        q4[pl.ds(hd, B, stride=G), :] = rope(qkv[:, hd * HD:(hd + 1) * HD])
    kn[...] = rope(qkv[:, QW:QW + HD])
    vn[...] = qkv[:, QW + HD:QW + 2 * HD].astype(BF16).astype(F32)

    scale = HD ** -0.5
    row = lax.broadcasted_iota(jnp.int32, (4 * G, HD), 0) // G
    lane = lax.broadcasted_iota(jnp.int32, (CB * G, HD), 1)
    even = (row % 2) == 0
    low = row < 2

    def place(buf, new, slot, b0, i, rowid):
        hit = rowid == jnp.full((S, HD), pos_ref[b0 + i].astype(F32), F32).astype(BF16)
        r = jnp.broadcast_to(new[pl.ds(b0 + i, 1), :], (S, HD)).astype(BF16)
        t = jnp.where(hit, r, buf[slot, i])
        buf[slot, i] = t
        return t

    def quad(ts):
        return jnp.concatenate([jnp.concatenate(ts[:2], axis=1), jnp.concatenate(ts[2:], axis=1)], axis=0)

    def scores(c):
        slot = c % NS
        b0 = c * CB
        rowid = rid[...]
        out = []
        for g in range(CB // 4):
            kt = quad([place(kb, kn, slot, b0, 4 * g + i, rowid) for i in range(4)])
            q = q4[pl.ds(pl.multiple_of(b0 * G + 4 * G * g, 4 * G), 4 * G), :]
            lhs = jnp.concatenate([jnp.where(even, q, 0.0), jnp.where(even, 0.0, q)], axis=1).astype(BF16)
            s2 = lax.dot_general(lhs, kt, (((1,), (1,)), ((), ())), preferred_element_type=F32)
            out.append(jnp.where(low, s2[:, :S], s2[:, S:]))
        return jnp.concatenate(out, axis=0)

    def values(c, s):
        slot = c % NS
        b0 = c * CB
        rowid = rid[...]
        posr = []
        for g in range(CB // 4):
            t = jnp.zeros((4 * G, HD), jnp.int32)
            for i in range(4):
                t = jnp.where(row == i, pos_ref[b0 + 4 * g + i], t)
            posr.append(t)
        s = jnp.where(lane <= jnp.concatenate(posr, axis=0), s * scale, -jnp.inf)
        e = jnp.exp(s - jnp.max(s, axis=1, keepdims=True))
        p = e / jnp.sum(e, axis=1, keepdims=True)
        for g in range(CB // 4):
            vt = quad([place(vb, vn, slot, b0, 4 * g + i, rowid) for i in range(4)])
            pg = p[4 * G * g:4 * G * (g + 1)]
            lhs = jnp.concatenate([jnp.where(low, pg, 0.0), jnp.where(low, 0.0, pg)], axis=1).astype(BF16)
            o2 = jnp.dot(lhs, vt, preferred_element_type=F32)
            o4[pl.ds(pl.multiple_of(b0 * G + 4 * G * g, 4 * G), 4 * G), :] = jnp.where(even, o2[:, :HD], o2[:, HD:])

    def turn(c, j):
        kv_out(c, c % NS)[j].start()
        nxt = c + PF

        @pl.when(nxt < NCH)
        def _():
            @pl.when(nxt >= NS)
            def _():
                kv_out(nxt - NS, nxt % NS)[j].wait()
            kv_in(nxt, nxt % NS)[j].start()

    def arrived(c, j):
        kv_in(c, c % NS)[j].wait()

    arrived(0, 0)
    s0 = scores(0)
    turn(0, 0)

    def chunk(c, s):
        arrived(c + 1, 0)
        arrived(c, 1)
        sn = scores(c + 1)
        values(c, s)
        turn(c + 1, 0)
        turn(c, 1)
        return sn

    sl = lax.fori_loop(0, NCH - 1, chunk, s0)
    arrived(NCH - 1, 1)
    values(NCH - 1, sl)
    turn(NCH - 1, 1)
    for hd in range(G):
        o_v[:, hd * HD:(hd + 1) * HD] = o4[pl.ds(hd, B, stride=G), :].astype(BF16)
    ocopy = pltpu.make_async_copy(o_v, o_ref, xsem)
    ocopy.start()
    for c in range(NCH - NS, NCH):
        for t in kv_out(c, c % NS):
            t.wait()
    ocopy.wait()


def attn_call(layer, pos, x, nw, wq, wk, wv, kc, vc, prev):
    first = prev is None
    cache = jax.ShapeDtypeStruct(kc.shape, BF16)
    ins = [pos, x, nw, wq, wk, wv, kc, vc]
    specs = [ANY] * 8
    alias = {}
    if not first:
        alias = {len(ins): 1, len(ins) + 1: 2}
        ins += list(prev)
        specs += [ANY, ANY]
    return pl.pallas_call(
        functools.partial(attn_kernel, layer, first),
        name=f"attn{layer}",
        out_shape=(jax.ShapeDtypeStruct((B, QW), BF16), cache, cache),
        in_specs=specs,
        out_specs=(ANY, ANY, ANY),
        scratch_shapes=[
            pltpu.SMEM((B,), jnp.int32),
            pltpu.VMEM((2, D), BF16),
            pltpu.VMEM((B, D), BF16),
            pltpu.VMEM((B, D), BF16),
            pltpu.VMEM((S, HD), F32),
            pltpu.VMEM((S, HD), F32),
            pltpu.VMEM((B, HD), F32),
            pltpu.VMEM((B, HD), F32),
            pltpu.VMEM((D, QW), BF16),
            pltpu.VMEM((D, HD), BF16),
            pltpu.VMEM((D, HD), BF16),
            pltpu.VMEM((B, QW + 2 * HD), F32),
            pltpu.VMEM((B, QW + 2 * HD), BF16),
            pltpu.VMEM((B, QW), BF16),
            pltpu.VMEM((B * G, HD), F32),
            pltpu.VMEM((B * G, HD), F32),
            pltpu.VMEM((B, HD), F32),
            pltpu.VMEM((B, HD), F32),
            pltpu.VMEM((S, HD), BF16),
            pltpu.VMEM((NS, CB, S, HD), BF16),
            pltpu.VMEM((NS, CB, S, HD), BF16),
            pltpu.SemaphoreType.DMA((4, 3)),
            pltpu.SemaphoreType.DMA,
            pltpu.SemaphoreType.DMA((2,)),
            pltpu.SemaphoreType.DMA((NS,)),
            pltpu.SemaphoreType.DMA((NS,)),
            pltpu.SemaphoreType.DMA((NS,)),
            pltpu.SemaphoreType.DMA((NS,)),
        ],
        input_output_aliases=alias,
        compiler_params=pltpu.CompilerParams(vmem_limit_bytes=67043328),
    )(*ins)


def mlp_kernel(layer, last, o_hbm, x_hbm, nw_hbm, an_hbm, wo_hbm, wg_hbm, wu_hbm, wd_hbm, wq_hbm, wk_hbm, wv_hbm, *rest):
    if last:
        xo_hbm = rest[0]
        rest = rest[1:]
    else:
        xo_hbm, qkv_hbm = rest[:2]
        rest = rest[2:]
    (o_ref, nw_ref, an_ref, wo_v, wg_v, wu_v, wd_v, part, xg, hc, acc, a_v, qkv_v, xown, d2d, r1, r2, ssb, r_v,
     wsem, osem, xsem, isem, qsem, ssem, rsem) = rest
    me = lax.axis_index("tp")
    k = me % 2
    cx = (me // 2) % 2
    cy = me // 4
    pt = me + 1 - 2 * k
    xn = me + 2 - 4 * cx
    yn = me + 4 - 8 * cy
    dg = xn + 4 - 8 * cy

    def other(p):
        return p + 1 - 2 * k

    peers = (pt, xn, yn, dg, other(xn), other(yn), other(dg))
    order = (dg, xn, yn, me)
    top = pl.ds(0, HB)
    bot = pl.ds(HB, HB)

    def cols(p, h):
        return pl.ds(pl.multiple_of(p * PW + h * PH, PH), PH)

    def chip_cols(p):
        return pl.ds(pl.multiple_of((p // 2) * 2 * PW, 2 * PW), 2 * PW)

    barrier = pltpu.get_barrier_semaphore()
    for d in peers:
        pl.semaphore_signal(barrier, inc=1, device_id={"tp": d}, device_id_type=MESH)

    wos = [pltpu.make_async_copy(wo_hbm.at[layer, :, chip_cols(p)], wo_v.at[:, chip_cols(p)], osem.at[i]) for i, p in enumerate(order)]
    xcs = [pltpu.make_async_copy(x_hbm.at[h] if last else x_hbm.at[:, cols(me, h)], xown.at[h], xsem.at[h]) for h in range(2)]
    NG = 4
    gus = []
    for i in range(NG):
        rs = pl.ds(i * (D // NG), D // NG)
        gus.append(pltpu.make_async_copy(wg_hbm.at[layer, rs], wg_v.at[rs], wsem.at[2 * i]))
        gus.append(pltpu.make_async_copy(wu_hbm.at[layer, rs], wu_v.at[rs], wsem.at[2 * i + 1]))
    ND = 4
    wds = []
    for i in range(ND):
        rs = pl.ds(i * (FW // ND), FW // ND)
        wds.append(pltpu.make_async_copy(wd_hbm.at[layer, rs], wd_v.at[rs], wsem.at[2 * NG + i]))
    ocopy = pltpu.make_async_copy(o_hbm, o_ref, isem.at[0])
    ncopies = [pltpu.make_async_copy(nw_hbm, nw_ref, isem.at[1]), pltpu.make_async_copy(an_hbm, an_ref, isem.at[2])]
    for t in [ocopy] + wos + ncopies + xcs:
        t.start()
    ocopy.wait()

    def remote(src, dst, i, dev):
        return pltpu.make_async_remote_copy(src_ref=src, dst_ref=dst, send_sem=ssem.at[i], recv_sem=rsem.at[i],
                                            device_id={"tp": dev}, device_id_type=MESH)

    def send(src, dst, i, dev):
        c = remote(src, dst, i, dev)
        c.start()
        return c

    def reduce_scatter(make, enter=False):
        live = [{}, {}]

        def pair(h, t):
            c = live[h]
            p = order[t]
            c["d%d" % t].wait_recv()
            part[h, p] = (part[h, p].astype(F32) + d2d[h, t].astype(F32)).astype(BF16)
            if t == 0:
                c["a0"] = send(part.at[h, dg, top], r1.at[h, 0], NC * h + 4, xn)
                c["b0"] = send(part.at[h, dg, bot], r1.at[h, 2], NC * h + 5, yn)
            elif t == 1:
                c["a1"] = send(part.at[h, xn, top], r1.at[h, 1], NC * h + 6, xn)
            elif t == 2:
                c["b1"] = send(part.at[h, yn, bot], r1.at[h, 3], NC * h + 7, yn)

        todo = []
        for h in range(2):
            for t, p in enumerate(order):
                q = other(p)
                make(h, t, p, q)
                if enter and (h, t) == (0, 0):
                    pl.semaphore_wait(barrier, len(peers))
                live[h]["d%d" % t] = send(part.at[h, q], d2d.at[h, t], NC * h + t, pt)
                if todo:
                    pair(*todo.pop(0))
                todo.append((h, t))
        pair(*todo.pop(0))
        for h in range(2):
            c = live[h]
            c["a0"].wait_recv()
            part[h, yn, top] = (part[h, yn, top].astype(F32) + r1[h, 0].astype(F32)).astype(BF16)
            c["a2"] = send(part.at[h, yn, top], r2.at[h, 0], NC * h + 8, yn)
            c["b0"].wait_recv()
            part[h, xn, bot] = (part[h, xn, bot].astype(F32) + r1[h, 2].astype(F32)).astype(BF16)
            c["b2"] = send(part.at[h, xn, bot], r2.at[h, 1], NC * h + 9, xn)
        return live

    def final(h, c):
        for rs, a, b, i, j in ((top, "a1", "a2", 1, 0), (bot, "b1", "b2", 3, 1)):
            c[a].wait_recv()
            c[b].wait_recv()
            tot = part[h, me, rs].astype(F32) + r1[h, i].astype(F32) + r2[h, j].astype(F32)
            new = (xown[h, rs].astype(F32) + tot.astype(BF16).astype(F32)).astype(BF16)
            xown[h, rs] = new
            xg[h, me, rs] = new

    def go(h, c, name, p, rs, i, dev):
        c[name] = send(xg.at[h, p, rs], xg.at[h, p, rs], NC * h + i, dev)

    def gather_first(h, c):
        go(h, c, "ga0", me, top, 10, yn)
        go(h, c, "gb0", me, bot, 11, xn)
        c["p0"] = send(xg.at[h, me], xg.at[h, me], NC * h + 14, pt)

    def gather_second(h, c):
        go(h, c, "ga1", me, top, 12, xn)
        go(h, c, "gb1", me, bot, 13, yn)

    def forward(h, c, got, name, p, rs, i):
        c[got].wait_recv()
        c[name] = send(xg.at[h, p, rs], xg.at[h, p, rs], NC * h + i, pt)

    def relay(h, c):
        forward(h, c, "ga0", "p1", yn, top, 15)
        c["ga2"] = send(xg.at[h, yn, top], xg.at[h, yn, top], NC * h + 16, xn)
        forward(h, c, "gb0", "p2", xn, bot, 17)
        c["gb2"] = send(xg.at[h, xn, bot], xg.at[h, xn, bot], NC * h + 18, yn)

    def near(h, c):
        forward(h, c, "ga1", "p3", xn, top, 19)
        forward(h, c, "gb1", "p4", yn, bot, 20)

    def far(h, c):
        forward(h, c, "ga2", "p5", dg, top, 21)
        forward(h, c, "gb2", "p6", dg, bot, 22)

    def drain(live):
        for c in live:
            for t in c.values():
                t.wait_send()

    def got(live, *names):
        for c in live:
            for n in names:
                c[n].wait_recv()

    def out_half(h, i, p, q):
        if h == 0:
            wos[i].wait()
            if i == 3:
                for t in gus:
                    t.start()
        w = jnp.concatenate([wo_v[:, cols(p, h)], wo_v[:, cols(q, h)]], axis=1)
        t = jnp.dot(o_ref[...], w, preferred_element_type=F32).astype(BF16)
        part[h, p] = t[:, :PH]
        part[h, q] = t[:, PH:]

    def square_start():
        sq = jnp.zeros((B, 128), F32)
        for h in range(2):
            for c in range(PH // 128):
                t = xg[h, me, :, c * 128:(c + 1) * 128].astype(F32)
                sq = sq + t * t
        ssb[0] = jnp.broadcast_to(jnp.sum(sq.T, axis=0, keepdims=True), (8, B))
        return [send(ssb.at[0], ssb.at[1 + j], 2 * NC + j, d) for j, d in enumerate(peers)]

    def square_end(sss):
        for t in sss:
            t.wait_recv()
        tot = ssb[0]
        for j in range(len(peers)):
            tot = tot + ssb[1 + j]
        rr = lax.rsqrt(tot * (1.0 / D) + 1e-5)
        r_v[...] = jnp.broadcast_to(rr[0:1], (128, B)).T

    def norm_rows_of(p, w_ref, row, first, n):
        base = pl.multiple_of((p // 2) * 2 * PW, 2 * PW)

        def norm_step(i, carry):
            sl = pl.ds(pl.multiple_of(first + i * 64, 64), 64)
            r = r_v[sl, :]
            for c in range(2 * PW // 128):
                cs = slice(c * 128, (c + 1) * 128)
                e, h, o = c // 4, (c // 2) % 2, (c % 2) * 128
                w = w_ref[row:row + 1, pl.ds(pl.multiple_of(base + c * 128, 128), 128)].astype(F32)
                hc[sl, cs] = (xg[h, (p // 2) * 2 + e, sl, o:o + 128].astype(F32) * r * w).astype(BF16)
            return carry

        lax.fori_loop(0, n // 64, norm_step, 0)
        return pl.ds(base, 2 * PW)

    def norm_chunk(ps, w_ref, row):
        if len(ps) == 1:
            return [norm_rows_of(ps[0], w_ref, row, 0, B)]
        return [norm_rows_of(p, w_ref, row, i * HB, HB) for i, p in enumerate(ps)]

    def chunk_dot(kss, weight):
        if len(kss) == 1:
            return jnp.dot(hc[...], weight(kss[0]), preferred_element_type=F32)
        return jnp.concatenate([jnp.dot(hc[i * HB:(i + 1) * HB, :], weight(ks), preferred_element_type=F32)
                                for i, ks in enumerate(kss)], axis=0)

    live = reduce_scatter(out_half, True)
    for t in xcs + ncopies:
        t.wait()
    final(0, live[0])
    gather_first(0, live[0])
    final(1, live[1])
    sss = square_start()
    gather_first(1, live[1])
    for h in range(2):
        gather_second(h, live[h])
    relay(0, live[0])
    square_end(sss)
    relay(1, live[1])
    for t in gus:
        t.wait()
    for t in wds:
        t.start()

    TN = 256

    def gate_up(ps, first, last, between={}):
        kss = norm_chunk(ps, nw_ref, layer)
        for j in range(FW // TN):
            cs = slice(j * TN, (j + 1) * TN)
            gu = chunk_dot(kss, lambda ks: jnp.concatenate([wg_v[ks, cs], wu_v[ks, cs]], axis=1))
            if not first:
                gu = gu + acc[j]
            if not last:
                acc[j] = gu
            else:
                gt = gu[:, :TN].astype(BF16).astype(F32)
                up = gu[:, TN:].astype(BF16).astype(F32)
                a_v[:, cs] = (gt * (1.0 / (1.0 + jnp.exp(-gt))) * up).astype(BF16)
            if j in between:
                between[j]()

    got(live, "p0")
    gate_up([me], True, False)
    near(0, live[0])

    def crossed(i, carry):
        for h in range(2):
            for n in (15 + 4 * i, 17 + 3 * i):
                remote(xg.at[h, me, top], xg.at[h, me, top], NC * h + n, pt).wait_recv()

        def sends():
            pl.when(i == 0)(lambda: near(1, dict(live[1])))
            pl.when(i == 1)(lambda: far(0, dict(live[0])))

        gate_up([yn + i * (xn - yn), xn + i * (yn - xn)], False, False, {2: sends})
        return carry

    lax.fori_loop(0, 2, crossed, 0)
    for h, name, p, rs, i in ((1, "p3", xn, top, 19), (1, "p4", yn, bot, 20), (0, "p5", dg, top, 21), (0, "p6", dg, bot, 22)):
        live[h][name] = remote(xg.at[h, p, rs], xg.at[h, p, rs], NC * h + i, pt)
    far(1, live[1])
    got(live, "p5", "p6")
    gate_up([dg], False, True)
    drain(live)
    for t in sss:
        t.wait_send()
    if not last:
        qs = []
        for i in range(2):
            rs = pl.ds(i * (D // 2), D // 2)
            qs += [pltpu.make_async_copy(wq_hbm.at[layer + 1, rs], wg_v.at[rs, pl.ds(0, QW)], qsem.at[i, 0]),
                   pltpu.make_async_copy(wk_hbm.at[layer + 1, rs], wg_v.at[rs, pl.ds(QW, HD)], qsem.at[i, 1]),
                   pltpu.make_async_copy(wv_hbm.at[layer + 1, rs], wg_v.at[rs, pl.ds(QW + HD, HD)], qsem.at[i, 2])]
    for t in wds:
        t.wait()
    if not last:
        for t in qs:
            t.start()

    def down_half(h, i, p, q):
        w = jnp.concatenate([wd_v[:, cols(p, h)], wd_v[:, cols(q, h)]], axis=1)
        t = jnp.dot(a_v[...], w, preferred_element_type=F32).astype(BF16)
        part[h, p] = t[:, :PH]
        part[h, q] = t[:, PH:]

    live = reduce_scatter(down_half)
    if last:
        for h in range(2):
            final(h, live[h])
            gather_first(h, live[h])
        for h in range(2):
            gather_second(h, live[h])
        for h in range(2):
            relay(h, live[h])
        for h in range(2):
            near(h, live[h])
        outs = []

        def write(p):
            for e in range(2):
                for h in range(2):
                    n = (p // 2) * 2 + e
                    c = pltpu.make_async_copy(xg.at[h, n], xo_hbm.at[:, cols(n, h)], wsem.at[len(outs)])
                    c.start()
                    outs.append(c)

        got(live, "p0")
        write(me)
        for h in range(2):
            far(h, live[h])
        got(live, "p2", "p3")
        write(xn)
        got(live, "p1", "p4")
        write(yn)
        got(live, "p5", "p6")
        write(dg)
        drain(live)
        for c in outs:
            c.wait()
    else:
        final(0, live[0])
        gather_first(0, live[0])
        final(1, live[1])
        sss = square_start()
        gather_first(1, live[1])
        for h in range(2):
            gather_second(h, live[h])
        outs = [pltpu.make_async_copy(xown, xo_hbm, isem.at[0])]
        outs[0].start()
        relay(0, live[0])
        square_end(sss)
        relay(1, live[1])
        for h in range(2):
            near(h, live[h])
        for t in qs:
            t.wait()

        def qkv(ps, first, end):
            kss = norm_chunk(ps, an_ref, layer + 1)
            r = chunk_dot(kss, lambda ks: wg_v[ks, :QW + 2 * HD])
            if not first:
                r = r + jnp.concatenate([acc[0], acc[1, :, :2 * HD]], axis=1)
            if end:
                qkv_v[...] = r.astype(BF16)
            else:
                acc[0] = r[:, :QW]
                acc[1, :, :2 * HD] = r[:, QW:]

        got(live, "p0")
        qkv([me], True, False)
        got(live, "p1", "p2")
        qkv([yn, xn], False, False)
        far(0, live[0])
        got(live, "p3", "p4")
        qkv([xn, yn], False, False)
        far(1, live[1])
        got(live, "p5", "p6")
        qkv([dg], False, True)
        outs.append(pltpu.make_async_copy(qkv_v, qkv_hbm, isem.at[1]))
        outs[1].start()
        drain(live)
        for t in sss:
            t.wait_send()
        for c in outs:
            c.wait()


def mlp_call(layer, last, o, x, nw, an, wo, wg, wu, wd, wq, wk, wv):
    if last:
        out_shape = jax.ShapeDtypeStruct((B, D), BF16)
        out_specs = ANY
    else:
        out_shape = (jax.ShapeDtypeStruct((2, B, PH), BF16), jax.ShapeDtypeStruct((B, QW + 2 * HD), BF16))
        out_specs = (ANY, ANY)
    return pl.pallas_call(
        functools.partial(mlp_kernel, layer, last),
        name=f"mlp{layer}",
        out_shape=out_shape,
        in_specs=[ANY] * 11,
        out_specs=out_specs,
        scratch_shapes=[
            pltpu.VMEM((B, QW), BF16),
            pltpu.VMEM((2, D), BF16),
            pltpu.VMEM((2, D), BF16),
            pltpu.VMEM((QW, D), BF16),
            pltpu.VMEM((D, FW), BF16),
            pltpu.VMEM((D, FW), BF16),
            pltpu.VMEM((FW, D), BF16),
            pltpu.VMEM((2, NP, B, PH), BF16),
            pltpu.VMEM((2, NP, B, PH), BF16),
            pltpu.VMEM((B, 2 * PW), BF16),
            pltpu.VMEM((FW // 256, B, 512), F32),
            pltpu.VMEM((B, FW), BF16),
            pltpu.VMEM((B, QW + 2 * HD), BF16),
            pltpu.VMEM((2, B, PH), BF16),
            pltpu.VMEM((2, 4, B, PH), BF16),
            pltpu.VMEM((2, 4, HB, PH), BF16),
            pltpu.VMEM((2, 2, HB, PH), BF16),
            pltpu.VMEM((8, 8, B), F32),
            pltpu.VMEM((B, 128), F32),
            pltpu.SemaphoreType.DMA((16,)),
            pltpu.SemaphoreType.DMA((4,)),
            pltpu.SemaphoreType.DMA((2,)),
            pltpu.SemaphoreType.DMA((3,)),
            pltpu.SemaphoreType.DMA((2, 3)),
            pltpu.SemaphoreType.DMA((2 * NC + 7,)),
            pltpu.SemaphoreType.DMA((2 * NC + 7,)),
        ],
        compiler_params=pltpu.CompilerParams(collective_id=layer, has_side_effects=True, vmem_limit_bytes=67043328),
    )(o, x, nw, an, wo, wg, wu, wd, wq, wk, wv)


def copy_kernel(x_hbm, o_hbm, buf, isem, osem):
    n = buf.shape[0]
    rows = B // n
    ins = [pltpu.make_async_copy(x_hbm.at[pl.ds(i * rows, rows)], buf.at[i], isem.at[i]) for i in range(n)]
    outs = [pltpu.make_async_copy(buf.at[i], o_hbm.at[pl.ds(i * rows, rows)], osem.at[i]) for i in range(n)]
    for t in ins:
        t.start()
    for i in range(n):
        ins[i].wait()
        outs[i].start()
    for t in outs:
        t.wait()


def copy_call(x):
    n = 8
    return pl.pallas_call(
        copy_kernel,
        name="emit",
        out_shape=jax.ShapeDtypeStruct(x.shape, x.dtype),
        in_specs=[ANY],
        out_specs=ANY,
        scratch_shapes=[pltpu.VMEM((n, B // n, D), BF16), pltpu.SemaphoreType.DMA((n,)), pltpu.SemaphoreType.DMA((n,))],
        compiler_params=pltpu.CompilerParams(vmem_limit_bytes=67043328),
    )(x)


def solution(mesh):
    row_spec = P('dp', None)
    pos_spec = P('dp')
    cache_spec = P(None, 'dp', None, 'tp', None)
    norm_spec = P(None, None)
    col_spec = P(None, None, 'tp')
    split_rows = P(None, 'tp', None)

    def local_step(hidden, positions, k_cache, v_cache, attn_norm, w_query, w_key, w_value, w_out, mlp_norm, w_gate, w_up, w_down):
        kc = k_cache.reshape(2, B, S, HD)
        vc = v_cache.reshape(2, B, S, HD)
        x = hidden
        prev = None
        for layer in range(2):
            o, ko, vo = attn_call(layer, positions, x if layer == 0 else qkv, attn_norm, w_query, w_key, w_value, kc, vc, prev)
            prev = (ko, vo)
            y = mlp_call(layer, layer == 1, o, x, mlp_norm, attn_norm, w_out, w_gate, w_up, w_down, w_query, w_key, w_value)
            if layer == 0:
                x, qkv = y
            else:
                x = y
        return copy_call(x), prev[0].reshape(k_cache.shape), prev[1].reshape(v_cache.shape)

    return jax.shard_map(local_step, mesh=mesh, in_specs=(row_spec, pos_spec, cache_spec, cache_spec, norm_spec, col_spec, col_spec, col_spec, split_rows, norm_spec, col_spec, col_spec, split_rows), out_specs=(row_spec, cache_spec, cache_spec), check_vma=False)
```

```python
import functools
import math
import jax
import jax.numpy as jnp
from jax import lax
from jax.experimental import pallas as pl
from jax.experimental.pallas import tpu as pltpu
from jax.sharding import PartitionSpec as P

MESH = pl.DeviceIdType.MESH
F32 = jnp.float32
BF16 = jnp.bfloat16
ANY = pl.BlockSpec(memory_space=pl.ANY)
VMEM = pl.BlockSpec(memory_space=pltpu.VMEM)
SMEM = pl.BlockSpec(memory_space=pltpu.SMEM)

B = 256
D = 4096
S = 128
HD = 128
G = 4
QW = G * HD
NP = 8
PW = D // NP
FW = 1792
HB = B // 2
PH = PW // 2
NC = 23

CB = 32
NCH = B // CB
NS = 8
PF = 6


def rope_tables(shape):
    half = HD // 2
    lane = lax.broadcasted_iota(jnp.int32, shape, 1)
    index = jnp.where(lane < half, lane, lane - half).astype(F32)
    inv_freq = jnp.exp(index * (-2.0 / HD * math.log(500000.0)))
    wavelen = (2.0 * math.pi) / inv_freq
    smooth = (8192.0 / wavelen - 1.0) / 3.0
    blended = (1.0 - smooth) * inv_freq / 8.0 + smooth * inv_freq
    scaled = jnp.where(wavelen < 2048.0, inv_freq, jnp.where(wavelen > 8192.0, inv_freq / 8.0, blended))
    angles = lax.broadcasted_iota(jnp.int32, shape, 0).astype(F32) * scaled
    return jnp.cos(angles), jnp.where(lane < half, -1.0, 1.0) * jnp.sin(angles)


def norm_rows(x_ref, h_ref, w_ref, layer, rows=32):
    def step(i, carry):
        sl = pl.ds(pl.multiple_of(i * rows, rows), rows)
        acc = jnp.zeros((rows, 128), F32)
        for c in range(D // 128):
            t = x_ref[sl, c * 128:(c + 1) * 128].astype(F32)
            acc = acc + t * t
        r = lax.rsqrt(jnp.sum(acc, axis=1, keepdims=True) * (1.0 / D) + 1e-5)
        for c in range(D // 512):
            cs = slice(c * 512, (c + 1) * 512)
            h_ref[sl, cs] = (x_ref[sl, cs].astype(F32) * r * w_ref[layer:layer + 1, cs].astype(F32)).astype(BF16)
        return carry
    lax.fori_loop(0, B // rows, step, 0, unroll=2)


def attn_kernel(layer, first, pos_hbm, x_hbm, nw_hbm, wq_hbm, wk_hbm, wv_hbm, kc_hbm, vc_hbm, *rest):
    if first:
        o_ref, ko_hbm, vo_hbm = rest[:3]
        rest = rest[3:]
    else:
        o_ref, ko_hbm, vo_hbm = rest[2:5]
        rest = rest[5:]
    pos_ref, nw_ref, x_v, h_v, cos_t, sin_t, cos_ref, sin_ref, wq_v, wk_v, wv_v, acc, qkv_v, o_v, q4, o4, kn, vn, rid, kb, vb, wsem, xsem, psem, ksem, vsem, kosem, vosem = rest

    def kv_in(c, slot):
        rs = pl.ds(c * CB, CB)
        return (pltpu.make_async_copy(kc_hbm.at[layer, rs], kb.at[slot], ksem.at[slot]),
                pltpu.make_async_copy(vc_hbm.at[layer, rs], vb.at[slot], vsem.at[slot]))

    def kv_out(c, slot):
        rs = pl.ds(c * CB, CB)
        return (pltpu.make_async_copy(kb.at[slot], ko_hbm.at[layer, rs], kosem.at[slot]),
                pltpu.make_async_copy(vb.at[slot], vo_hbm.at[layer, rs], vosem.at[slot]))

    poscopy = pltpu.make_async_copy(pos_hbm, pos_ref, psem.at[0])
    poscopy.start()
    KC = D // 4
    if first:
        xcopy = pltpu.make_async_copy(x_hbm, x_v, xsem)
        xcopy.start()
        nwcopy = pltpu.make_async_copy(nw_hbm, nw_ref, psem.at[1])
        nwcopy.start()
        wcopies = []
        for c in range(4):
            rs = pl.ds(c * KC, KC)
            wcopies.append([pltpu.make_async_copy(wq_hbm.at[layer, rs], wq_v.at[rs], wsem.at[c, 0]),
                            pltpu.make_async_copy(wk_hbm.at[layer, rs], wk_v.at[rs], wsem.at[c, 1]),
                            pltpu.make_async_copy(wv_hbm.at[layer, rs], wv_v.at[rs], wsem.at[c, 2])])
        for t in wcopies[0]:
            t.start()
    else:
        xcopy = pltpu.make_async_copy(x_hbm, qkv_v, xsem)
        xcopy.start()
        for c in range(PF):
            for t in kv_in(c, c):
                t.start()

    rid[...] = lax.broadcasted_iota(jnp.int32, (S, HD), 0).astype(F32).astype(BF16)
    cos_t[...], sin_t[...] = rope_tables((S, HD))

    def look_up(b, carry):
        p = pos_ref[b]
        cos_ref[pl.ds(b, 1), :] = cos_t[pl.ds(p, 1), :]
        sin_ref[pl.ds(b, 1), :] = sin_t[pl.ds(p, 1), :]
        return carry

    poscopy.wait()
    lax.fori_loop(0, B, look_up, 0, unroll=8)
    xcopy.wait()
    if first:
        nwcopy.wait()
        for cs in wcopies[1:]:
            for t in cs:
                t.start()
        norm_rows(x_v, h_v, nw_ref, layer)
        for c in range(PF):
            for t in kv_in(c, c):
                t.start()
        for c in range(4):
            for t in wcopies[c]:
                t.wait()
            rs = slice(c * KC, (c + 1) * KC)
            w = jnp.concatenate([wq_v[rs, :], wk_v[rs, :], wv_v[rs, :]], axis=1)
            r = jnp.dot(h_v[:, rs], w, preferred_element_type=F32)
            if c == 0:
                acc[...] = r
            else:
                acc[...] += r
        qkv = acc
    else:
        qkv = qkv_v

    cos = cos_ref[...]
    sin = sin_ref[...]

    def rope(t):
        t = t.astype(BF16).astype(F32)
        return (t * cos + pltpu.roll(t, HD // 2, 1) * sin).astype(BF16).astype(F32)

    for hd in range(G):
        q4[pl.ds(hd, B, stride=G), :] = rope(qkv[:, hd * HD:(hd + 1) * HD])
    kn[...] = rope(qkv[:, QW:QW + HD])
    vn[...] = qkv[:, QW + HD:QW + 2 * HD].astype(BF16).astype(F32)

    scale = HD ** -0.5
    row = lax.broadcasted_iota(jnp.int32, (4 * G, HD), 0) // G
    lane = lax.broadcasted_iota(jnp.int32, (CB * G, HD), 1)
    even = (row % 2) == 0
    low = row < 2

    def place(buf, new, slot, b0, i, rowid):
        hit = rowid == jnp.full((S, HD), pos_ref[b0 + i].astype(F32), F32).astype(BF16)
        r = jnp.broadcast_to(new[pl.ds(b0 + i, 1), :], (S, HD)).astype(BF16)
        t = jnp.where(hit, r, buf[slot, i])
        buf[slot, i] = t
        return t

    def quad(ts):
        return jnp.concatenate([jnp.concatenate(ts[:2], axis=1), jnp.concatenate(ts[2:], axis=1)], axis=0)

    def scores(c):
        slot = c % NS
        b0 = c * CB
        rowid = rid[...]
        out = []
        for g in range(CB // 4):
            kt = quad([place(kb, kn, slot, b0, 4 * g + i, rowid) for i in range(4)])
            q = q4[pl.ds(pl.multiple_of(b0 * G + 4 * G * g, 4 * G), 4 * G), :]
            lhs = jnp.concatenate([jnp.where(even, q, 0.0), jnp.where(even, 0.0, q)], axis=1).astype(BF16)
            s2 = lax.dot_general(lhs, kt, (((1,), (1,)), ((), ())), preferred_element_type=F32)
            out.append(jnp.where(low, s2[:, :S], s2[:, S:]))
        return jnp.concatenate(out, axis=0)

    def values(c, s):
        slot = c % NS
        b0 = c * CB
        rowid = rid[...]
        posr = []
        for g in range(CB // 4):
            t = jnp.zeros((4 * G, HD), jnp.int32)
            for i in range(4):
                t = jnp.where(row == i, pos_ref[b0 + 4 * g + i], t)
            posr.append(t)
        s = jnp.where(lane <= jnp.concatenate(posr, axis=0), s * scale, -jnp.inf)
        e = jnp.exp(s - jnp.max(s, axis=1, keepdims=True))
        p = e / jnp.sum(e, axis=1, keepdims=True)
        for g in range(CB // 4):
            vt = quad([place(vb, vn, slot, b0, 4 * g + i, rowid) for i in range(4)])
            pg = p[4 * G * g:4 * G * (g + 1)]
            lhs = jnp.concatenate([jnp.where(low, pg, 0.0), jnp.where(low, 0.0, pg)], axis=1).astype(BF16)
            o2 = jnp.dot(lhs, vt, preferred_element_type=F32)
            o4[pl.ds(pl.multiple_of(b0 * G + 4 * G * g, 4 * G), 4 * G), :] = jnp.where(even, o2[:, :HD], o2[:, HD:])

    def turn(c, j):
        kv_out(c, c % NS)[j].start()
        nxt = c + PF

        @pl.when(nxt < NCH)
        def _():
            @pl.when(nxt >= NS)
            def _():
                kv_out(nxt - NS, nxt % NS)[j].wait()
            kv_in(nxt, nxt % NS)[j].start()

    def arrived(c, j):
        kv_in(c, c % NS)[j].wait()

    arrived(0, 0)
    s0 = scores(0)
    turn(0, 0)

    def chunk(c, s):
        arrived(c + 1, 0)
        arrived(c, 1)
        sn = scores(c + 1)
        values(c, s)
        turn(c + 1, 0)
        turn(c, 1)
        return sn

    sl = lax.fori_loop(0, NCH - 1, chunk, s0)
    arrived(NCH - 1, 1)
    values(NCH - 1, sl)
    turn(NCH - 1, 1)
    for hd in range(G):
        o_v[:, hd * HD:(hd + 1) * HD] = o4[pl.ds(hd, B, stride=G), :].astype(BF16)
    ocopy = pltpu.make_async_copy(o_v, o_ref, xsem)
    ocopy.start()
    for c in range(NCH - NS, NCH):
        for t in kv_out(c, c % NS):
            t.wait()
    ocopy.wait()


def attn_call(layer, pos, x, nw, wq, wk, wv, kc, vc, prev):
    first = prev is None
    cache = jax.ShapeDtypeStruct(kc.shape, BF16)
    ins = [pos, x, nw, wq, wk, wv, kc, vc]
    specs = [ANY] * 8
    alias = {}
    if not first:
        alias = {len(ins): 1, len(ins) + 1: 2}
        ins += list(prev)
        specs += [ANY, ANY]
    return pl.pallas_call(
        functools.partial(attn_kernel, layer, first),
        name=f"attn{layer}",
        out_shape=(jax.ShapeDtypeStruct((B, QW), BF16), cache, cache),
        in_specs=specs,
        out_specs=(ANY, ANY, ANY),
        scratch_shapes=[
            pltpu.SMEM((B,), jnp.int32),
            pltpu.VMEM((2, D), BF16),
            pltpu.VMEM((B, D), BF16),
            pltpu.VMEM((B, D), BF16),
            pltpu.VMEM((S, HD), F32),
            pltpu.VMEM((S, HD), F32),
            pltpu.VMEM((B, HD), F32),
            pltpu.VMEM((B, HD), F32),
            pltpu.VMEM((D, QW), BF16),
            pltpu.VMEM((D, HD), BF16),
            pltpu.VMEM((D, HD), BF16),
            pltpu.VMEM((B, QW + 2 * HD), F32),
            pltpu.VMEM((B, QW + 2 * HD), BF16),
            pltpu.VMEM((B, QW), BF16),
            pltpu.VMEM((B * G, HD), F32),
            pltpu.VMEM((B * G, HD), F32),
            pltpu.VMEM((B, HD), F32),
            pltpu.VMEM((B, HD), F32),
            pltpu.VMEM((S, HD), BF16),
            pltpu.VMEM((NS, CB, S, HD), BF16),
            pltpu.VMEM((NS, CB, S, HD), BF16),
            pltpu.SemaphoreType.DMA((4, 3)),
            pltpu.SemaphoreType.DMA,
            pltpu.SemaphoreType.DMA((2,)),
            pltpu.SemaphoreType.DMA((NS,)),
            pltpu.SemaphoreType.DMA((NS,)),
            pltpu.SemaphoreType.DMA((NS,)),
            pltpu.SemaphoreType.DMA((NS,)),
        ],
        input_output_aliases=alias,
        compiler_params=pltpu.CompilerParams(vmem_limit_bytes=67043328),
    )(*ins)


def mlp_kernel(layer, last, o_hbm, x_hbm, nw_hbm, an_hbm, wo_hbm, wg_hbm, wu_hbm, wd_hbm, wq_hbm, wk_hbm, wv_hbm, *rest):
    if last:
        xo_hbm = rest[0]
        rest = rest[1:]
    else:
        xo_hbm, qkv_hbm = rest[:2]
        rest = rest[2:]
    (o_ref, nw_ref, an_ref, wo_v, wg_v, wu_v, wd_v, part, xg, hc, acc, a_v, qkv_v, xown, d2d, r1, r2, ssb, r_v,
     wsem, osem, xsem, isem, qsem, ssem, rsem) = rest
    me = lax.axis_index("tp")
    k = me % 2
    cx = (me // 2) % 2
    cy = me // 4
    pt = me + 1 - 2 * k
    xn = me + 2 - 4 * cx
    yn = me + 4 - 8 * cy
    dg = xn + 4 - 8 * cy

    def other(p):
        return p + 1 - 2 * k

    peers = (pt, xn, yn, dg, other(xn), other(yn), other(dg))
    order = (dg, xn, yn, me)
    top = pl.ds(0, HB)
    bot = pl.ds(HB, HB)

    def cols(p, h):
        return pl.ds(pl.multiple_of(p * PW + h * PH, PH), PH)

    def chip_cols(p):
        return pl.ds(pl.multiple_of((p // 2) * 2 * PW, 2 * PW), 2 * PW)

    barrier = pltpu.get_barrier_semaphore()
    for d in peers:
        pl.semaphore_signal(barrier, inc=1, device_id={"tp": d}, device_id_type=MESH)

    wos = [pltpu.make_async_copy(wo_hbm.at[layer, :, chip_cols(p)], wo_v.at[:, chip_cols(p)], osem.at[i]) for i, p in enumerate(order)]
    xcs = [pltpu.make_async_copy(x_hbm.at[h] if last else x_hbm.at[:, cols(me, h)], xown.at[h], xsem.at[h]) for h in range(2)]
    NG = 4
    gus = []
    for i in range(NG):
        rs = pl.ds(i * (D // NG), D // NG)
        gus.append(pltpu.make_async_copy(wg_hbm.at[layer, rs], wg_v.at[rs], wsem.at[2 * i]))
        gus.append(pltpu.make_async_copy(wu_hbm.at[layer, rs], wu_v.at[rs], wsem.at[2 * i + 1]))
    ND = 4
    wds = []
    for i in range(ND):
        rs = pl.ds(i * (FW // ND), FW // ND)
        wds.append(pltpu.make_async_copy(wd_hbm.at[layer, rs], wd_v.at[rs], wsem.at[2 * NG + i]))
    ocopy = pltpu.make_async_copy(o_hbm, o_ref, isem.at[0])
    ncopies = [pltpu.make_async_copy(nw_hbm, nw_ref, isem.at[1]), pltpu.make_async_copy(an_hbm, an_ref, isem.at[2])]
    for t in [ocopy] + wos[:2]:
        t.start()
    ocopy.wait()
    for t in wos[2:] + ncopies + xcs:
        t.start()

    def remote(src, dst, i, dev):
        return pltpu.make_async_remote_copy(src_ref=src, dst_ref=dst, send_sem=ssem.at[i], recv_sem=rsem.at[i],
                                            device_id={"tp": dev}, device_id_type=MESH)

    def send(src, dst, i, dev):
        c = remote(src, dst, i, dev)
        c.start()
        return c

    def reduce_scatter(make, enter=False):
        live = [{}, {}]

        def pair(h, t):
            c = live[h]
            p = order[t]
            c["d%d" % t].wait_recv()
            part[h, p] = (part[h, p].astype(F32) + d2d[h, t].astype(F32)).astype(BF16)
            if t == 0:
                c["a0"] = send(part.at[h, dg, top], r1.at[h, 0], NC * h + 4, xn)
                c["b0"] = send(part.at[h, dg, bot], r1.at[h, 2], NC * h + 5, yn)
            elif t == 1 and h == 0:
                c["a1"] = send(part.at[h, xn, top], r1.at[h, 1], NC * h + 6, xn)
            elif t == 2 and h == 0:
                c["b1"] = send(part.at[h, yn, bot], r1.at[h, 3], NC * h + 7, yn)

        todo = []
        for h in range(2):
            for t, p in enumerate(order):
                q = other(p)
                make(h, t, p, q)
                if enter and (h, t) == (0, 0):
                    pl.semaphore_wait(barrier, len(peers))
                live[h]["d%d" % t] = send(part.at[h, q], d2d.at[h, t], NC * h + t, pt)
                if todo:
                    pair(*todo.pop(0))
                todo.append((h, t))
        pair(*todo.pop(0))
        for h in range(2):
            c = live[h]
            c["a0"].wait_recv()
            part[h, yn, top] = (part[h, yn, top].astype(F32) + r1[h, 0].astype(F32)).astype(BF16)
            c["a2"] = send(part.at[h, yn, top], r2.at[h, 0], NC * h + 8, yn)
            c["b0"].wait_recv()
            part[h, xn, bot] = (part[h, xn, bot].astype(F32) + r1[h, 2].astype(F32)).astype(BF16)
            c["b2"] = send(part.at[h, xn, bot], r2.at[h, 1], NC * h + 9, xn)
            if h == 0:
                live[1]["a1"] = send(part.at[1, xn, top], r1.at[1, 1], NC + 6, xn)
                live[1]["b1"] = send(part.at[1, yn, bot], r1.at[1, 3], NC + 7, yn)
        return live

    def final(h, c):
        for rs, a, b, i, j in ((top, "a1", "a2", 1, 0), (bot, "b1", "b2", 3, 1)):
            c[a].wait_recv()
            c[b].wait_recv()
            tot = part[h, me, rs].astype(F32) + r1[h, i].astype(F32) + r2[h, j].astype(F32)
            new = (xown[h, rs].astype(F32) + tot.astype(BF16).astype(F32)).astype(BF16)
            xown[h, rs] = new
            xg[h, me, rs] = new

    def go(h, c, name, p, rs, i, dev):
        c[name] = send(xg.at[h, p, rs], xg.at[h, p, rs], NC * h + i, dev)

    def gather_first(h, c):
        go(h, c, "ga0", me, top, 10, yn)
        go(h, c, "gb0", me, bot, 11, xn)
        c["p0"] = send(xg.at[h, me], xg.at[h, me], NC * h + 14, pt)

    def gather_second(h, c):
        go(h, c, "ga1", me, top, 12, xn)
        go(h, c, "gb1", me, bot, 13, yn)

    def forward(h, c, got, name, p, rs, i):
        c[got].wait_recv()
        c[name] = send(xg.at[h, p, rs], xg.at[h, p, rs], NC * h + i, pt)

    def relay(h, c):
        forward(h, c, "ga0", "p1", yn, top, 15)
        c["ga2"] = send(xg.at[h, yn, top], xg.at[h, yn, top], NC * h + 16, xn)
        forward(h, c, "gb0", "p2", xn, bot, 17)
        c["gb2"] = send(xg.at[h, xn, bot], xg.at[h, xn, bot], NC * h + 18, yn)

    def near(h, c):
        forward(h, c, "ga1", "p3", xn, top, 19)
        forward(h, c, "gb1", "p4", yn, bot, 20)

    def far(h, c):
        forward(h, c, "ga2", "p5", dg, top, 21)
        forward(h, c, "gb2", "p6", dg, bot, 22)

    def drain(live):
        for c in live:
            for t in c.values():
                t.wait_send()

    def got(live, *names):
        for c in live:
            for n in names:
                c[n].wait_recv()

    def out_half(h, i, p, q):
        if h == 0:
            wos[i].wait()
            if i == 3:
                for t in gus:
                    t.start()
        w = jnp.concatenate([wo_v[:, cols(p, h)], wo_v[:, cols(q, h)]], axis=1)
        t = jnp.dot(o_ref[...], w, preferred_element_type=F32).astype(BF16)
        part[h, p] = t[:, :PH]
        part[h, q] = t[:, PH:]

    def square_start():
        sq = jnp.zeros((B, 128), F32)
        for h in range(2):
            for c in range(PH // 128):
                t = xg[h, me, :, c * 128:(c + 1) * 128].astype(F32)
                sq = sq + t * t
        ssb[0] = jnp.broadcast_to(jnp.sum(sq.T, axis=0, keepdims=True), (8, B))
        return [send(ssb.at[0], ssb.at[1 + j], 2 * NC + j, d) for j, d in enumerate(peers)]

    def square_end(sss):
        for t in sss:
            t.wait_recv()
        tot = ssb[0]
        for j in range(len(peers)):
            tot = tot + ssb[1 + j]
        rr = lax.rsqrt(tot * (1.0 / D) + 1e-5)
        r_v[...] = jnp.broadcast_to(rr[0:1], (128, B)).T

    def norm_rows_of(p, w_ref, row, first, n):
        base = pl.multiple_of((p // 2) * 2 * PW, 2 * PW)

        def norm_step(i, carry):
            sl = pl.ds(pl.multiple_of(first + i * 64, 64), 64)
            r = r_v[sl, :]
            for c in range(2 * PW // 128):
                cs = slice(c * 128, (c + 1) * 128)
                e, h, o = c // 4, (c // 2) % 2, (c % 2) * 128
                w = w_ref[row:row + 1, pl.ds(pl.multiple_of(base + c * 128, 128), 128)].astype(F32)
                hc[sl, cs] = (xg[h, (p // 2) * 2 + e, sl, o:o + 128].astype(F32) * r * w).astype(BF16)
            return carry

        lax.fori_loop(0, n // 64, norm_step, 0)
        return pl.ds(base, 2 * PW)

    def norm_chunk(ps, w_ref, row):
        if len(ps) == 1:
            return [norm_rows_of(ps[0], w_ref, row, 0, B)]
        return [norm_rows_of(p, w_ref, row, i * HB, HB) for i, p in enumerate(ps)]

    def chunk_dot(kss, weight):
        if len(kss) == 1:
            return jnp.dot(hc[...], weight(kss[0]), preferred_element_type=F32)
        return jnp.concatenate([jnp.dot(hc[i * HB:(i + 1) * HB, :], weight(ks), preferred_element_type=F32)
                                for i, ks in enumerate(kss)], axis=0)

    live = reduce_scatter(out_half, True)
    for t in xcs + ncopies:
        t.wait()
    final(0, live[0])
    gather_first(0, live[0])
    final(1, live[1])
    sss = square_start()
    gather_first(1, live[1])
    for h in range(2):
        gather_second(h, live[h])
    relay(0, live[0])
    square_end(sss)
    relay(1, live[1])
    for t in gus:
        t.wait()
    for t in wds:
        t.start()

    TN = 256

    def gate_up(ps, first, last, between={}):
        kss = norm_chunk(ps, nw_ref, layer)
        for j in range(FW // TN):
            cs = slice(j * TN, (j + 1) * TN)
            gu = chunk_dot(kss, lambda ks: jnp.concatenate([wg_v[ks, cs], wu_v[ks, cs]], axis=1))
            if not first:
                gu = gu + acc[j]
            if not last:
                acc[j] = gu
            else:
                gt = gu[:, :TN].astype(BF16).astype(F32)
                up = gu[:, TN:].astype(BF16).astype(F32)
                a_v[:, cs] = (gt * (1.0 / (1.0 + jnp.exp(-gt))) * up).astype(BF16)
            if j in between:
                between[j]()

    got(live, "p0")
    gate_up([me], True, False)
    near(0, live[0])

    def crossed(i, carry):
        for h in range(2):
            for n in (15 + 4 * i, 17 + 3 * i):
                remote(xg.at[h, me, top], xg.at[h, me, top], NC * h + n, pt).wait_recv()

        def sends():
            pl.when(i == 0)(lambda: near(1, dict(live[1])))
            pl.when(i == 1)(lambda: far(0, dict(live[0])))

        gate_up([yn + i * (xn - yn), xn + i * (yn - xn)], False, False, {2: sends})
        return carry

    lax.fori_loop(0, 2, crossed, 0)
    for h, name, p, rs, i in ((1, "p3", xn, top, 19), (1, "p4", yn, bot, 20), (0, "p5", dg, top, 21), (0, "p6", dg, bot, 22)):
        live[h][name] = remote(xg.at[h, p, rs], xg.at[h, p, rs], NC * h + i, pt)
    far(1, live[1])
    got(live, "p5", "p6")
    gate_up([dg], False, True)
    drain(live)
    for t in sss:
        t.wait_send()
    if not last:
        qs = []
        for i in range(2):
            rs = pl.ds(i * (D // 2), D // 2)
            qs += [pltpu.make_async_copy(wq_hbm.at[layer + 1, rs], wg_v.at[rs, pl.ds(0, QW)], qsem.at[i, 0]),
                   pltpu.make_async_copy(wk_hbm.at[layer + 1, rs], wg_v.at[rs, pl.ds(QW, HD)], qsem.at[i, 1]),
                   pltpu.make_async_copy(wv_hbm.at[layer + 1, rs], wg_v.at[rs, pl.ds(QW + HD, HD)], qsem.at[i, 2])]
    for t in wds:
        t.wait()
    if not last:
        for t in qs:
            t.start()

    def down_half(h, i, p, q):
        w = jnp.concatenate([wd_v[:, cols(p, h)], wd_v[:, cols(q, h)]], axis=1)
        t = jnp.dot(a_v[...], w, preferred_element_type=F32).astype(BF16)
        part[h, p] = t[:, :PH]
        part[h, q] = t[:, PH:]

    live = reduce_scatter(down_half)
    if last:
        for h in range(2):
            final(h, live[h])
            gather_first(h, live[h])
            gather_second(h, live[h])
        for h in range(2):
            relay(h, live[h])
        for h in range(2):
            near(h, live[h])
        outs = []

        def write(p):
            for e in range(2):
                for h in range(2):
                    n = (p // 2) * 2 + e
                    c = pltpu.make_async_copy(xg.at[h, n], xo_hbm.at[:, cols(n, h)], wsem.at[len(outs)])
                    c.start()
                    outs.append(c)

        got(live, "p0")
        write(me)
        for h in range(2):
            far(h, live[h])
        got(live, "p2", "p3")
        write(xn)
        got(live, "p1", "p4")
        write(yn)
        got(live, "p5", "p6")
        write(dg)
        drain(live)
        for c in outs:
            c.wait()
    else:
        final(0, live[0])
        gather_first(0, live[0])
        final(1, live[1])
        sss = square_start()
        gather_first(1, live[1])
        for h in range(2):
            gather_second(h, live[h])
        outs = [pltpu.make_async_copy(xown, xo_hbm, isem.at[0])]
        outs[0].start()
        relay(0, live[0])
        square_end(sss)
        relay(1, live[1])
        for h in range(2):
            near(h, live[h])
        for t in qs:
            t.wait()

        def qkv(ps, first, end):
            kss = norm_chunk(ps, an_ref, layer + 1)
            r = chunk_dot(kss, lambda ks: wg_v[ks, :QW + 2 * HD])
            if not first:
                r = r + jnp.concatenate([acc[0], acc[1, :, :2 * HD]], axis=1)
            if end:
                qkv_v[...] = r.astype(BF16)
            else:
                acc[0] = r[:, :QW]
                acc[1, :, :2 * HD] = r[:, QW:]

        got(live, "p0")
        qkv([me], True, False)
        got(live, "p1", "p2")
        qkv([yn, xn], False, False)
        far(0, live[0])
        got(live, "p3", "p4")
        qkv([xn, yn], False, False)
        far(1, live[1])
        got(live, "p5", "p6")
        qkv([dg], False, True)
        outs.append(pltpu.make_async_copy(qkv_v, qkv_hbm, isem.at[1]))
        outs[1].start()
        drain(live)
        for t in sss:
            t.wait_send()
        for c in outs:
            c.wait()


def mlp_call(layer, last, o, x, nw, an, wo, wg, wu, wd, wq, wk, wv):
    if last:
        out_shape = jax.ShapeDtypeStruct((B, D), BF16)
        out_specs = ANY
    else:
        out_shape = (jax.ShapeDtypeStruct((2, B, PH), BF16), jax.ShapeDtypeStruct((B, QW + 2 * HD), BF16))
        out_specs = (ANY, ANY)
    return pl.pallas_call(
        functools.partial(mlp_kernel, layer, last),
        name=f"mlp{layer}",
        out_shape=out_shape,
        in_specs=[ANY] * 11,
        out_specs=out_specs,
        scratch_shapes=[
            pltpu.VMEM((B, QW), BF16),
            pltpu.VMEM((2, D), BF16),
            pltpu.VMEM((2, D), BF16),
            pltpu.VMEM((QW, D), BF16),
            pltpu.VMEM((D, FW), BF16),
            pltpu.VMEM((D, FW), BF16),
            pltpu.VMEM((FW, D), BF16),
            pltpu.VMEM((2, NP, B, PH), BF16),
            pltpu.VMEM((2, NP, B, PH), BF16),
            pltpu.VMEM((B, 2 * PW), BF16),
            pltpu.VMEM((FW // 256, B, 512), F32),
            pltpu.VMEM((B, FW), BF16),
            pltpu.VMEM((B, QW + 2 * HD), BF16),
            pltpu.VMEM((2, B, PH), BF16),
            pltpu.VMEM((2, 4, B, PH), BF16),
            pltpu.VMEM((2, 4, HB, PH), BF16),
            pltpu.VMEM((2, 2, HB, PH), BF16),
            pltpu.VMEM((8, 8, B), F32),
            pltpu.VMEM((B, 128), F32),
            pltpu.SemaphoreType.DMA((16,)),
            pltpu.SemaphoreType.DMA((4,)),
            pltpu.SemaphoreType.DMA((2,)),
            pltpu.SemaphoreType.DMA((3,)),
            pltpu.SemaphoreType.DMA((2, 3)),
            pltpu.SemaphoreType.DMA((2 * NC + 7,)),
            pltpu.SemaphoreType.DMA((2 * NC + 7,)),
        ],
        compiler_params=pltpu.CompilerParams(collective_id=layer, has_side_effects=True, vmem_limit_bytes=67043328),
    )(o, x, nw, an, wo, wg, wu, wd, wq, wk, wv)


def copy_kernel(x_hbm, o_hbm, buf, isem, osem):
    n = buf.shape[0]
    rows = B // n
    ins = [pltpu.make_async_copy(x_hbm.at[pl.ds(i * rows, rows)], buf.at[i], isem.at[i]) for i in range(n)]
    outs = [pltpu.make_async_copy(buf.at[i], o_hbm.at[pl.ds(i * rows, rows)], osem.at[i]) for i in range(n)]
    for t in ins:
        t.start()
    for i in range(n):
        ins[i].wait()
        outs[i].start()
    for t in outs:
        t.wait()


def copy_call(x):
    n = 8
    return pl.pallas_call(
        copy_kernel,
        name="emit",
        out_shape=jax.ShapeDtypeStruct(x.shape, x.dtype),
        in_specs=[ANY],
        out_specs=ANY,
        scratch_shapes=[pltpu.VMEM((n, B // n, D), BF16), pltpu.SemaphoreType.DMA((n,)), pltpu.SemaphoreType.DMA((n,))],
        compiler_params=pltpu.CompilerParams(vmem_limit_bytes=67043328),
    )(x)


def solution(mesh):
    row_spec = P('dp', None)
    pos_spec = P('dp')
    cache_spec = P(None, 'dp', None, 'tp', None)
    norm_spec = P(None, None)
    col_spec = P(None, None, 'tp')
    split_rows = P(None, 'tp', None)

    def local_step(hidden, positions, k_cache, v_cache, attn_norm, w_query, w_key, w_value, w_out, mlp_norm, w_gate, w_up, w_down):
        kc = k_cache.reshape(2, B, S, HD)
        vc = v_cache.reshape(2, B, S, HD)
        x = hidden
        prev = None
        for layer in range(2):
            o, ko, vo = attn_call(layer, positions, x if layer == 0 else qkv, attn_norm, w_query, w_key, w_value, kc, vc, prev)
            prev = (ko, vo)
            y = mlp_call(layer, layer == 1, o, x, mlp_norm, attn_norm, w_out, w_gate, w_up, w_down, w_query, w_key, w_value)
            if layer == 0:
                x, qkv = y
            else:
                x = y
        return copy_call(x), prev[0].reshape(k_cache.shape), prev[1].reshape(v_cache.shape)

    return jax.shard_map(local_step, mesh=mesh, in_specs=(row_spec, pos_spec, cache_spec, cache_spec, norm_spec, col_spec, col_spec, col_spec, split_rows, norm_spec, col_spec, col_spec, split_rows), out_specs=(row_spec, cache_spec, cache_spec), check_vma=False)
```

```python
import functools
import math
import jax
import jax.numpy as jnp
from jax import lax
from jax.experimental import pallas as pl
from jax.experimental.pallas import tpu as pltpu
from jax.sharding import PartitionSpec as P

MESH = pl.DeviceIdType.MESH
F32 = jnp.float32
BF16 = jnp.bfloat16
ANY = pl.BlockSpec(memory_space=pl.ANY)
VMEM = pl.BlockSpec(memory_space=pltpu.VMEM)
SMEM = pl.BlockSpec(memory_space=pltpu.SMEM)

B = 256
D = 4096
S = 128
HD = 128
G = 4
QW = G * HD
NP = 8
PW = D // NP
FW = 1792
HB = B // 2
PH = PW // 2
NC = 23

CB = 32
NCH = B // CB
NS = 8
PF = 6


def rope_tables(shape):
    half = HD // 2
    lane = lax.broadcasted_iota(jnp.int32, shape, 1)
    index = jnp.where(lane < half, lane, lane - half).astype(F32)
    inv_freq = jnp.exp(index * (-2.0 / HD * math.log(500000.0)))
    wavelen = (2.0 * math.pi) / inv_freq
    smooth = (8192.0 / wavelen - 1.0) / 3.0
    blended = (1.0 - smooth) * inv_freq / 8.0 + smooth * inv_freq
    scaled = jnp.where(wavelen < 2048.0, inv_freq, jnp.where(wavelen > 8192.0, inv_freq / 8.0, blended))
    angles = lax.broadcasted_iota(jnp.int32, shape, 0).astype(F32) * scaled
    return jnp.cos(angles), jnp.where(lane < half, -1.0, 1.0) * jnp.sin(angles)


def norm_rows(x_ref, h_ref, w_ref, layer, rows=32):
    def step(i, carry):
        sl = pl.ds(pl.multiple_of(i * rows, rows), rows)
        acc = jnp.zeros((rows, 128), F32)
        for c in range(D // 128):
            t = x_ref[sl, c * 128:(c + 1) * 128].astype(F32)
            acc = acc + t * t
        r = lax.rsqrt(jnp.sum(acc, axis=1, keepdims=True) * (1.0 / D) + 1e-5)
        for c in range(D // 512):
            cs = slice(c * 512, (c + 1) * 512)
            h_ref[sl, cs] = (x_ref[sl, cs].astype(F32) * r * w_ref[layer:layer + 1, cs].astype(F32)).astype(BF16)
        return carry
    lax.fori_loop(0, B // rows, step, 0, unroll=2)


def attn_kernel(layer, first, pos_hbm, x_hbm, nw_hbm, wq_hbm, wk_hbm, wv_hbm, kc_hbm, vc_hbm, *rest):
    if first:
        o_ref, ko_hbm, vo_hbm = rest[:3]
        rest = rest[3:]
    else:
        o_ref, ko_hbm, vo_hbm = rest[2:5]
        rest = rest[5:]
    pos_ref, nw_ref, x_v, h_v, cos_t, sin_t, cos_ref, sin_ref, wq_v, wk_v, wv_v, acc, qkv_v, o_v, q4, o4, kn, vn, rid, kb, vb, wsem, xsem, psem, ksem, vsem, kosem, vosem = rest

    def kv_in(c, slot):
        rs = pl.ds(c * CB, CB)
        return (pltpu.make_async_copy(kc_hbm.at[layer, rs], kb.at[slot], ksem.at[slot]),
                pltpu.make_async_copy(vc_hbm.at[layer, rs], vb.at[slot], vsem.at[slot]))

    def kv_out(c, slot):
        rs = pl.ds(c * CB, CB)
        return (pltpu.make_async_copy(kb.at[slot], ko_hbm.at[layer, rs], kosem.at[slot]),
                pltpu.make_async_copy(vb.at[slot], vo_hbm.at[layer, rs], vosem.at[slot]))

    poscopy = pltpu.make_async_copy(pos_hbm, pos_ref, psem.at[0])
    poscopy.start()
    KC = D // 4
    if first:
        xcopy = pltpu.make_async_copy(x_hbm, x_v, xsem)
        xcopy.start()
        nwcopy = pltpu.make_async_copy(nw_hbm, nw_ref, psem.at[1])
        nwcopy.start()
        wcopies = []
        for c in range(4):
            rs = pl.ds(c * KC, KC)
            wcopies.append([pltpu.make_async_copy(wq_hbm.at[layer, rs], wq_v.at[rs], wsem.at[c, 0]),
                            pltpu.make_async_copy(wk_hbm.at[layer, rs], wk_v.at[rs], wsem.at[c, 1]),
                            pltpu.make_async_copy(wv_hbm.at[layer, rs], wv_v.at[rs], wsem.at[c, 2])])
        for t in wcopies[0]:
            t.start()
    else:
        xcopy = pltpu.make_async_copy(x_hbm, qkv_v, xsem)
        xcopy.start()
        for c in range(PF):
            for t in kv_in(c, c):
                t.start()

    rid[...] = lax.broadcasted_iota(jnp.int32, (S, HD), 0).astype(F32).astype(BF16)
    cos_t[...], sin_t[...] = rope_tables((S, HD))

    def look_up(b, carry):
        p = pos_ref[b]
        cos_ref[pl.ds(b, 1), :] = cos_t[pl.ds(p, 1), :]
        sin_ref[pl.ds(b, 1), :] = sin_t[pl.ds(p, 1), :]
        return carry

    poscopy.wait()
    lax.fori_loop(0, B, look_up, 0, unroll=8)
    xcopy.wait()
    if first:
        nwcopy.wait()
        for cs in wcopies[1:]:
            for t in cs:
                t.start()
        norm_rows(x_v, h_v, nw_ref, layer)
        for c in range(PF):
            for t in kv_in(c, c):
                t.start()
        for c in range(4):
            for t in wcopies[c]:
                t.wait()
            rs = slice(c * KC, (c + 1) * KC)
            w = jnp.concatenate([wq_v[rs, :], wk_v[rs, :], wv_v[rs, :]], axis=1)
            r = jnp.dot(h_v[:, rs], w, preferred_element_type=F32)
            if c == 0:
                acc[...] = r
            else:
                acc[...] += r
        qkv = acc
    else:
        qkv = qkv_v

    cos = cos_ref[...]
    sin = sin_ref[...]

    def rope(t):
        t = t.astype(BF16).astype(F32)
        return (t * cos + pltpu.roll(t, HD // 2, 1) * sin).astype(BF16).astype(F32)

    for hd in range(G):
        q4[pl.ds(hd, B, stride=G), :] = rope(qkv[:, hd * HD:(hd + 1) * HD])
    kn[...] = rope(qkv[:, QW:QW + HD])
    vn[...] = qkv[:, QW + HD:QW + 2 * HD].astype(BF16).astype(F32)

    scale = HD ** -0.5
    row = lax.broadcasted_iota(jnp.int32, (4 * G, HD), 0) // G
    lane = lax.broadcasted_iota(jnp.int32, (CB * G, HD), 1)
    even = (row % 2) == 0
    low = row < 2

    def place(buf, new, slot, b0, i, rowid):
        hit = rowid == jnp.full((S, HD), pos_ref[b0 + i].astype(F32), F32).astype(BF16)
        r = jnp.broadcast_to(new[pl.ds(b0 + i, 1), :], (S, HD)).astype(BF16)
        t = jnp.where(hit, r, buf[slot, i])
        buf[slot, i] = t
        return t

    def quad(ts):
        return jnp.concatenate([jnp.concatenate(ts[:2], axis=1), jnp.concatenate(ts[2:], axis=1)], axis=0)

    def scores(c):
        slot = c % NS
        b0 = c * CB
        rowid = rid[...]
        out = []
        for g in range(CB // 4):
            kt = quad([place(kb, kn, slot, b0, 4 * g + i, rowid) for i in range(4)])
            q = q4[pl.ds(pl.multiple_of(b0 * G + 4 * G * g, 4 * G), 4 * G), :]
            lhs = jnp.concatenate([jnp.where(even, q, 0.0), jnp.where(even, 0.0, q)], axis=1).astype(BF16)
            s2 = lax.dot_general(lhs, kt, (((1,), (1,)), ((), ())), preferred_element_type=F32)
            out.append(jnp.where(low, s2[:, :S], s2[:, S:]))
        return jnp.concatenate(out, axis=0)

    def values(c, s):
        slot = c % NS
        b0 = c * CB
        rowid = rid[...]
        posr = []
        for g in range(CB // 4):
            t = jnp.zeros((4 * G, HD), jnp.int32)
            for i in range(4):
                t = jnp.where(row == i, pos_ref[b0 + 4 * g + i], t)
            posr.append(t)
        s = jnp.where(lane <= jnp.concatenate(posr, axis=0), s * scale, -jnp.inf)
        e = jnp.exp(s - jnp.max(s, axis=1, keepdims=True))
        p = e / jnp.sum(e, axis=1, keepdims=True)
        for g in range(CB // 4):
            vt = quad([place(vb, vn, slot, b0, 4 * g + i, rowid) for i in range(4)])
            pg = p[4 * G * g:4 * G * (g + 1)]
            lhs = jnp.concatenate([jnp.where(low, pg, 0.0), jnp.where(low, 0.0, pg)], axis=1).astype(BF16)
            o2 = jnp.dot(lhs, vt, preferred_element_type=F32)
            o4[pl.ds(pl.multiple_of(b0 * G + 4 * G * g, 4 * G), 4 * G), :] = jnp.where(even, o2[:, :HD], o2[:, HD:])

    def turn(c, j):
        kv_out(c, c % NS)[j].start()
        nxt = c + PF

        @pl.when(nxt < NCH)
        def _():
            @pl.when(nxt >= NS)
            def _():
                kv_out(nxt - NS, nxt % NS)[j].wait()
            kv_in(nxt, nxt % NS)[j].start()

    def arrived(c, j):
        kv_in(c, c % NS)[j].wait()

    arrived(0, 0)
    s0 = scores(0)
    turn(0, 0)

    def chunk(c, s):
        arrived(c + 1, 0)
        arrived(c, 1)
        sn = scores(c + 1)
        values(c, s)
        turn(c + 1, 0)
        turn(c, 1)
        return sn

    sl = lax.fori_loop(0, NCH - 1, chunk, s0)
    arrived(NCH - 1, 1)
    values(NCH - 1, sl)
    turn(NCH - 1, 1)
    for hd in range(G):
        o_v[:, hd * HD:(hd + 1) * HD] = o4[pl.ds(hd, B, stride=G), :].astype(BF16)
    ocopy = pltpu.make_async_copy(o_v, o_ref, xsem)
    ocopy.start()
    for c in range(NCH - NS, NCH):
        for t in kv_out(c, c % NS):
            t.wait()
    ocopy.wait()


def attn_call(layer, pos, x, nw, wq, wk, wv, kc, vc, prev):
    first = prev is None
    cache = jax.ShapeDtypeStruct(kc.shape, BF16)
    ins = [pos, x, nw, wq, wk, wv, kc, vc]
    specs = [ANY] * 8
    alias = {}
    if not first:
        alias = {len(ins): 1, len(ins) + 1: 2}
        ins += list(prev)
        specs += [ANY, ANY]
    return pl.pallas_call(
        functools.partial(attn_kernel, layer, first),
        name=f"attn{layer}",
        out_shape=(jax.ShapeDtypeStruct((B, QW), BF16), cache, cache),
        in_specs=specs,
        out_specs=(ANY, ANY, ANY),
        scratch_shapes=[
            pltpu.SMEM((B,), jnp.int32),
            pltpu.VMEM((2, D), BF16),
            pltpu.VMEM((B, D), BF16),
            pltpu.VMEM((B, D), BF16),
            pltpu.VMEM((S, HD), F32),
            pltpu.VMEM((S, HD), F32),
            pltpu.VMEM((B, HD), F32),
            pltpu.VMEM((B, HD), F32),
            pltpu.VMEM((D, QW), BF16),
            pltpu.VMEM((D, HD), BF16),
            pltpu.VMEM((D, HD), BF16),
            pltpu.VMEM((B, QW + 2 * HD), F32),
            pltpu.VMEM((B, QW + 2 * HD), BF16),
            pltpu.VMEM((B, QW), BF16),
            pltpu.VMEM((B * G, HD), F32),
            pltpu.VMEM((B * G, HD), F32),
            pltpu.VMEM((B, HD), F32),
            pltpu.VMEM((B, HD), F32),
            pltpu.VMEM((S, HD), BF16),
            pltpu.VMEM((NS, CB, S, HD), BF16),
            pltpu.VMEM((NS, CB, S, HD), BF16),
            pltpu.SemaphoreType.DMA((4, 3)),
            pltpu.SemaphoreType.DMA,
            pltpu.SemaphoreType.DMA((2,)),
            pltpu.SemaphoreType.DMA((NS,)),
            pltpu.SemaphoreType.DMA((NS,)),
            pltpu.SemaphoreType.DMA((NS,)),
            pltpu.SemaphoreType.DMA((NS,)),
        ],
        input_output_aliases=alias,
        compiler_params=pltpu.CompilerParams(vmem_limit_bytes=67043328),
    )(*ins)


def mlp_kernel(layer, last, o_hbm, x_hbm, nw_hbm, an_hbm, wo_hbm, wg_hbm, wu_hbm, wd_hbm, wq_hbm, wk_hbm, wv_hbm, *rest):
    if last:
        xo_hbm = rest[0]
        rest = rest[1:]
    else:
        xo_hbm, qkv_hbm = rest[:2]
        rest = rest[2:]
    (o_ref, nw_ref, an_ref, wo_v, wg_v, wu_v, wd_v, part, xg, hc, acc, a_v, qkv_v, xown, d2d, r1, r2, ssb, r_v,
     wsem, osem, xsem, isem, qsem, ssem, rsem) = rest
    me = lax.axis_index("tp")
    k = me % 2
    cx = (me // 2) % 2
    cy = me // 4
    pt = me + 1 - 2 * k
    xn = me + 2 - 4 * cx
    yn = me + 4 - 8 * cy
    dg = xn + 4 - 8 * cy

    def other(p):
        return p + 1 - 2 * k

    peers = (pt, xn, yn, dg, other(xn), other(yn), other(dg))
    order = (dg, xn, yn, me)
    top = pl.ds(0, HB)
    bot = pl.ds(HB, HB)

    def cols(p, h):
        return pl.ds(pl.multiple_of(p * PW + h * PH, PH), PH)

    def chip_cols(p):
        return pl.ds(pl.multiple_of((p // 2) * 2 * PW, 2 * PW), 2 * PW)

    barrier = pltpu.get_barrier_semaphore()
    for d in peers:
        pl.semaphore_signal(barrier, inc=1, device_id={"tp": d}, device_id_type=MESH)

    wos = [pltpu.make_async_copy(wo_hbm.at[layer, :, chip_cols(p)], wo_v.at[:, chip_cols(p)], osem.at[i]) for i, p in enumerate(order)]
    xcs = [pltpu.make_async_copy(x_hbm.at[h] if last else x_hbm.at[:, cols(me, h)], xown.at[h], xsem.at[h]) for h in range(2)]
    NG = 4
    gus = []
    for i in range(NG):
        rs = pl.ds(i * (D // NG), D // NG)
        gus.append(pltpu.make_async_copy(wg_hbm.at[layer, rs], wg_v.at[rs], wsem.at[2 * i]))
        gus.append(pltpu.make_async_copy(wu_hbm.at[layer, rs], wu_v.at[rs], wsem.at[2 * i + 1]))
    ND = 4
    wds = []
    for i in range(ND):
        rs = pl.ds(i * (FW // ND), FW // ND)
        wds.append(pltpu.make_async_copy(wd_hbm.at[layer, rs], wd_v.at[rs], wsem.at[2 * NG + i]))
    ocopy = pltpu.make_async_copy(o_hbm, o_ref, isem.at[0])
    ncopies = [pltpu.make_async_copy(nw_hbm, nw_ref, isem.at[1]), pltpu.make_async_copy(an_hbm, an_ref, isem.at[2])]
    for t in [ocopy] + wos + ncopies + xcs:
        t.start()
    ocopy.wait()

    def remote(src, dst, i, dev):
        return pltpu.make_async_remote_copy(src_ref=src, dst_ref=dst, send_sem=ssem.at[i], recv_sem=rsem.at[i],
                                            device_id={"tp": dev}, device_id_type=MESH)

    def send(src, dst, i, dev):
        c = remote(src, dst, i, dev)
        c.start()
        return c

    def reduce_scatter(make, enter=False):
        live = [{}, {}]

        def pair(h, t):
            c = live[h]
            p = order[t]
            c["d%d" % t].wait_recv()
            part[h, p] = (part[h, p].astype(F32) + d2d[h, t].astype(F32)).astype(BF16)
            if t == 0:
                c["a0"] = send(part.at[h, dg, top], r1.at[h, 0], NC * h + 4, xn)
                c["b0"] = send(part.at[h, dg, bot], r1.at[h, 2], NC * h + 5, yn)
            elif t == 1:
                c["a1"] = send(part.at[h, xn, top], r1.at[h, 1], NC * h + 6, xn)
            elif t == 2:
                c["b1"] = send(part.at[h, yn, bot], r1.at[h, 3], NC * h + 7, yn)

        todo = []
        for h in range(2):
            for t, p in enumerate(order):
                q = other(p)
                make(h, t, p, q)
                if enter and (h, t) == (0, 0):
                    pl.semaphore_wait(barrier, len(peers))
                live[h]["d%d" % t] = send(part.at[h, q], d2d.at[h, t], NC * h + t, pt)
                if todo:
                    pair(*todo.pop(0))
                todo.append((h, t))
        pair(*todo.pop(0))
        for h in range(2):
            c = live[h]
            c["a0"].wait_recv()
            part[h, yn, top] = (part[h, yn, top].astype(F32) + r1[h, 0].astype(F32)).astype(BF16)
            c["a2"] = send(part.at[h, yn, top], r2.at[h, 0], NC * h + 8, yn)
            c["b0"].wait_recv()
            part[h, xn, bot] = (part[h, xn, bot].astype(F32) + r1[h, 2].astype(F32)).astype(BF16)
            c["b2"] = send(part.at[h, xn, bot], r2.at[h, 1], NC * h + 9, xn)
        return live

    def final(h, c):
        for rs, a, b, i, j in ((top, "a1", "a2", 1, 0), (bot, "b1", "b2", 3, 1)):
            c[a].wait_recv()
            c[b].wait_recv()
            tot = part[h, me, rs].astype(F32) + r1[h, i].astype(F32) + r2[h, j].astype(F32)
            new = (xown[h, rs].astype(F32) + tot.astype(BF16).astype(F32)).astype(BF16)
            xown[h, rs] = new
            xg[h, me, rs] = new

    def go(h, c, name, p, rs, i, dev):
        c[name] = send(xg.at[h, p, rs], xg.at[h, p, rs], NC * h + i, dev)

    def gather_first(h, c):
        go(h, c, "ga0", me, top, 10, yn)
        go(h, c, "gb0", me, bot, 11, xn)
        c["p0"] = send(xg.at[h, me], xg.at[h, me], NC * h + 14, pt)

    def gather_second(h, c):
        go(h, c, "ga1", me, top, 12, xn)
        go(h, c, "gb1", me, bot, 13, yn)

    def forward(h, c, got, name, p, rs, i):
        c[got].wait_recv()
        c[name] = send(xg.at[h, p, rs], xg.at[h, p, rs], NC * h + i, pt)

    def relay(h, c):
        forward(h, c, "ga0", "p1", yn, top, 15)
        c["ga2"] = send(xg.at[h, yn, top], xg.at[h, yn, top], NC * h + 16, xn)
        forward(h, c, "gb0", "p2", xn, bot, 17)
        c["gb2"] = send(xg.at[h, xn, bot], xg.at[h, xn, bot], NC * h + 18, yn)

    def near(h, c):
        forward(h, c, "ga1", "p3", xn, top, 19)
        forward(h, c, "gb1", "p4", yn, bot, 20)

    def far(h, c):
        forward(h, c, "ga2", "p5", dg, top, 21)
        forward(h, c, "gb2", "p6", dg, bot, 22)

    def drain(live):
        for c in live:
            for t in c.values():
                t.wait_send()

    def got(live, *names):
        for c in live:
            for n in names:
                c[n].wait_recv()

    def out_half(h, i, p, q):
        if h == 0:
            wos[i].wait()
            if i == 3:
                for t in gus:
                    t.start()
        w = jnp.concatenate([wo_v[:, cols(p, h)], wo_v[:, cols(q, h)]], axis=1)
        t = jnp.dot(o_ref[...], w, preferred_element_type=F32).astype(BF16)
        part[h, p] = t[:, :PH]
        part[h, q] = t[:, PH:]

    def square_start():
        sq = jnp.zeros((B, 128), F32)
        for h in range(2):
            for c in range(PH // 128):
                t = xg[h, me, :, c * 128:(c + 1) * 128].astype(F32)
                sq = sq + t * t
        ssb[0] = jnp.broadcast_to(jnp.sum(sq.T, axis=0, keepdims=True), (8, B))
        return [send(ssb.at[0], ssb.at[1 + j], 2 * NC + j, d) for j, d in enumerate(peers)]

    def square_end(sss):
        for t in sss:
            t.wait_recv()
        tot = ssb[0]
        for j in range(len(peers)):
            tot = tot + ssb[1 + j]
        rr = lax.rsqrt(tot * (1.0 / D) + 1e-5)
        r_v[...] = jnp.broadcast_to(rr[0:1], (128, B)).T

    def norm_rows_of(p, w_ref, row, first, n):
        base = pl.multiple_of((p // 2) * 2 * PW, 2 * PW)

        def norm_step(i, carry):
            sl = pl.ds(pl.multiple_of(first + i * 64, 64), 64)
            r = r_v[sl, :]
            for c in range(2 * PW // 128):
                cs = slice(c * 128, (c + 1) * 128)
                e, h, o = c // 4, (c // 2) % 2, (c % 2) * 128
                w = w_ref[row:row + 1, pl.ds(pl.multiple_of(base + c * 128, 128), 128)].astype(F32)
                hc[sl, cs] = (xg[h, (p // 2) * 2 + e, sl, o:o + 128].astype(F32) * r * w).astype(BF16)
            return carry

        lax.fori_loop(0, n // 64, norm_step, 0)
        return pl.ds(base, 2 * PW)

    def norm_chunk(ps, w_ref, row):
        if len(ps) == 1:
            return [norm_rows_of(ps[0], w_ref, row, 0, B)]
        return [norm_rows_of(p, w_ref, row, i * HB, HB) for i, p in enumerate(ps)]

    def chunk_dot(kss, weight):
        if len(kss) == 1:
            return jnp.dot(hc[...], weight(kss[0]), preferred_element_type=F32)
        return jnp.concatenate([jnp.dot(hc[i * HB:(i + 1) * HB, :], weight(ks), preferred_element_type=F32)
                                for i, ks in enumerate(kss)], axis=0)

    live = reduce_scatter(out_half, True)
    for t in xcs + ncopies:
        t.wait()
    final(0, live[0])
    gather_first(0, live[0])
    final(1, live[1])
    sss = square_start()
    gather_first(1, live[1])
    for h in range(2):
        gather_second(h, live[h])
    relay(0, live[0])
    square_end(sss)
    relay(1, live[1])
    for t in gus:
        t.wait()
    for t in wds:
        t.start()

    TN = 256

    def gate_up(ps, first, last, between={}):
        kss = norm_chunk(ps, nw_ref, layer)
        for j in range(FW // TN):
            cs = slice(j * TN, (j + 1) * TN)
            gu = chunk_dot(kss, lambda ks: jnp.concatenate([wg_v[ks, cs], wu_v[ks, cs]], axis=1))
            if not first:
                gu = gu + acc[j]
            if not last:
                acc[j] = gu
            else:
                gt = gu[:, :TN].astype(BF16).astype(F32)
                up = gu[:, TN:].astype(BF16).astype(F32)
                a_v[:, cs] = (gt * (1.0 / (1.0 + jnp.exp(-gt))) * up).astype(BF16)
            if j in between:
                between[j]()

    got(live, "p0")
    gate_up([me], True, False)
    near(0, live[0])

    def crossed(i, carry):
        for h in range(2):
            for n in (15 + 4 * i, 17 + 3 * i):
                remote(xg.at[h, me, top], xg.at[h, me, top], NC * h + n, pt).wait_recv()

        def sends():
            pl.when(i == 0)(lambda: near(1, dict(live[1])))
            pl.when(i == 1)(lambda: far(0, dict(live[0])))

        gate_up([yn + i * (xn - yn), xn + i * (yn - xn)], False, False, {2: sends})
        return carry

    lax.fori_loop(0, 2, crossed, 0)
    for h, name, p, rs, i in ((1, "p3", xn, top, 19), (1, "p4", yn, bot, 20), (0, "p5", dg, top, 21), (0, "p6", dg, bot, 22)):
        live[h][name] = remote(xg.at[h, p, rs], xg.at[h, p, rs], NC * h + i, pt)
    far(1, live[1])
    got(live, "p5", "p6")
    gate_up([dg], False, True)
    drain(live)
    for t in sss:
        t.wait_send()
    if not last:
        qs = []
        for i in range(2):
            rs = pl.ds(i * (D // 2), D // 2)
            qs += [pltpu.make_async_copy(wq_hbm.at[layer + 1, rs], wg_v.at[rs, pl.ds(0, QW)], qsem.at[i, 0]),
                   pltpu.make_async_copy(wk_hbm.at[layer + 1, rs], wg_v.at[rs, pl.ds(QW, HD)], qsem.at[i, 1]),
                   pltpu.make_async_copy(wv_hbm.at[layer + 1, rs], wg_v.at[rs, pl.ds(QW + HD, HD)], qsem.at[i, 2])]
    for t in wds:
        t.wait()
    if not last:
        for t in qs:
            t.start()

    def down_half(h, i, p, q):
        w = jnp.concatenate([wd_v[:, cols(p, h)], wd_v[:, cols(q, h)]], axis=1)
        t = jnp.dot(a_v[...], w, preferred_element_type=F32).astype(BF16)
        part[h, p] = t[:, :PH]
        part[h, q] = t[:, PH:]

    live = reduce_scatter(down_half)
    if last:
        for h in range(2):
            final(h, live[h])
            gather_first(h, live[h])
            gather_second(h, live[h])
        for h in range(2):
            relay(h, live[h])
        for h in range(2):
            near(h, live[h])
        outs = []

        def write(p):
            for e in range(2):
                for h in range(2):
                    n = (p // 2) * 2 + e
                    c = pltpu.make_async_copy(xg.at[h, n], xo_hbm.at[:, cols(n, h)], wsem.at[len(outs)])
                    c.start()
                    outs.append(c)

        got(live, "p0")
        write(me)
        for h in range(2):
            far(h, live[h])
        got(live, "p2", "p3")
        write(xn)
        got(live, "p1", "p4")
        write(yn)
        got(live, "p5", "p6")
        write(dg)
        drain(live)
        for c in outs:
            c.wait()
    else:
        final(0, live[0])
        gather_first(0, live[0])
        gather_second(0, live[0])
        final(1, live[1])
        sss = square_start()
        gather_first(1, live[1])
        gather_second(1, live[1])
        outs = [pltpu.make_async_copy(xown, xo_hbm, isem.at[0])]
        outs[0].start()
        relay(0, live[0])
        near(0, live[0])
        square_end(sss)
        relay(1, live[1])
        for t in qs:
            t.wait()

        def qkv(ps, first, end):
            kss = norm_chunk(ps, an_ref, layer + 1)
            r = chunk_dot(kss, lambda ks: wg_v[ks, :QW + 2 * HD])
            if not first:
                r = r + jnp.concatenate([acc[0], acc[1, :, :2 * HD]], axis=1)
            if end:
                qkv_v[...] = r.astype(BF16)
            else:
                acc[0] = r[:, :QW]
                acc[1, :, :2 * HD] = r[:, QW:]

        got(live, "p0")
        qkv([me], True, False)
        near(1, live[1])
        got(live, "p1", "p2")
        qkv([yn, xn], False, False)
        far(0, live[0])
        got(live, "p3", "p4")
        qkv([xn, yn], False, False)
        far(1, live[1])
        got(live, "p5", "p6")
        qkv([dg], False, True)
        outs.append(pltpu.make_async_copy(qkv_v, qkv_hbm, isem.at[1]))
        outs[1].start()
        drain(live)
        for t in sss:
            t.wait_send()
        for c in outs:
            c.wait()


def mlp_call(layer, last, o, x, nw, an, wo, wg, wu, wd, wq, wk, wv):
    if last:
        out_shape = jax.ShapeDtypeStruct((B, D), BF16)
        out_specs = ANY
    else:
        out_shape = (jax.ShapeDtypeStruct((2, B, PH), BF16), jax.ShapeDtypeStruct((B, QW + 2 * HD), BF16))
        out_specs = (ANY, ANY)
    return pl.pallas_call(
        functools.partial(mlp_kernel, layer, last),
        name=f"mlp{layer}",
        out_shape=out_shape,
        in_specs=[ANY] * 11,
        out_specs=out_specs,
        scratch_shapes=[
            pltpu.VMEM((B, QW), BF16),
            pltpu.VMEM((2, D), BF16),
            pltpu.VMEM((2, D), BF16),
            pltpu.VMEM((QW, D), BF16),
            pltpu.VMEM((D, FW), BF16),
            pltpu.VMEM((D, FW), BF16),
            pltpu.VMEM((FW, D), BF16),
            pltpu.VMEM((2, NP, B, PH), BF16),
            pltpu.VMEM((2, NP, B, PH), BF16),
            pltpu.VMEM((B, 2 * PW), BF16),
            pltpu.VMEM((FW // 256, B, 512), F32),
            pltpu.VMEM((B, FW), BF16),
            pltpu.VMEM((B, QW + 2 * HD), BF16),
            pltpu.VMEM((2, B, PH), BF16),
            pltpu.VMEM((2, 4, B, PH), BF16),
            pltpu.VMEM((2, 4, HB, PH), BF16),
            pltpu.VMEM((2, 2, HB, PH), BF16),
            pltpu.VMEM((8, 8, B), F32),
            pltpu.VMEM((B, 128), F32),
            pltpu.SemaphoreType.DMA((16,)),
            pltpu.SemaphoreType.DMA((4,)),
            pltpu.SemaphoreType.DMA((2,)),
            pltpu.SemaphoreType.DMA((3,)),
            pltpu.SemaphoreType.DMA((2, 3)),
            pltpu.SemaphoreType.DMA((2 * NC + 7,)),
            pltpu.SemaphoreType.DMA((2 * NC + 7,)),
        ],
        compiler_params=pltpu.CompilerParams(collective_id=layer, has_side_effects=True, vmem_limit_bytes=67043328),
    )(o, x, nw, an, wo, wg, wu, wd, wq, wk, wv)


def copy_kernel(x_hbm, o_hbm, buf, isem, osem):
    n = buf.shape[0]
    rows = B // n
    ins = [pltpu.make_async_copy(x_hbm.at[pl.ds(i * rows, rows)], buf.at[i], isem.at[i]) for i in range(n)]
    outs = [pltpu.make_async_copy(buf.at[i], o_hbm.at[pl.ds(i * rows, rows)], osem.at[i]) for i in range(n)]
    for t in ins:
        t.start()
    for i in range(n):
        ins[i].wait()
        outs[i].start()
    for t in outs:
        t.wait()


def copy_call(x):
    n = 8
    return pl.pallas_call(
        copy_kernel,
        name="emit",
        out_shape=jax.ShapeDtypeStruct(x.shape, x.dtype),
        in_specs=[ANY],
        out_specs=ANY,
        scratch_shapes=[pltpu.VMEM((n, B // n, D), BF16), pltpu.SemaphoreType.DMA((n,)), pltpu.SemaphoreType.DMA((n,))],
        compiler_params=pltpu.CompilerParams(vmem_limit_bytes=67043328),
    )(x)


def solution(mesh):
    row_spec = P('dp', None)
    pos_spec = P('dp')
    cache_spec = P(None, 'dp', None, 'tp', None)
    norm_spec = P(None, None)
    col_spec = P(None, None, 'tp')
    split_rows = P(None, 'tp', None)

    def local_step(hidden, positions, k_cache, v_cache, attn_norm, w_query, w_key, w_value, w_out, mlp_norm, w_gate, w_up, w_down):
        kc = k_cache.reshape(2, B, S, HD)
        vc = v_cache.reshape(2, B, S, HD)
        x = hidden
        prev = None
        for layer in range(2):
            o, ko, vo = attn_call(layer, positions, x if layer == 0 else qkv, attn_norm, w_query, w_key, w_value, kc, vc, prev)
            prev = (ko, vo)
            y = mlp_call(layer, layer == 1, o, x, mlp_norm, attn_norm, w_out, w_gate, w_up, w_down, w_query, w_key, w_value)
            if layer == 0:
                x, qkv = y
            else:
                x = y
        return copy_call(x), prev[0].reshape(k_cache.shape), prev[1].reshape(v_cache.shape)

    return jax.shard_map(local_step, mesh=mesh, in_specs=(row_spec, pos_spec, cache_spec, cache_spec, norm_spec, col_spec, col_spec, col_spec, split_rows, norm_spec, col_spec, col_spec, split_rows), out_specs=(row_spec, cache_spec, cache_spec), check_vma=False)
```

```python
import functools
import math
import jax
import jax.numpy as jnp
from jax import lax
from jax.experimental import pallas as pl
from jax.experimental.pallas import tpu as pltpu
from jax.sharding import PartitionSpec as P

MESH = pl.DeviceIdType.MESH
F32 = jnp.float32
BF16 = jnp.bfloat16
ANY = pl.BlockSpec(memory_space=pl.ANY)
VMEM = pl.BlockSpec(memory_space=pltpu.VMEM)
SMEM = pl.BlockSpec(memory_space=pltpu.SMEM)

B = 256
D = 4096
S = 128
HD = 128
G = 4
QW = G * HD
NP = 8
PW = D // NP
FW = 1792
HB = B // 2
PH = PW // 2
NC = 23

CB = 32
NCH = B // CB
NS = 8
PF = 6


def rope_tables(shape):
    half = HD // 2
    lane = lax.broadcasted_iota(jnp.int32, shape, 1)
    index = jnp.where(lane < half, lane, lane - half).astype(F32)
    inv_freq = jnp.exp(index * (-2.0 / HD * math.log(500000.0)))
    wavelen = (2.0 * math.pi) / inv_freq
    smooth = (8192.0 / wavelen - 1.0) / 3.0
    blended = (1.0 - smooth) * inv_freq / 8.0 + smooth * inv_freq
    scaled = jnp.where(wavelen < 2048.0, inv_freq, jnp.where(wavelen > 8192.0, inv_freq / 8.0, blended))
    angles = lax.broadcasted_iota(jnp.int32, shape, 0).astype(F32) * scaled
    return jnp.cos(angles), jnp.where(lane < half, -1.0, 1.0) * jnp.sin(angles)


def norm_rows(x_ref, h_ref, w_ref, layer, rows=32):
    def step(i, carry):
        sl = pl.ds(pl.multiple_of(i * rows, rows), rows)
        acc = jnp.zeros((rows, 128), F32)
        for c in range(D // 128):
            t = x_ref[sl, c * 128:(c + 1) * 128].astype(F32)
            acc = acc + t * t
        r = lax.rsqrt(jnp.sum(acc, axis=1, keepdims=True) * (1.0 / D) + 1e-5)
        for c in range(D // 512):
            cs = slice(c * 512, (c + 1) * 512)
            h_ref[sl, cs] = (x_ref[sl, cs].astype(F32) * r * w_ref[layer:layer + 1, cs].astype(F32)).astype(BF16)
        return carry
    lax.fori_loop(0, B // rows, step, 0, unroll=2)


def attn_kernel(layer, first, pos_hbm, x_hbm, nw_hbm, wq_hbm, wk_hbm, wv_hbm, kc_hbm, vc_hbm, *rest):
    if first:
        o_ref, ko_hbm, vo_hbm = rest[:3]
        rest = rest[3:]
    else:
        o_ref, ko_hbm, vo_hbm = rest[2:5]
        rest = rest[5:]
    pos_ref, nw_ref, x_v, h_v, cos_t, sin_t, cos_ref, sin_ref, wq_v, wk_v, wv_v, acc, qkv_v, o_v, q4, o4, kn, vn, rid, kb, vb, wsem, xsem, psem, ksem, vsem, kosem, vosem = rest

    def kv_in(c, slot):
        rs = pl.ds(c * CB, CB)
        return (pltpu.make_async_copy(kc_hbm.at[layer, rs], kb.at[slot], ksem.at[slot]),
                pltpu.make_async_copy(vc_hbm.at[layer, rs], vb.at[slot], vsem.at[slot]))

    def kv_out(c, slot):
        rs = pl.ds(c * CB, CB)
        return (pltpu.make_async_copy(kb.at[slot], ko_hbm.at[layer, rs], kosem.at[slot]),
                pltpu.make_async_copy(vb.at[slot], vo_hbm.at[layer, rs], vosem.at[slot]))

    poscopy = pltpu.make_async_copy(pos_hbm, pos_ref, psem.at[0])
    poscopy.start()
    KC = D // 4
    if first:
        xcopy = pltpu.make_async_copy(x_hbm, x_v, xsem)
        xcopy.start()
        nwcopy = pltpu.make_async_copy(nw_hbm, nw_ref, psem.at[1])
        nwcopy.start()
        wcopies = []
        for c in range(4):
            rs = pl.ds(c * KC, KC)
            wcopies.append([pltpu.make_async_copy(wq_hbm.at[layer, rs], wq_v.at[rs], wsem.at[c, 0]),
                            pltpu.make_async_copy(wk_hbm.at[layer, rs], wk_v.at[rs], wsem.at[c, 1]),
                            pltpu.make_async_copy(wv_hbm.at[layer, rs], wv_v.at[rs], wsem.at[c, 2])])
        for t in wcopies[0]:
            t.start()
    else:
        xcopy = pltpu.make_async_copy(x_hbm, qkv_v, xsem)
        xcopy.start()
        for c in range(PF):
            for t in kv_in(c, c):
                t.start()

    rid[...] = lax.broadcasted_iota(jnp.int32, (S, HD), 0).astype(F32).astype(BF16)
    cos_t[...], sin_t[...] = rope_tables((S, HD))

    def look_up(b, carry):
        p = pos_ref[b]
        cos_ref[pl.ds(b, 1), :] = cos_t[pl.ds(p, 1), :]
        sin_ref[pl.ds(b, 1), :] = sin_t[pl.ds(p, 1), :]
        return carry

    poscopy.wait()
    lax.fori_loop(0, B, look_up, 0, unroll=8)
    xcopy.wait()
    if first:
        nwcopy.wait()
        for cs in wcopies[1:]:
            for t in cs:
                t.start()
        norm_rows(x_v, h_v, nw_ref, layer)
        for c in range(PF):
            for t in kv_in(c, c):
                t.start()
        for c in range(4):
            for t in wcopies[c]:
                t.wait()
            rs = slice(c * KC, (c + 1) * KC)
            w = jnp.concatenate([wq_v[rs, :], wk_v[rs, :], wv_v[rs, :]], axis=1)
            r = jnp.dot(h_v[:, rs], w, preferred_element_type=F32)
            if c == 0:
                acc[...] = r
            else:
                acc[...] += r
        qkv = acc
    else:
        qkv = qkv_v

    cos = cos_ref[...]
    sin = sin_ref[...]

    def rope(t):
        t = t.astype(BF16).astype(F32)
        return (t * cos + pltpu.roll(t, HD // 2, 1) * sin).astype(BF16).astype(F32)

    for hd in range(G):
        q4[pl.ds(hd, B, stride=G), :] = rope(qkv[:, hd * HD:(hd + 1) * HD])
    kn[...] = rope(qkv[:, QW:QW + HD])
    vn[...] = qkv[:, QW + HD:QW + 2 * HD].astype(BF16).astype(F32)

    scale = HD ** -0.5
    row = lax.broadcasted_iota(jnp.int32, (4 * G, HD), 0) // G
    lane = lax.broadcasted_iota(jnp.int32, (CB * G, HD), 1)
    even = (row % 2) == 0
    low = row < 2

    def place(buf, new, slot, b0, i, rowid):
        hit = rowid == jnp.full((S, HD), pos_ref[b0 + i].astype(F32), F32).astype(BF16)
        r = jnp.broadcast_to(new[pl.ds(b0 + i, 1), :], (S, HD)).astype(BF16)
        t = jnp.where(hit, r, buf[slot, i])
        buf[slot, i] = t
        return t

    def quad(ts):
        return jnp.concatenate([jnp.concatenate(ts[:2], axis=1), jnp.concatenate(ts[2:], axis=1)], axis=0)

    def scores(c):
        slot = c % NS
        b0 = c * CB
        rowid = rid[...]
        out = []
        for g in range(CB // 4):
            kt = quad([place(kb, kn, slot, b0, 4 * g + i, rowid) for i in range(4)])
            q = q4[pl.ds(pl.multiple_of(b0 * G + 4 * G * g, 4 * G), 4 * G), :]
            lhs = jnp.concatenate([jnp.where(even, q, 0.0), jnp.where(even, 0.0, q)], axis=1).astype(BF16)
            s2 = lax.dot_general(lhs, kt, (((1,), (1,)), ((), ())), preferred_element_type=F32)
            out.append(jnp.where(low, s2[:, :S], s2[:, S:]))
        return jnp.concatenate(out, axis=0)

    def values(c, s):
        slot = c % NS
        b0 = c * CB
        rowid = rid[...]
        posr = []
        for g in range(CB // 4):
            t = jnp.zeros((4 * G, HD), jnp.int32)
            for i in range(4):
                t = jnp.where(row == i, pos_ref[b0 + 4 * g + i], t)
            posr.append(t)
        s = jnp.where(lane <= jnp.concatenate(posr, axis=0), s * scale, -jnp.inf)
        e = jnp.exp(s - jnp.max(s, axis=1, keepdims=True))
        p = e / jnp.sum(e, axis=1, keepdims=True)
        for g in range(CB // 4):
            vt = quad([place(vb, vn, slot, b0, 4 * g + i, rowid) for i in range(4)])
            pg = p[4 * G * g:4 * G * (g + 1)]
            lhs = jnp.concatenate([jnp.where(low, pg, 0.0), jnp.where(low, 0.0, pg)], axis=1).astype(BF16)
            o2 = jnp.dot(lhs, vt, preferred_element_type=F32)
            o4[pl.ds(pl.multiple_of(b0 * G + 4 * G * g, 4 * G), 4 * G), :] = jnp.where(even, o2[:, :HD], o2[:, HD:])

    def turn(c, j):
        kv_out(c, c % NS)[j].start()
        nxt = c + PF

        @pl.when(nxt < NCH)
        def _():
            @pl.when(nxt >= NS)
            def _():
                kv_out(nxt - NS, nxt % NS)[j].wait()
            kv_in(nxt, nxt % NS)[j].start()

    def arrived(c, j):
        kv_in(c, c % NS)[j].wait()

    arrived(0, 0)
    s0 = scores(0)
    turn(0, 0)

    def chunk(c, s):
        arrived(c + 1, 0)
        arrived(c, 1)
        sn = scores(c + 1)
        values(c, s)
        turn(c + 1, 0)
        turn(c, 1)
        return sn

    sl = lax.fori_loop(0, NCH - 1, chunk, s0)
    arrived(NCH - 1, 1)
    values(NCH - 1, sl)
    turn(NCH - 1, 1)
    for hd in range(G):
        o_v[:, hd * HD:(hd + 1) * HD] = o4[pl.ds(hd, B, stride=G), :].astype(BF16)
    ocopy = pltpu.make_async_copy(o_v, o_ref, xsem)
    ocopy.start()
    for c in range(NCH - NS, NCH):
        for t in kv_out(c, c % NS):
            t.wait()
    ocopy.wait()


def attn_call(layer, pos, x, nw, wq, wk, wv, kc, vc, prev):
    first = prev is None
    cache = jax.ShapeDtypeStruct(kc.shape, BF16)
    ins = [pos, x, nw, wq, wk, wv, kc, vc]
    specs = [ANY] * 8
    alias = {}
    if not first:
        alias = {len(ins): 1, len(ins) + 1: 2}
        ins += list(prev)
        specs += [ANY, ANY]
    return pl.pallas_call(
        functools.partial(attn_kernel, layer, first),
        name=f"attn{layer}",
        out_shape=(jax.ShapeDtypeStruct((B, QW), BF16), cache, cache),
        in_specs=specs,
        out_specs=(ANY, ANY, ANY),
        scratch_shapes=[
            pltpu.SMEM((B,), jnp.int32),
            pltpu.VMEM((2, D), BF16),
            pltpu.VMEM((B, D), BF16),
            pltpu.VMEM((B, D), BF16),
            pltpu.VMEM((S, HD), F32),
            pltpu.VMEM((S, HD), F32),
            pltpu.VMEM((B, HD), F32),
            pltpu.VMEM((B, HD), F32),
            pltpu.VMEM((D, QW), BF16),
            pltpu.VMEM((D, HD), BF16),
            pltpu.VMEM((D, HD), BF16),
            pltpu.VMEM((B, QW + 2 * HD), F32),
            pltpu.VMEM((B, QW + 2 * HD), BF16),
            pltpu.VMEM((B, QW), BF16),
            pltpu.VMEM((B * G, HD), F32),
            pltpu.VMEM((B * G, HD), F32),
            pltpu.VMEM((B, HD), F32),
            pltpu.VMEM((B, HD), F32),
            pltpu.VMEM((S, HD), BF16),
            pltpu.VMEM((NS, CB, S, HD), BF16),
            pltpu.VMEM((NS, CB, S, HD), BF16),
            pltpu.SemaphoreType.DMA((4, 3)),
            pltpu.SemaphoreType.DMA,
            pltpu.SemaphoreType.DMA((2,)),
            pltpu.SemaphoreType.DMA((NS,)),
            pltpu.SemaphoreType.DMA((NS,)),
            pltpu.SemaphoreType.DMA((NS,)),
            pltpu.SemaphoreType.DMA((NS,)),
        ],
        input_output_aliases=alias,
        compiler_params=pltpu.CompilerParams(vmem_limit_bytes=67043328),
    )(*ins)


def mlp_kernel(layer, last, o_hbm, x_hbm, nw_hbm, an_hbm, wo_hbm, wg_hbm, wu_hbm, wd_hbm, wq_hbm, wk_hbm, wv_hbm, *rest):
    if last:
        xo_hbm = rest[0]
        rest = rest[1:]
    else:
        xo_hbm, qkv_hbm = rest[:2]
        rest = rest[2:]
    (o_ref, nw_ref, an_ref, wo_v, wg_v, wu_v, wd_v, part, xg, hc, acc, a_v, qkv_v, xown, d2d, r1, r2, ssb, r_v,
     wsem, osem, xsem, isem, qsem, ssem, rsem) = rest
    me = lax.axis_index("tp")
    k = me % 2
    cx = (me // 2) % 2
    cy = me // 4
    pt = me + 1 - 2 * k
    xn = me + 2 - 4 * cx
    yn = me + 4 - 8 * cy
    dg = xn + 4 - 8 * cy

    def other(p):
        return p + 1 - 2 * k

    peers = (pt, xn, yn, dg, other(xn), other(yn), other(dg))
    order = (dg, xn, yn, me)
    top = pl.ds(0, HB)
    bot = pl.ds(HB, HB)

    def cols(p, h):
        return pl.ds(pl.multiple_of(p * PW + h * PH, PH), PH)

    def chip_cols(p):
        return pl.ds(pl.multiple_of((p // 2) * 2 * PW, 2 * PW), 2 * PW)

    barrier = pltpu.get_barrier_semaphore()
    for d in peers:
        pl.semaphore_signal(barrier, inc=1, device_id={"tp": d}, device_id_type=MESH)

    wos = [pltpu.make_async_copy(wo_hbm.at[layer, :, chip_cols(p)], wo_v.at[:, chip_cols(p)], osem.at[i]) for i, p in enumerate(order)]
    xcs = [pltpu.make_async_copy(x_hbm.at[h] if last else x_hbm.at[:, cols(me, h)], xown.at[h], xsem.at[h]) for h in range(2)]
    NG = 4
    gus = []
    for i in range(NG):
        rs = pl.ds(i * (D // NG), D // NG)
        gus.append(pltpu.make_async_copy(wg_hbm.at[layer, rs], wg_v.at[rs], wsem.at[2 * i]))
        gus.append(pltpu.make_async_copy(wu_hbm.at[layer, rs], wu_v.at[rs], wsem.at[2 * i + 1]))
    ND = 4
    wds = []
    for i in range(ND):
        rs = pl.ds(i * (FW // ND), FW // ND)
        wds.append(pltpu.make_async_copy(wd_hbm.at[layer, rs], wd_v.at[rs], wsem.at[2 * NG + i]))
    ocopy = pltpu.make_async_copy(o_hbm, o_ref, isem.at[0])
    ncopies = [pltpu.make_async_copy(nw_hbm, nw_ref, isem.at[1]), pltpu.make_async_copy(an_hbm, an_ref, isem.at[2])]
    for t in [ocopy] + wos + ncopies + xcs:
        t.start()
    ocopy.wait()

    def remote(src, dst, i, dev):
        return pltpu.make_async_remote_copy(src_ref=src, dst_ref=dst, send_sem=ssem.at[i], recv_sem=rsem.at[i],
                                            device_id={"tp": dev}, device_id_type=MESH)

    def send(src, dst, i, dev):
        c = remote(src, dst, i, dev)
        c.start()
        return c

    def reduce_scatter(make, enter=False):
        live = [{}, {}]

        def pair(h, t):
            c = live[h]
            p = order[t]
            c["d%d" % t].wait_recv()
            part[h, p] = (part[h, p].astype(F32) + d2d[h, t].astype(F32)).astype(BF16)
            if t == 0:
                c["a0"] = send(part.at[h, dg, top], r1.at[h, 0], NC * h + 4, xn)
                c["b0"] = send(part.at[h, dg, bot], r1.at[h, 2], NC * h + 5, yn)
            elif t == 1:
                c["a1"] = send(part.at[h, xn, top], r1.at[h, 1], NC * h + 6, xn)
            elif t == 2:
                c["b1"] = send(part.at[h, yn, bot], r1.at[h, 3], NC * h + 7, yn)

        todo = []
        for h in range(2):
            for t, p in enumerate(order):
                q = other(p)
                make(h, t, p, q)
                if enter and (h, t) == (0, 0):
                    pl.semaphore_wait(barrier, len(peers))
                live[h]["d%d" % t] = send(part.at[h, q], d2d.at[h, t], NC * h + t, pt)
                if todo:
                    pair(*todo.pop(0))
                todo.append((h, t))
        pair(*todo.pop(0))
        for h in range(2):
            c = live[h]
            c["a0"].wait_recv()
            part[h, yn, top] = (part[h, yn, top].astype(F32) + r1[h, 0].astype(F32)).astype(BF16)
            c["a2"] = send(part.at[h, yn, top], r2.at[h, 0], NC * h + 8, yn)
            c["b0"].wait_recv()
            part[h, xn, bot] = (part[h, xn, bot].astype(F32) + r1[h, 2].astype(F32)).astype(BF16)
            c["b2"] = send(part.at[h, xn, bot], r2.at[h, 1], NC * h + 9, xn)
        return live

    def final(h, c):
        for rs, a, b, i, j in ((top, "a1", "a2", 1, 0), (bot, "b1", "b2", 3, 1)):
            c[a].wait_recv()
            c[b].wait_recv()
            tot = part[h, me, rs].astype(F32) + r1[h, i].astype(F32) + r2[h, j].astype(F32)
            new = (xown[h, rs].astype(F32) + tot.astype(BF16).astype(F32)).astype(BF16)
            xown[h, rs] = new
            xg[h, me, rs] = new

    def go(h, c, name, p, rs, i, dev):
        c[name] = send(xg.at[h, p, rs], xg.at[h, p, rs], NC * h + i, dev)

    def gather_first(h, c):
        go(h, c, "ga0", me, top, 10, yn)
        go(h, c, "gb0", me, bot, 11, xn)
        c["p0"] = send(xg.at[h, me], xg.at[h, me], NC * h + 14, pt)

    def gather_second(h, c):
        go(h, c, "ga1", me, top, 12, xn)
        go(h, c, "gb1", me, bot, 13, yn)

    def forward(h, c, got, name, p, rs, i):
        c[got].wait_recv()
        c[name] = send(xg.at[h, p, rs], xg.at[h, p, rs], NC * h + i, pt)

    def relay(h, c):
        forward(h, c, "ga0", "p1", yn, top, 15)
        c["ga2"] = send(xg.at[h, yn, top], xg.at[h, yn, top], NC * h + 16, xn)
        forward(h, c, "gb0", "p2", xn, bot, 17)
        c["gb2"] = send(xg.at[h, xn, bot], xg.at[h, xn, bot], NC * h + 18, yn)

    def near(h, c):
        forward(h, c, "ga1", "p3", xn, top, 19)
        forward(h, c, "gb1", "p4", yn, bot, 20)

    def far(h, c):
        forward(h, c, "ga2", "p5", dg, top, 21)
        forward(h, c, "gb2", "p6", dg, bot, 22)

    def drain(live):
        for c in live:
            for t in c.values():
                t.wait_send()

    def got(live, *names):
        for c in live:
            for n in names:
                c[n].wait_recv()

    def out_half(h, i, p, q):
        if h == 0:
            wos[i].wait()
            if i == 3:
                for t in gus:
                    t.start()
        w = jnp.concatenate([wo_v[:, cols(p, h)], wo_v[:, cols(q, h)]], axis=1)
        t = jnp.dot(o_ref[...], w, preferred_element_type=F32).astype(BF16)
        part[h, p] = t[:, :PH]
        part[h, q] = t[:, PH:]

    def square_start():
        sq = jnp.zeros((B, 128), F32)
        for h in range(2):
            for c in range(PH // 128):
                t = xg[h, me, :, c * 128:(c + 1) * 128].astype(F32)
                sq = sq + t * t
        ssb[0] = jnp.broadcast_to(jnp.sum(sq.T, axis=0, keepdims=True), (8, B))
        return [send(ssb.at[0], ssb.at[1 + j], 2 * NC + j, d) for j, d in enumerate(peers)]

    def square_end(sss):
        for t in sss:
            t.wait_recv()
        tot = ssb[0]
        for j in range(len(peers)):
            tot = tot + ssb[1 + j]
        rr = lax.rsqrt(tot * (1.0 / D) + 1e-5)
        r_v[...] = jnp.broadcast_to(rr[0:1], (128, B)).T

    def norm_rows_of(p, w_ref, row, first, n):
        base = pl.multiple_of((p // 2) * 2 * PW, 2 * PW)

        def norm_step(i, carry):
            sl = pl.ds(pl.multiple_of(first + i * 64, 64), 64)
            r = r_v[sl, :]
            for c in range(2 * PW // 128):
                cs = slice(c * 128, (c + 1) * 128)
                e, h, o = c // 4, (c // 2) % 2, (c % 2) * 128
                w = w_ref[row:row + 1, pl.ds(pl.multiple_of(base + c * 128, 128), 128)].astype(F32)
                hc[sl, cs] = (xg[h, (p // 2) * 2 + e, sl, o:o + 128].astype(F32) * r * w).astype(BF16)
            return carry

        lax.fori_loop(0, n // 64, norm_step, 0)
        return pl.ds(base, 2 * PW)

    def norm_chunk(ps, w_ref, row):
        if len(ps) == 1:
            return [norm_rows_of(ps[0], w_ref, row, 0, B)]
        return [norm_rows_of(p, w_ref, row, i * HB, HB) for i, p in enumerate(ps)]

    def chunk_dot(kss, weight):
        if len(kss) == 1:
            return jnp.dot(hc[...], weight(kss[0]), preferred_element_type=F32)
        return jnp.concatenate([jnp.dot(hc[i * HB:(i + 1) * HB, :], weight(ks), preferred_element_type=F32)
                                for i, ks in enumerate(kss)], axis=0)

    live = reduce_scatter(out_half, True)
    for t in xcs + ncopies:
        t.wait()
    final(0, live[0])
    gather_first(0, live[0])
    gather_second(0, live[0])
    final(1, live[1])
    sss = square_start()
    gather_first(1, live[1])
    gather_second(1, live[1])
    relay(0, live[0])
    square_end(sss)
    relay(1, live[1])
    for t in gus:
        t.wait()
    for t in wds:
        t.start()

    TN = 256

    def gate_up(ps, first, last, between={}):
        kss = norm_chunk(ps, nw_ref, layer)
        for j in range(FW // TN):
            cs = slice(j * TN, (j + 1) * TN)
            gu = chunk_dot(kss, lambda ks: jnp.concatenate([wg_v[ks, cs], wu_v[ks, cs]], axis=1))
            if not first:
                gu = gu + acc[j]
            if not last:
                acc[j] = gu
            else:
                gt = gu[:, :TN].astype(BF16).astype(F32)
                up = gu[:, TN:].astype(BF16).astype(F32)
                a_v[:, cs] = (gt * (1.0 / (1.0 + jnp.exp(-gt))) * up).astype(BF16)
            if j in between:
                between[j]()

    got(live, "p0")
    gate_up([me], True, False)
    near(0, live[0])

    def crossed(i, carry):
        for h in range(2):
            for n in (15 + 4 * i, 17 + 3 * i):
                remote(xg.at[h, me, top], xg.at[h, me, top], NC * h + n, pt).wait_recv()

        def sends():
            pl.when(i == 0)(lambda: near(1, dict(live[1])))
            pl.when(i == 1)(lambda: far(0, dict(live[0])))

        gate_up([yn + i * (xn - yn), xn + i * (yn - xn)], False, False, {2: sends})
        return carry

    lax.fori_loop(0, 2, crossed, 0)
    for h, name, p, rs, i in ((1, "p3", xn, top, 19), (1, "p4", yn, bot, 20), (0, "p5", dg, top, 21), (0, "p6", dg, bot, 22)):
        live[h][name] = remote(xg.at[h, p, rs], xg.at[h, p, rs], NC * h + i, pt)
    far(1, live[1])
    got(live, "p5", "p6")
    gate_up([dg], False, True)
    drain(live)
    for t in sss:
        t.wait_send()
    if not last:
        qs = []
        for i in range(2):
            rs = pl.ds(i * (D // 2), D // 2)
            qs += [pltpu.make_async_copy(wq_hbm.at[layer + 1, rs], wg_v.at[rs, pl.ds(0, QW)], qsem.at[i, 0]),
                   pltpu.make_async_copy(wk_hbm.at[layer + 1, rs], wg_v.at[rs, pl.ds(QW, HD)], qsem.at[i, 1]),
                   pltpu.make_async_copy(wv_hbm.at[layer + 1, rs], wg_v.at[rs, pl.ds(QW + HD, HD)], qsem.at[i, 2])]
    for t in wds:
        t.wait()
    if not last:
        for t in qs:
            t.start()

    def down_half(h, i, p, q):
        w = jnp.concatenate([wd_v[:, cols(p, h)], wd_v[:, cols(q, h)]], axis=1)
        t = jnp.dot(a_v[...], w, preferred_element_type=F32).astype(BF16)
        part[h, p] = t[:, :PH]
        part[h, q] = t[:, PH:]

    live = reduce_scatter(down_half)
    if last:
        for h in range(2):
            final(h, live[h])
            gather_first(h, live[h])
            gather_second(h, live[h])
        for h in range(2):
            relay(h, live[h])
        for h in range(2):
            near(h, live[h])
        outs = []

        def write(p):
            for e in range(2):
                for h in range(2):
                    n = (p // 2) * 2 + e
                    c = pltpu.make_async_copy(xg.at[h, n], xo_hbm.at[:, cols(n, h)], wsem.at[len(outs)])
                    c.start()
                    outs.append(c)

        got(live, "p0")
        write(me)
        for h in range(2):
            far(h, live[h])
        got(live, "p2", "p3")
        write(xn)
        got(live, "p1", "p4")
        write(yn)
        got(live, "p5", "p6")
        write(dg)
        drain(live)
        for c in outs:
            c.wait()
    else:
        final(0, live[0])
        gather_first(0, live[0])
        gather_second(0, live[0])
        final(1, live[1])
        sss = square_start()
        gather_first(1, live[1])
        gather_second(1, live[1])
        outs = [pltpu.make_async_copy(xown, xo_hbm, isem.at[0])]
        outs[0].start()
        relay(0, live[0])
        near(0, live[0])
        square_end(sss)
        relay(1, live[1])
        for t in qs:
            t.wait()

        def qkv(ps, first, end):
            kss = norm_chunk(ps, an_ref, layer + 1)
            r = chunk_dot(kss, lambda ks: wg_v[ks, :QW + 2 * HD])
            if not first:
                r = r + jnp.concatenate([acc[0], acc[1, :, :2 * HD]], axis=1)
            if end:
                qkv_v[...] = r.astype(BF16)
            else:
                acc[0] = r[:, :QW]
                acc[1, :, :2 * HD] = r[:, QW:]

        got(live, "p0")
        qkv([me], True, False)
        near(1, live[1])
        got(live, "p1", "p2")
        qkv([yn, xn], False, False)
        far(0, live[0])
        got(live, "p3", "p4")
        qkv([xn, yn], False, False)
        far(1, live[1])
        got(live, "p5", "p6")
        qkv([dg], False, True)
        outs.append(pltpu.make_async_copy(qkv_v, qkv_hbm, isem.at[1]))
        outs[1].start()
        drain(live)
        for t in sss:
            t.wait_send()
        for c in outs:
            c.wait()


def mlp_call(layer, last, o, x, nw, an, wo, wg, wu, wd, wq, wk, wv):
    if last:
        out_shape = jax.ShapeDtypeStruct((B, D), BF16)
        out_specs = ANY
    else:
        out_shape = (jax.ShapeDtypeStruct((2, B, PH), BF16), jax.ShapeDtypeStruct((B, QW + 2 * HD), BF16))
        out_specs = (ANY, ANY)
    return pl.pallas_call(
        functools.partial(mlp_kernel, layer, last),
        name=f"mlp{layer}",
        out_shape=out_shape,
        in_specs=[ANY] * 11,
        out_specs=out_specs,
        scratch_shapes=[
            pltpu.VMEM((B, QW), BF16),
            pltpu.VMEM((2, D), BF16),
            pltpu.VMEM((2, D), BF16),
            pltpu.VMEM((QW, D), BF16),
            pltpu.VMEM((D, FW), BF16),
            pltpu.VMEM((D, FW), BF16),
            pltpu.VMEM((FW, D), BF16),
            pltpu.VMEM((2, NP, B, PH), BF16),
            pltpu.VMEM((2, NP, B, PH), BF16),
            pltpu.VMEM((B, 2 * PW), BF16),
            pltpu.VMEM((FW // 256, B, 512), F32),
            pltpu.VMEM((B, FW), BF16),
            pltpu.VMEM((B, QW + 2 * HD), BF16),
            pltpu.VMEM((2, B, PH), BF16),
            pltpu.VMEM((2, 4, B, PH), BF16),
            pltpu.VMEM((2, 4, HB, PH), BF16),
            pltpu.VMEM((2, 2, HB, PH), BF16),
            pltpu.VMEM((8, 8, B), F32),
            pltpu.VMEM((B, 128), F32),
            pltpu.SemaphoreType.DMA((16,)),
            pltpu.SemaphoreType.DMA((4,)),
            pltpu.SemaphoreType.DMA((2,)),
            pltpu.SemaphoreType.DMA((3,)),
            pltpu.SemaphoreType.DMA((2, 3)),
            pltpu.SemaphoreType.DMA((2 * NC + 7,)),
            pltpu.SemaphoreType.DMA((2 * NC + 7,)),
        ],
        compiler_params=pltpu.CompilerParams(collective_id=layer, has_side_effects=True, vmem_limit_bytes=67043328),
    )(o, x, nw, an, wo, wg, wu, wd, wq, wk, wv)


def copy_kernel(x_hbm, o_hbm, buf, isem, osem):
    n = buf.shape[0]
    rows = B // n
    ins = [pltpu.make_async_copy(x_hbm.at[pl.ds(i * rows, rows)], buf.at[i], isem.at[i]) for i in range(n)]
    outs = [pltpu.make_async_copy(buf.at[i], o_hbm.at[pl.ds(i * rows, rows)], osem.at[i]) for i in range(n)]
    for t in ins:
        t.start()
    for i in range(n):
        ins[i].wait()
        outs[i].start()
    for t in outs:
        t.wait()


def copy_call(x):
    n = 8
    return pl.pallas_call(
        copy_kernel,
        name="emit",
        out_shape=jax.ShapeDtypeStruct(x.shape, x.dtype),
        in_specs=[ANY],
        out_specs=ANY,
        scratch_shapes=[pltpu.VMEM((n, B // n, D), BF16), pltpu.SemaphoreType.DMA((n,)), pltpu.SemaphoreType.DMA((n,))],
        compiler_params=pltpu.CompilerParams(vmem_limit_bytes=67043328),
    )(x)


def solution(mesh):
    row_spec = P('dp', None)
    pos_spec = P('dp')
    cache_spec = P(None, 'dp', None, 'tp', None)
    norm_spec = P(None, None)
    col_spec = P(None, None, 'tp')
    split_rows = P(None, 'tp', None)

    def local_step(hidden, positions, k_cache, v_cache, attn_norm, w_query, w_key, w_value, w_out, mlp_norm, w_gate, w_up, w_down):
        kc = k_cache.reshape(2, B, S, HD)
        vc = v_cache.reshape(2, B, S, HD)
        x = hidden
        prev = None
        for layer in range(2):
            o, ko, vo = attn_call(layer, positions, x if layer == 0 else qkv, attn_norm, w_query, w_key, w_value, kc, vc, prev)
            prev = (ko, vo)
            y = mlp_call(layer, layer == 1, o, x, mlp_norm, attn_norm, w_out, w_gate, w_up, w_down, w_query, w_key, w_value)
            if layer == 0:
                x, qkv = y
            else:
                x = y
        return copy_call(x), prev[0].reshape(k_cache.shape), prev[1].reshape(v_cache.shape)

    return jax.shard_map(local_step, mesh=mesh, in_specs=(row_spec, pos_spec, cache_spec, cache_spec, norm_spec, col_spec, col_spec, col_spec, split_rows, norm_spec, col_spec, col_spec, split_rows), out_specs=(row_spec, cache_spec, cache_spec), check_vma=False)
```
